128 devices in a mesh: model: 1, data: 128 (over z, y, x, core).
Axes of the slice: x: 4, y: 4, z: 4, core: 2. Of those that a mesh axis runs over, the one named last changes fastest.
Arguments:
- grad_sq: float32 [128, 2, 896, 896], P(('model', 'data'))
- mom_sq: float32 [2, 896, 896], P('model', 'data')
- weight_sq: float32 [2, 896, 896], P('model', 'data')
- grad_kv: float32 [128, 2, 896, 64], P(('model', 'data'))
- mom_kv: float32 [2, 896, 64], P('model', 'data')
- weight_kv: float32 [2, 896, 64], P('model', 'data')
- grad_up: float32 [128, 2, 896, 256], P(('model', 'data'))
- mom_up: float32 [2, 896, 256], P('model', 'data')
- weight_up: float32 [2, 896, 256], P('model', 'data')
- grad_down: float32 [128, 1, 256, 896], P(('model', 'data'))
- mom_down: float32 [1, 256, 896], P('model', 'data')
- weight_down: float32 [1, 256, 896], P('model', 'data')
Outputs:
- output 1: float32 [2, 896, 896], P('model', 'data')
- output 2: float32 [2, 896, 896], P('model', 'data')
- output 3: bfloat16 [2, 896, 896], P('model')
- output 4: float32 [2, 896, 64], P('model', 'data')
- output 5: float32 [2, 896, 64], P('model', 'data')
- output 6: bfloat16 [2, 896, 64], P('model')
- output 7: float32 [2, 896, 256], P('model', 'data')
- output 8: float32 [2, 896, 256], P('model', 'data')
- output 9: bfloat16 [2, 896, 256], P('model')
- output 10: float32 [1, 256, 896], P('model', 'data')
- output 11: float32 [1, 256, 896], P('model', 'data')
- output 12: bfloat16 [1, 256, 896], P('model')
All inputs are finite; a program needn't handle non-finite values.
Results may differ from the reference program's by a relative error of at most 0.0103988.
Values are sent between devices in bfloat16 or wider.
A program may use at most 1 GiB of HBM per device.

```python
import math
import jax
import jax.numpy as jnp
from jax import lax

GROUP = 128
LAYERS = 1
D = 896
FF = 256
KVD = 64
NS_STEPS = 5
MU = 0.95
LR = 0.1
WD = 0.5
EPS = 1e-7
COEF_A = 3.4445
COEF_B = -4.7750
COEF_C = 2.0315


def draw_family(key, count, rows, columns):
    key_grad, key_mom, key_weight = jax.random.split(key, 3)
    grad_part = jax.random.normal(key_grad, (GROUP, count, rows, columns), jnp.float32) * math.sqrt(GROUP)
    momentum = jax.random.normal(key_mom, (count, rows, columns), jnp.float32)
    weight = 0.1 * jax.random.normal(key_weight, (count, rows, columns), jnp.float32)
    return grad_part, momentum, weight


def setup_inputs(seed: int = 0, part: int = 0) -> dict:
    base_key = jax.random.fold_in(jax.random.key(seed), part)
    family_keys = jax.random.split(base_key, 4)
    shapes = (("sq", 2 * LAYERS, D, D), ("kv", 2 * LAYERS, D, KVD), ("up", 2 * LAYERS, D, FF), ("down", LAYERS, FF, D))
    result = {}
    for index, (family_name, count, rows, columns) in enumerate(shapes):
        grad_part, momentum, weight = draw_family(family_keys[index], count, rows, columns)
        result["grad_" + family_name] = grad_part
        result["mom_" + family_name] = momentum
        result["weight_" + family_name] = weight
    return result


def orthogonalize(update):
    rows, columns = update.shape
    update_f32 = update.astype(jnp.float32)
    frob_norm = jnp.sqrt(jnp.sum(update_f32 * update_f32))
    ortho = (update_f32 / (frob_norm + EPS)).astype(jnp.bfloat16)
    if rows > columns:
        ortho = ortho.T
    for step_index in range(NS_STEPS):
        gram_mat = jnp.dot(ortho, ortho.T, preferred_element_type=jnp.float32).astype(jnp.bfloat16)
        square = jnp.dot(gram_mat, gram_mat, preferred_element_type=jnp.float32)
        poly_mat = (COEF_B * gram_mat.astype(jnp.float32) + COEF_C * square).astype(jnp.bfloat16)
        ortho = (COEF_A * ortho.astype(jnp.float32) + jnp.dot(poly_mat, ortho, preferred_element_type=jnp.float32)).astype(jnp.bfloat16)
    if rows > columns:
        ortho = ortho.T
    return ortho


def family_step(grad_part, momentum, weight):
    rows, columns = weight.shape[1], weight.shape[2]
    summed = jnp.sum(grad_part, axis=0) / GROUP
    mom_new = MU * momentum + summed
    update = (summed + MU * mom_new).astype(jnp.bfloat16)
    ortho = lax.map(orthogonalize, update)
    scale = 0.2 * math.sqrt(max(rows, columns))
    weight_new = weight - LR * (scale * ortho.astype(jnp.float32) + WD * weight)
    return mom_new, weight_new, weight_new.astype(jnp.bfloat16)


def reference(grad_sq, mom_sq, weight_sq, grad_kv, mom_kv, weight_kv, grad_up, mom_up, weight_up, grad_down, mom_down, weight_down):
    sq_mom, sq_weight, sq_bf16 = family_step(grad_sq, mom_sq, weight_sq)
    kv_mom, kv_weight, kv_bf16 = family_step(grad_kv, mom_kv, weight_kv)
    up_mom, up_weight, up_bf16 = family_step(grad_up, mom_up, weight_up)
    down_mom, down_weight, down_bf16 = family_step(grad_down, mom_down, weight_down)
    return (sq_mom, sq_weight, sq_bf16, kv_mom, kv_weight, kv_bf16, up_mom, up_weight, up_bf16, down_mom, down_weight, down_bf16)
```

```python
import math
import jax
import jax.numpy as jnp
from jax import lax
from jax.experimental import pallas as pl
from jax.experimental.pallas import tpu as pltpu
from jax.sharding import PartitionSpec as P

NS_STEPS = 5
MU = 0.95
LR = 0.1
WD = 0.5
EPS = 1e-7
COEF_A = 3.4445
COEF_B = -4.7750
COEF_C = 2.0315
GROUP = 128
D = 896
SCALE = 0.2 * math.sqrt(896.0)
MESH = pl.DeviceIdType.MESH
F32 = jnp.float32
BF16 = jnp.bfloat16
DMA = pltpu.SemaphoreType.DMA


def kernel(
    g_sq, g_kv, g_up, g_dn,
    m_sq, m_kv, m_up, m_dn,
    w_sq, w_kv, w_up, w_dn,
    mo_sq, mo_kv, mo_up, mo_dn,
    wo_sq, wo_kv, wo_up, wo_dn,
    b_sq, b_kv, b_up, b_dn,
    br, bp, kvb, upb, dnb, acc,
    r1a, r1b, r1c, r2, r3,
    pieces, recvp, mb, nb, outp, mrecv, outw, wrecv,
    xg, wg, xx, aa, bb, ss, sa, sb,
    vb_sq, vb_kv, vb_up, vb_dn,
    own_s, d2d_s, d2d_r, pre_s, pre_r, mo_s, mo_r, wo_s, wo_r,
    rs1_s, rs1_r, rs2_s, rs2_r, rs3_s, rs3_r,
    u3_s, u3_r, u2_s, u2_r, u1_s, u1_r,
    w3_s, w3_r, w2_s, w2_r, w1_s, w1_r,
    ol_s, or_s, or_r,
):
    me = lax.axis_index("data")
    core = lax.rem(me, 2)
    x = lax.rem(lax.div(me, 2), 4)
    y = lax.rem(lax.div(me, 8), 4)
    z = lax.div(me, 32)
    slot = 2 * x + core
    other = 1 - core
    around = {
        "x": [x] + [lax.rem(x + d, 4) for d in (1, 2, 3)],
        "y": [y] + [lax.rem(y + d, 4) for d in (1, 2, 3)],
        "z": [z] + [lax.rem(z + d, 4) for d in (1, 2, 3)],
    }
    partner = me + other - core
    stride = {"x": 2, "y": 8, "z": 32}
    peers = {dim: [me + (a - around[dim][0]) * stride[dim] for a in around[dim]] for dim in "xyz"}
    row_x = [2 * a - 2 * x for a in around["x"]]

    def peer(dim, delta):
        return peers[dim][delta]

    def remote(src, dst, ssem, rsem, device):
        return pltpu.make_async_remote_copy(
            src_ref=src, dst_ref=dst, send_sem=ssem, recv_sem=rsem,
            device_id={"data": device}, device_id_type=MESH)

    row_peers = [(dx, dc) for dx in range(4) for dc in range(2) if (dx, dc) != (0, 0)]

    row_dev = {(dx, dc): (me, partner)[dc] + row_x[dx] for dx in range(4) for dc in range(2)}
    row_slot = {(dx, dc): 2 * around["x"][dx] + (core, other)[dc] for dx in range(4) for dc in range(2)}

    def row_peer(dx, dc):
        return row_dev[dx, dc]

    barrier = pltpu.get_barrier_semaphore()
    for dx, dc in row_peers:
        pl.semaphore_signal(barrier, inc=1, device_id={"data": row_peer(dx, dc)}, device_id_type=MESH)
    for dim in ("y", "z"):
        for delta in (1, 2, 3):
            pl.semaphore_signal(barrier, inc=1, device_id={"data": peer(dim, delta)}, device_id_type=MESH)

    OFFS = (2, 1, 3, 0)

    def lanes(j):
        return pl.ds(pl.multiple_of(j * 128, 128), 128)

    def common_items(tc, k, w):
        jx, jz = around["x"][OFFS[k]], around["z"][OFFS[k]]
        return [
            (g_sq.at[tc, :, :, :, lanes(jx)], br.at[w, jx]),
            (g_sq.at[tc, jz, :, :, pl.ds(512, 384)], bp.at[w, jz]),
        ]

    def special_items(tc, k, w):
        jz, jy = around["z"][OFFS[k]], around["y"][OFFS[k]]
        if tc == 0:
            return [
                (g_kv.at[0, jz], kvb.at[w, 0, jz]),
                (g_dn.at[:, jy], dnb.at[w, :, jy]),
                (g_kv.at[1, :, jy], kvb.at[w, 1, :, jy]),
            ]
        return [
            (g_up.at[0, jz, :, :, pl.ds(0, 128)], upb.at[w, 0, jz, :, :, pl.ds(0, 128)]),
            (g_up.at[0, :, jy, :, pl.ds(128, 128)], upb.at[w, 0, :, jy, :, pl.ds(128, 128)]),
            (g_up.at[1, :, jy], upb.at[w, 1, :, jy]),
        ]

    def own_copy(k, i, item):
        return pltpu.make_async_copy(item[0], item[1], own_s.at[k, i])

    def par_copy(k, i, item):
        return remote(item[0], item[1], d2d_s.at[k, i], d2d_r.at[k, i], partner)

    def start_own(k):
        for i, item in enumerate(common_items(core, k, 0)):
            own_copy(k, i, item).start()
        for tc in range(2):
            @pl.when(core == tc)
            def _():
                for i, item in enumerate(special_items(tc, k, 0)):
                    own_copy(k, 2 + i, item).start()

    def start_par(k):
        for i, item in enumerate(common_items(other, k, 1)):
            par_copy(k, i, item).start()
        for tc in range(2):
            @pl.when(core == 1 - tc)
            def _():
                for i, item in enumerate(special_items(tc, k, 1)):
                    par_copy(k, 2 + i, item).start()

    def add_chunk(k):
        jx, jy, jz = [around[d][OFFS[k]] for d in "xyz"]
        for i, item in enumerate(common_items(core, k, 0)):
            own_copy(k, i, item).wait()
        for i, item in enumerate(common_items(core, k, 1)):
            par_copy(k, i, item).wait_recv()
        acc[jx] = br[0, jx] + br[1, jx]
        for u in range(3):
            acc[4 + u, jz] = bp[0, jz, :, :, 128 * u:128 * u + 128] + bp[1, jz, :, :, 128 * u:128 * u + 128]

        @pl.when(core == 0)
        def _():
            for i, item in enumerate(special_items(0, k, 0)):
                own_copy(k, 2 + i, item).wait()
            for i, item in enumerate(special_items(0, k, 1)):
                par_copy(k, 2 + i, item).wait_recv()
            acc[7, jz, :, :, 0:64] = kvb[0, 0, jz] + kvb[1, 0, jz]
            acc[7, jz, :, :, 64:128] = jnp.zeros((4, 56, 64), F32)
            rows = dnb[0, :, jy] + dnb[1, :, jy]
            for i in range(7):
                acc[8, :, jy, 8 * i:8 * i + 8, :] = rows[:, 0:8, 128 * i:128 * i + 128]
                acc[9, :, jy, 8 * i:8 * i + 8, :] = rows[:, 8:16, 128 * i:128 * i + 128]
            acc[10, :, jy, :, 0:64] = kvb[0, 1, :, jy] + kvb[1, 1, :, jy]
            acc[10, :, jy, :, 64:128] = jnp.zeros((4, 56, 64), F32)

        @pl.when(core == 1)
        def _():
            for i, item in enumerate(special_items(1, k, 0)):
                own_copy(k, 2 + i, item).wait()
            for i, item in enumerate(special_items(1, k, 1)):
                par_copy(k, 2 + i, item).wait_recv()
            acc[7, jz] = upb[0, 0, jz, :, :, 0:128] + upb[1, 0, jz, :, :, 0:128]
            acc[8, :, jy] = upb[0, 0, :, jy, :, 128:256] + upb[1, 0, :, jy, :, 128:256]
            acc[9, :, jy] = upb[0, 1, :, jy, :, 0:128] + upb[1, 1, :, jy, :, 0:128]
            acc[10, :, jy] = upb[0, 1, :, jy, :, 128:256] + upb[1, 1, :, jy, :, 128:256]

    DIMS1, DIMS2, DIMS3 = ("x", "z", "y"), ("y", "x", "z"), ("z", "y", "x")

    def half1(buf, grp, j, h):
        if grp == 0:
            return buf.at[j, pl.ds(2 * h, 2)]
        if grp == 1:
            return buf.at[pl.ds(4 + 2 * h, 2), j]
        return buf.at[pl.ds(8, 3), pl.ds(2 * h, 2), j]

    def half2(buf, grp, j, h):
        if grp == 0:
            return buf.at[x, pl.ds(2 * h, 2), j]
        if grp == 1:
            return buf.at[4 + j, z, pl.ds(2 * h, 2)]
        return buf.at[pl.ds(8 + 2 * h, 2), j, y]

    def seg3(buf, grp, j):
        if grp == 0:
            return buf.at[x, j, y]
        if grp == 1:
            return buf.at[4 + x, z, j]
        return buf.at[8 + j, z, y]

    def block(buf, grp):
        return buf.at[4 * grp + x, z, y]

    def rs_ring(half, buf, dims, rbufs, ssem, rsem):
        def desc(grp, i):
            dim = dims[grp]
            d, h = ((2, 0), (1, 1), (1, 0), (2, 1), (3, 0), (3, 1))[i]
            src = (around[dim][d], h)
            return remote(half(buf, grp, src[0], src[1]), rbufs[grp].at[i], ssem.at[grp, i], rsem.at[grp, i], peer(dim, 1 if i < 3 else 3))

        def add(grp, j, h, i):
            desc(grp, i).wait_recv()
            ref = half(buf, grp, j, h)
            ref[...] += rbufs[grp][i]

        def first():
            for grp in range(3):
                desc(grp, 0).start()
                desc(grp, 3).start()

        def second():
            for grp in range(3):
                desc(grp, 1).start()
                desc(grp, 4).start()

        def third():
            for grp in range(3):
                p = around[dims[grp]]
                add(grp, p[1], 0, 0)
                desc(grp, 2).start()
                add(grp, p[3], 1, 3)
                desc(grp, 5).start()

        def last():
            for grp in range(3):
                p = around[dims[grp]][0]
                add(grp, p, 1, 1)
                add(grp, p, 0, 4)
            for grp in range(3):
                p = around[dims[grp]][0]
                add(grp, p, 0, 2)
                add(grp, p, 1, 5)

        def drain():
            for grp in range(3):
                for i in range(6):
                    desc(grp, i).wait_send()

        return first, second, third, last, drain

    def ag_ring(half, buf, dims, ssem, rsem):
        def desc(grp, i):
            dim = dims[grp]
            d, h = ((0, 0), (0, 1), (3, 0), (0, 1), (0, 0), (1, 1))[i]
            ref = half(buf, grp, around[dim][d], h)
            return remote(ref, ref, ssem.at[grp, i], rsem.at[grp, i], peer(dim, 1 if i < 3 else 3))

        def first():
            for grp in range(3):
                for i in (0, 3, 1, 4):
                    desc(grp, i).start()

        def second():
            for grp in range(3):
                desc(grp, 0).wait_recv()
                desc(grp, 2).start()
                desc(grp, 3).wait_recv()
                desc(grp, 5).start()

        def last():
            for i in (1, 4, 2, 5):
                for grp in range(3):
                    desc(grp, i).wait_recv()

        def drain():
            for grp in range(3):
                for i in range(6):
                    desc(grp, i).wait_send()

        return first, second, last, drain

    def rs_direct(buf, ssem, rsem):
        def desc(grp, i):
            delta = (2, 1, 3)[i]
            j = around[DIMS3[grp]][delta]
            return remote(seg3(buf, grp, j), r3.at[grp, i], ssem.at[grp, i], rsem.at[grp, i], peer(DIMS3[grp], delta))

        def first():
            for i in range(3):
                for grp in range(3):
                    desc(grp, i).start()

        def last():
            for grp in range(3):
                for i in range(3):
                    desc(grp, i).wait_recv()

        def drain():
            for grp in range(3):
                for i in range(3):
                    desc(grp, i).wait_send()

        return first, last, drain

    def ag_direct(buf, ssem, rsem):
        def desc(grp, i):
            delta = (2, 1, 3)[i]
            ref = block(buf, grp)
            return remote(ref, ref, ssem.at[grp, i], rsem.at[grp, i], peer(DIMS3[grp], delta))

        def first():
            for i in range(3):
                for grp in range(3):
                    desc(grp, i).start()

        def last():
            for grp in range(3):
                for i in range(3):
                    desc(grp, i).wait_recv()

        def drain():
            for grp in range(3):
                for i in range(3):
                    desc(grp, i).wait_send()

        return first, last, drain

    rs1 = rs_ring(half1, acc, DIMS1, (r1a, r1b, r1c), rs1_s, rs1_r)
    rs2 = rs_ring(half2, acc, DIMS2, (r2.at[0], r2.at[1], r2.at[2]), rs2_s, rs2_r)
    rs3 = rs_direct(acc, rs3_s, rs3_r)
    u3 = ag_direct(xg, u3_s, u3_r)
    u2 = ag_ring(half2, xg, DIMS2, u2_s, u2_r)
    u1 = ag_ring(half1, xg, DIMS1, u1_s, u1_r)
    wg3 = ag_direct(wg, w3_s, w3_r)
    wg2 = ag_ring(half2, wg, DIMS2, w2_s, w2_r)
    wg1 = ag_ring(half1, wg, DIMS1, w1_s, w1_r)

    for k in range(4):
        start_own(k)

    for a, (q_sq, q_kv, q_up, q_dn) in enumerate(((m_sq, m_kv, m_up, m_dn), (w_sq, w_kv, w_up, w_dn))):
        for c in range(2):
            for xd in range(4):
                pieces[a, c, xd, 0:7, :] = q_sq[c, :, 128 * xd:128 * xd + 128]
                if xd < 3:
                    pieces[a, c, xd, 8:15, :] = q_sq[c, :, 512 + 128 * xd:640 + 128 * xd]
        pieces[a, 0, 3, 8:15, 0:64] = q_kv[0]
        pieces[a, 0, 2, 16:23, 0:64] = q_kv[1]
        pieces[a, 1, 3, 8:15, :] = q_up[0, :, 0:128]
        pieces[a, 1, 0, 16:23, :] = q_up[0, :, 128:256]
        pieces[a, 1, 1, 16:23, :] = q_up[1, :, 0:128]
        pieces[a, 1, 2, 16:23, :] = q_up[1, :, 128:256]
        for xd in range(2):
            for j in range(7):
                pieces[a, 0, xd, 24 + 2 * j:26 + 2 * j, :] = q_dn[0, :, 128 * j:128 * j + 128]
    acc[11] = jnp.zeros((4, 4, 56, 128), F32)

    pl.semaphore_wait(barrier, 13)

    for k in range(4):
        start_par(k)

    def pre(i):
        dx, dc = row_peers[i]
        return remote(pieces.at[:, (core, other)[dc], around["x"][dx]], recvp.at[slot], pre_s.at[i], pre_r.at[i], row_peer(dx, dc))

    for i in range(7):
        pre(i).start()
    recvp[slot] = pieces[:, core, x]

    add_chunk(0)
    rs1[0]()
    add_chunk(1)
    add_chunk(2)
    rs1[1]()
    add_chunk(3)

    for i in range(7):
        pre(i).wait_recv()
    for a in range(2):
        for g in range(3):
            for s in range(8):
                mb[a, g, 7 * s:7 * s + 7, :] = recvp[s, a, 8 * g:8 * g + 7, :]

    @pl.when(jnp.logical_and(core == 0, x < 2))
    def _():
        for a in range(2):
            for i in range(4):
                for j in range(7):
                    mb[a, 2, 8 * j + 2 * i:8 * j + 2 * i + 2, :] = recvp[4 * x + i, a, 24 + 2 * j:26 + 2 * j, :]

    for g in range(3):
        wg[4 * g + x, z, y] = mb[1, g]

    rs1[2]()
    wg3[0]()
    rs1[3]()
    rs2[0]()
    rs2[1]()
    rs2[2]()
    rs2[3]()
    rs3[0]()
    wg3[1]()
    rs3[1]()

    for g in range(3):
        grad = (acc[4 * g + x, z, y] + r3[g, 0] + r3[g, 1] + r3[g, 2]) * (1.0 / GROUP)
        mom_new = MU * mb[0, g] + grad
        nb[g] = mom_new
        xg[4 * g + x, z, y] = (grad + MU * mom_new).astype(BF16)
    u3[0]()

    def pack_rows(src, dst):
        for s in range(8):
            for g in range(3):
                dst[s, 8 * g:8 * g + 7, :] = src[g, 7 * s:7 * s + 7, :]
            for j in range(7):
                r = 8 * j + 2 * (s % 4)
                dst[s, 24 + 2 * j:26 + 2 * j, :] = src[2, r:r + 2, :]

    def post(src, dst, ssem, rsem, i):
        dx, dc = row_peers[i]
        dest = row_slot[dx, dc]
        return remote(src.at[dest], dst.at[slot], ssem.at[i], rsem.at[i], row_peer(dx, dc))

    def unpack_rows(src, o_sq, o_kv, o_up, o_dn):
        for c in range(2):
            for xs in range(4):
                t = 2 * xs + c
                o_sq[c, :, 128 * xs:128 * xs + 128] = src[t, 0:7, :]
                if xs < 3:
                    o_sq[c, :, 512 + 128 * xs:640 + 128 * xs] = src[t, 8:15, :]
        o_kv[0] = src[6, 8:15, 0:64]
        o_kv[1] = src[4, 16:23, 0:64]
        o_up[0, :, 0:128] = src[7, 8:15, :]
        o_up[0, :, 128:256] = src[1, 16:23, :]
        o_up[1, :, 0:128] = src[3, 16:23, :]
        o_up[1, :, 128:256] = src[5, 16:23, :]
        t = 2 * lax.div(slot, 4)
        for j in range(7):
            o_dn[0, :, 128 * j:128 * j + 128] = src[t, 24 + 2 * j:26 + 2 * j, :]

    pack_rows(nb, outp)
    u3[1]()
    u2[0]()
    u2[1]()
    u2[2]()
    u1[0]()
    for i in range(7):
        post(outp, mrecv, mo_s, mo_r, i).start()
    mrecv[slot] = outp[slot]
    wg2[0]()
    u1[1]()
    wg2[1]()
    u1[2]()

    def total(units, width=128):
        part = jnp.zeros((56, width), F32)
        for u in units:
            v = xg[u].astype(F32)
            part = part + jnp.sum(v * v, axis=(0, 1))[:, 0:width]
        return 1.0 / (jnp.sqrt(jnp.sum(part, keepdims=True)) + EPS)

    def column(u, inv):
        return xg[u].astype(F32).reshape(D, 128) * inv

    inv = total(range(7))
    for u in range(7):
        xx[0, :, 128 * u:128 * u + 128] = column(u, inv).astype(BF16)

    @pl.when(core == 0)
    def _():
        inv_d = total((8, 9))
        both = [(xg[u].astype(F32) * inv_d).reshape(16, 7, 8, 128) for u in (8, 9)]
        both = jnp.concatenate(both, axis=2)
        for j in range(7):
            ss[0, 0, :, 128 * j:128 * j + 128] = both[:, j].reshape(256, 128).astype(BF16)
        inv_0, inv_1 = total((7,), 64), total((10,), 64)
        ss[0, 1, 0:64, :] = column(7, inv_0).T[0:64].astype(BF16)
        ss[0, 1, 64:128, :] = column(10, inv_1).T[0:64].astype(BF16)
        ss[0, 1, 128:256, :] = jnp.zeros((128, D), BF16)

    @pl.when(core == 1)
    def _():
        for i in range(2):
            inv_u = total((7 + 2 * i, 8 + 2 * i))
            for h in range(2):
                ss[0, i, 128 * h:128 * h + 128, :] = column(7 + 2 * i + h, inv_u).T.astype(BF16)

    wg2[2]()
    wg1[0]()

    NT = (((1,), (1,)), ((), ()))
    ROWS = ((0, 256), (256, 256), (512, 256), (768, 128))
    row_id = lax.broadcasted_iota(jnp.int32, (256, 256), 0) // 64
    col_id = lax.broadcasted_iota(jnp.int32, (256, 256), 1) // 64
    keep = jnp.logical_or(row_id == col_id, core == 1)

    def step(it, carry):
        cur = lax.rem(it, 2)
        nxt = 1 - cur
        for r, n in ROWS:
            aa[r:r + n, :] = lax.dot_general(xx[cur, r:r + n, :], xx[cur], NT, preferred_element_type=F32).astype(BF16)
        for i in range(2):
            g = lax.dot_general(ss[cur, i], ss[cur, i], NT, preferred_element_type=F32)
            if i == 1:
                g = jnp.where(keep, g, 0.0)
            sa[i] = g.astype(BF16)

        @pl.when(it == 1)
        def _():
            wg1[1]()

        for r, n in ROWS:
            sq = jnp.dot(aa[r:r + n, :], aa[...], preferred_element_type=F32)
            bb[r:r + n, :] = (COEF_B * aa[r:r + n, :].astype(F32) + COEF_C * sq).astype(BF16)
        for i in range(2):
            sq = jnp.dot(sa[i], sa[i], preferred_element_type=F32)
            sb[i] = (COEF_B * sa[i].astype(F32) + COEF_C * sq).astype(BF16)
        for r, n in ROWS:
            prod = jnp.dot(bb[r:r + n, :], xx[cur], preferred_element_type=F32)
            xx[nxt, r:r + n, :] = (COEF_A * xx[cur, r:r + n, :].astype(F32) + prod).astype(BF16)
        for i in range(2):
            prod = jnp.dot(sb[i], ss[cur, i], preferred_element_type=F32)
            ss[nxt, i] = (COEF_A * ss[cur, i].astype(F32) + prod).astype(BF16)
        return carry

    lax.fori_loop(0, NS_STEPS, step, 0)
    fin = NS_STEPS % 2

    wg1[2]()
    wg1[3]()
    wg2[3]()
    wg3[2]()

    def update(w, v):
        return w - LR * (SCALE * v + WD * w)

    def out_copies(i, refs):
        src, dst = refs
        return (pltpu.make_async_copy(src, dst, ol_s.at[i]),
                remote(src, dst, or_s.at[i], or_r.at[i], partner))

    def sq_refs(p, c):
        return vb_sq.at[pl.ds(112 * p, 112)], b_sq.at[c, pl.ds(112 * p, 112)]

    def small_refs(i, c):
        if c == 0:
            return ((vb_kv.at[0], b_kv.at[0]), (vb_dn, b_dn.at[0]), (vb_kv.at[1], b_kv.at[1]))[i]
        return ((vb_up.at[0], b_up.at[0]), (vb_up.at[1], b_up.at[1]))[i]

    def column_out(u, v, width, dst, lane):
        new = update(wg[u, :, :, :, 0:width].reshape(D, width), v)
        wg[u, :, :, :, 0:width] = new.reshape(4, 4, 56, width)
        dst[:, lane:lane + width] = new.astype(BF16)

    @pl.when(core == 0)
    def _():
        v = ss[fin, 1, 0:128, :].astype(F32).T
        column_out(7, v[:, 0:64], 64, vb_kv.at[0], 0)
        column_out(10, v[:, 64:128], 64, vb_kv.at[1], 0)
        for j in range(7):
            v = ss[fin, 0, :, 128 * j:128 * j + 128].astype(F32).reshape(4, 4, 16, 128)
            lo = update(wg[8, :, :, 8 * j:8 * j + 8, :], v[:, :, 0:8])
            hi = update(wg[9, :, :, 8 * j:8 * j + 8, :], v[:, :, 8:16])
            wg[8, :, :, 8 * j:8 * j + 8, :] = lo
            wg[9, :, :, 8 * j:8 * j + 8, :] = hi
            vb_dn[:, 128 * j:128 * j + 128] = jnp.concatenate([lo, hi], axis=2).reshape(256, 128).astype(BF16)
        for i in range(3):
            for cp in out_copies(8 + i, small_refs(i, 0)):
                cp.start()

    @pl.when(core == 1)
    def _():
        for i in range(2):
            for h in range(2):
                v = ss[fin, i, 128 * h:128 * h + 128, :].astype(F32).T
                column_out(7 + 2 * i + h, v, 128, vb_up.at[i], 128 * h)
        for i in range(2):
            for cp in out_copies(8 + i, small_refs(i, 1)):
                cp.start()

    for p in range(8):
        zz, yy = p // 2, 2 * (p % 2)
        v = xx[fin, 112 * p:112 * p + 112, :].astype(F32)
        for u in range(7):
            new = update(wg[u, zz, yy:yy + 2].reshape(112, 128), v[:, 128 * u:128 * u + 128])
            wg[u, zz, yy:yy + 2] = new.reshape(2, 56, 128)
            vb_sq[112 * p:112 * p + 112, 128 * u:128 * u + 128] = new.astype(BF16)
        for cp in out_copies(p, sq_refs(p, core)):
            cp.start()

    for g in range(3):
        nb[g] = wg[4 * g + x, z, y]
    pack_rows(nb, outw)
    for i in range(7):
        post(outw, wrecv, wo_s, wo_r, i).start()
    wrecv[slot] = outw[slot]

    for i in range(7):
        post(outp, mrecv, mo_s, mo_r, i).wait_recv()
    unpack_rows(mrecv, mo_sq, mo_kv, mo_up, mo_dn)
    for i in range(7):
        post(outw, wrecv, wo_s, wo_r, i).wait_recv()
    unpack_rows(wrecv, wo_sq, wo_kv, wo_up, wo_dn)

    for p in range(8):
        loc, rem = out_copies(p, sq_refs(p, core))
        loc.wait()
        rem.wait()
    for c in range(2):
        @pl.when(core == c)
        def _():
            for i in range(3 - c):
                loc, rem = out_copies(8 + i, small_refs(i, c))
                loc.wait()
                rem.wait_send()
            for i in range(2 + c):
                out_copies(8 + i, small_refs(i, 1 - c))[1].wait_recv()
    for i in range(7):
        pre(i).wait_send()
        post(outp, mrecv, mo_s, mo_r, i).wait_send()
        post(outw, wrecv, wo_s, wo_r, i).wait_send()
    for k in range(4):
        for i, item in enumerate(common_items(other, k, 1)):
            par_copy(k, i, item).wait_send()
        for tc in range(2):
            @pl.when(core == 1 - tc)
            def _():
                for i, item in enumerate(special_items(tc, k, 1)):
                    par_copy(k, 2 + i, item).wait_send()
    rs1[4]()
    rs2[4]()
    rs3[2]()
    u3[2]()
    u2[3]()
    u1[3]()


def solution(mesh):
    grad_spec = P(("model", "data"))
    slab_spec = P("model", "data")
    full_spec = P("model")

    def local_step(g_sq, m_sq, w_sq, g_kv, m_kv, w_kv, g_up, m_up, w_up, g_dn, m_dn, w_dn):
        g_sq = g_sq.reshape(2, 4, 4, 56, 896)
        g_kv = g_kv.reshape(2, 4, 4, 56, 64)
        g_up = g_up.reshape(2, 4, 4, 56, 256)
        g_dn = g_dn.reshape(4, 4, 16, 896)
        vm = pl.BlockSpec(memory_space=pltpu.VMEM)
        hb = pl.BlockSpec(memory_space=pl.ANY)
        rows = [jax.ShapeDtypeStruct(s, F32) for s in ((2, 7, 896), (2, 7, 64), (2, 7, 256), (1, 2, 896))]
        full = [jax.ShapeDtypeStruct(s, BF16) for s in ((2, 896, 896), (2, 896, 64), (2, 896, 256), (1, 256, 896))]
        V = pltpu.VMEM
        scratch = [
            V((2, 4, 4, 4, 56, 128), F32), V((2, 4, 4, 56, 384), F32), V((2, 2, 4, 4, 56, 64), F32),
            V((2, 2, 4, 4, 56, 256), F32), V((2, 4, 4, 16, 896), F32), V((12, 4, 4, 56, 128), F32),
            V((6, 2, 4, 56, 128), F32), V((6, 2, 4, 56, 128), F32), V((6, 3, 2, 56, 128), F32),
            V((3, 6, 2, 56, 128), F32), V((3, 3, 56, 128), F32),
            V((2, 2, 4, 40, 128), F32), V((8, 2, 40, 128), F32), V((2, 3, 56, 128), F32), V((3, 56, 128), F32),
            V((8, 40, 128), F32), V((8, 40, 128), F32), V((8, 40, 128), F32), V((8, 40, 128), F32),
            V((12, 4, 4, 56, 128), BF16), V((12, 4, 4, 56, 128), F32),
            V((2, D, D), BF16), V((D, D), BF16), V((D, D), BF16),
            V((2, 2, 256, D), BF16), V((2, 256, 256), BF16), V((2, 256, 256), BF16),
            V((D, D), BF16), V((2, D, 64), BF16), V((2, D, 256), BF16), V((256, D), BF16),
            DMA((4, 5)), DMA((4, 5)), DMA((4, 5)), DMA((7,)), DMA((7,)), DMA((7,)), DMA((7,)), DMA((7,)), DMA((7,)),
            DMA((3, 6)), DMA((3, 6)), DMA((3, 6)), DMA((3, 6)), DMA((3, 3)), DMA((3, 3)),
            DMA((3, 3)), DMA((3, 3)), DMA((3, 6)), DMA((3, 6)), DMA((3, 6)), DMA((3, 6)),
            DMA((3, 3)), DMA((3, 3)), DMA((3, 6)), DMA((3, 6)), DMA((3, 6)), DMA((3, 6)),
            DMA((11,)), DMA((11,)), DMA((11,)),
        ]
        out = pl.pallas_call(
            kernel,
            out_shape=rows + rows + full,
            in_specs=[hb] * 4 + [vm] * 8,
            out_specs=[vm] * 8 + [hb] * 4,
            scratch_shapes=scratch,
            compiler_params=pltpu.CompilerParams(collective_id=0, has_side_effects=True, vmem_limit_bytes=63_000_000),
            name="muon",
        )(g_sq, g_kv, g_up, g_dn, m_sq, m_kv, m_up, m_dn, w_sq, w_kv, w_up, w_dn)
        m, w, b = out[0:4], out[4:8], out[8:12]
        result = []
        for i in range(4):
            result += [m[i], w[i], b[i]]
        return tuple(result)

    in_specs = (grad_spec, slab_spec, slab_spec) * 4
    out_specs = (slab_spec, slab_spec, full_spec) * 4
    return jax.shard_map(local_step, mesh=mesh, in_specs=in_specs, out_specs=out_specs, check_vma=False)
```

```python
import math
import jax
import jax.numpy as jnp
from jax import lax
from jax.experimental import pallas as pl
from jax.experimental.pallas import tpu as pltpu
from jax.sharding import PartitionSpec as P

NS_STEPS = 5
MU = 0.95
LR = 0.1
WD = 0.5
EPS = 1e-7
COEF_A = 3.4445
COEF_B = -4.7750
COEF_C = 2.0315
GROUP = 128
D = 896
SCALE = 0.2 * math.sqrt(896.0)
MESH = pl.DeviceIdType.MESH
F32 = jnp.float32
BF16 = jnp.bfloat16
DMA = pltpu.SemaphoreType.DMA


def kernel(
    g_sq, g_kv, g_up, g_dn,
    m_sq, m_kv, m_up, m_dn,
    w_sq, w_kv, w_up, w_dn,
    mrecv, wrecv, vb_sq, vb_kv, vb_up, vb_dn,
    br, bp, kvb, upb, dnb, acc,
    r1a, r1b, r1c, r2, r3,
    q_sq, q_kv, q_up, q_dn,
    pieces, recvp, mb, nb, outp, outw,
    xg, wg, xx, aa, bb, ss, sa, sb,
    own_s, row_s, d2d_s, d2d_r, pre_s, pre_r, mo_s, mo_r, wo_s, wo_r,
    rs1_s, rs1_r, rs2_s, rs2_r, rs3_s, rs3_r,
    u3_s, u3_r, u2_s, u2_r, u1_s, u1_r,
    w3_s, w3_r, w2_s, w2_r, w1_s, w1_r,
    or_s, or_r,
):
    me = lax.axis_index("data")
    core = lax.rem(me, 2)
    x = lax.rem(lax.div(me, 2), 4)
    y = lax.rem(lax.div(me, 8), 4)
    z = lax.div(me, 32)
    slot = 2 * x + core
    other = 1 - core
    around = {
        "x": [x] + [lax.rem(x + d, 4) for d in (1, 2, 3)],
        "y": [y] + [lax.rem(y + d, 4) for d in (1, 2, 3)],
        "z": [z] + [lax.rem(z + d, 4) for d in (1, 2, 3)],
    }
    partner = me + other - core
    stride = {"x": 2, "y": 8, "z": 32}
    peers = {dim: [me + (a - around[dim][0]) * stride[dim] for a in around[dim]] for dim in "xyz"}
    row_x = [2 * a - 2 * x for a in around["x"]]

    def peer(dim, delta):
        return peers[dim][delta]

    def remote(src, dst, ssem, rsem, device):
        return pltpu.make_async_remote_copy(
            src_ref=src, dst_ref=dst, send_sem=ssem, recv_sem=rsem,
            device_id={"data": device}, device_id_type=MESH)

    row_peers = [(dx, dc) for dx in range(4) for dc in range(2) if (dx, dc) != (0, 0)]

    row_dev = {(dx, dc): (me, partner)[dc] + row_x[dx] for dx in range(4) for dc in range(2)}
    row_slot = {(dx, dc): 2 * around["x"][dx] + (core, other)[dc] for dx in range(4) for dc in range(2)}

    def row_peer(dx, dc):
        return row_dev[dx, dc]

    barrier = pltpu.get_barrier_semaphore()
    for dx, dc in row_peers:
        pl.semaphore_signal(barrier, inc=1, device_id={"data": row_peer(dx, dc)}, device_id_type=MESH)
    for dim in ("y", "z"):
        for delta in (1, 2, 3):
            pl.semaphore_signal(barrier, inc=1, device_id={"data": peer(dim, delta)}, device_id_type=MESH)

    OFFS = (2, 1, 3, 0)

    def lanes(j):
        return pl.ds(pl.multiple_of(j * 128, 128), 128)

    def common_items(tc, k, w):
        jx, jz = around["x"][OFFS[k]], around["z"][OFFS[k]]
        return [
            (g_sq.at[tc, :, :, :, lanes(jx)], br.at[w, jx]),
            (g_sq.at[tc, jz, :, :, pl.ds(512, 384)], bp.at[w, jz]),
        ]

    def special_items(tc, k, w):
        jz, jy = around["z"][OFFS[k]], around["y"][OFFS[k]]
        if tc == 0:
            items = [(g_dn.at[:, jy], dnb.at[w, :, jy])]
            return items + [(g_kv, kvb.at[w])] if k == 0 else items
        return [
            (g_up.at[0, jz, :, :, pl.ds(0, 128)], upb.at[w, 0, jz, :, :, pl.ds(0, 128)]),
            (g_up.at[0, :, jy, :, pl.ds(128, 128)], upb.at[w, 0, :, jy, :, pl.ds(128, 128)]),
            (g_up.at[1, :, jy], upb.at[w, 1, :, jy]),
        ]

    def own_copy(k, i, item):
        return pltpu.make_async_copy(item[0], item[1], own_s.at[k, i])

    def par_copy(k, i, item):
        return remote(item[0], item[1], d2d_s.at[k, i], d2d_r.at[k, i], partner)

    def start_own(k):
        for i, item in enumerate(common_items(core, k, 0)):
            own_copy(k, i, item).start()
        for tc in range(2):
            @pl.when(core == tc)
            def _():
                for i, item in enumerate(special_items(tc, k, 0)):
                    own_copy(k, 2 + i, item).start()

    def start_par(k):
        for i, item in enumerate(common_items(other, k, 1)):
            par_copy(k, i, item).start()
        for tc in range(2):
            @pl.when(core == 1 - tc)
            def _():
                for i, item in enumerate(special_items(tc, k, 1)):
                    par_copy(k, 2 + i, item).start()

    def arrive(k, i, own, par):
        own_copy(k, i, own).wait()
        par_copy(k, i, par).wait_recv()

    def add_r(k):
        jx = around["x"][OFFS[k]]
        arrive(k, 0, common_items(core, k, 0)[0], common_items(core, k, 1)[0])
        acc[jx] = br[0, jx] + br[1, jx]

    def add_p(k):
        jz = around["z"][OFFS[k]]
        arrive(k, 1, common_items(core, k, 0)[1], common_items(core, k, 1)[1])
        for u in range(3):
            acc[4 + u, jz] = bp[0, jz, :, :, 128 * u:128 * u + 128] + bp[1, jz, :, :, 128 * u:128 * u + 128]

        @pl.when(core == 1)
        def _():
            arrive(k, 2, special_items(1, k, 0)[0], special_items(1, k, 1)[0])
            acc[7, jz] = upb[0, 0, jz, :, :, 0:128] + upb[1, 0, jz, :, :, 0:128]

    def add_q(k):
        jy = around["y"][OFFS[k]]

        @pl.when(core == 0)
        def _():
            arrive(k, 2, special_items(0, k, 0)[0], special_items(0, k, 1)[0])
            rows = dnb[0, :, jy] + dnb[1, :, jy]
            for i in range(7):
                acc[8, :, jy, 8 * i:8 * i + 8, :] = rows[:, 0:8, 128 * i:128 * i + 128]
                acc[9, :, jy, 8 * i:8 * i + 8, :] = rows[:, 8:16, 128 * i:128 * i + 128]

        @pl.when(core == 1)
        def _():
            for i in (1, 2):
                arrive(k, 2 + i, special_items(1, k, 0)[i], special_items(1, k, 1)[i])
            acc[8, :, jy] = upb[0, 0, :, jy, :, 128:256] + upb[1, 0, :, jy, :, 128:256]
            acc[9, :, jy] = upb[0, 1, :, jy, :, 0:128] + upb[1, 1, :, jy, :, 0:128]
            acc[10, :, jy] = upb[0, 1, :, jy, :, 128:256] + upb[1, 1, :, jy, :, 128:256]

    def add_kv():
        @pl.when(core == 0)
        def _():
            own_copy(0, 3, special_items(0, 0, 0)[1]).wait()
            par_copy(0, 3, special_items(0, 0, 1)[1]).wait_recv()
            acc[7] = (kvb[0] + kvb[1]).reshape(128, D).T.reshape(4, 4, 56, 128)

    DIMS1, DIMS2, DIMS3 = ("x", "z", "y"), ("y", "x", "z"), ("z", "y", "x")

    def half1(buf, grp, j, h):
        if grp == 0:
            return buf.at[j, pl.ds(2 * h, 2)]
        if grp == 1:
            return buf.at[pl.ds(4 + 2 * h, 2), j]
        return buf.at[pl.ds(8, 3), pl.ds(2 * h, 2), j]

    def half2(buf, grp, j, h):
        if grp == 0:
            return buf.at[x, pl.ds(2 * h, 2), j]
        if grp == 1:
            return buf.at[4 + j, z, pl.ds(2 * h, 2)]
        return buf.at[pl.ds(8 + 2 * h, 2), j, y]

    def seg3(buf, grp, j):
        if grp == 0:
            return buf.at[x, j, y]
        if grp == 1:
            return buf.at[4 + x, z, j]
        return buf.at[8 + j, z, y]

    def block(buf, grp):
        return buf.at[4 * grp + x, z, y]

    def rs_ring(half, buf, dims, rbufs, ssem, rsem):
        def desc(grp, i):
            dim = dims[grp]
            d, h = ((2, 0), (1, 1), (1, 0), (2, 1), (3, 0), (3, 1))[i]
            src = (around[dim][d], h)
            return remote(half(buf, grp, src[0], src[1]), rbufs[grp].at[i], ssem.at[grp, i], rsem.at[grp, i], peer(dim, 1 if i < 3 else 3))

        def add(grp, j, h, i):
            desc(grp, i).wait_recv()
            ref = half(buf, grp, j, h)
            ref[...] += rbufs[grp][i]

        def first(groups=(0, 1, 2)):
            for grp in groups:
                desc(grp, 0).start()
                desc(grp, 3).start()

        def second(groups=(0, 1, 2)):
            for grp in groups:
                desc(grp, 1).start()
                desc(grp, 4).start()

        def third(groups=(0, 1, 2)):
            for grp in groups:
                p = around[dims[grp]]
                add(grp, p[1], 0, 0)
                desc(grp, 2).start()
                add(grp, p[3], 1, 3)
                desc(grp, 5).start()

        def last(groups=(0, 1, 2)):
            for grp in groups:
                p = around[dims[grp]][0]
                add(grp, p, 1, 1)
                add(grp, p, 0, 4)
                add(grp, p, 0, 2)
                add(grp, p, 1, 5)

        def drain():
            for grp in range(3):
                for i in range(6):
                    desc(grp, i).wait_send()

        return first, second, third, last, drain

    def ag_ring(half, buf, dims, ssem, rsem):
        def desc(grp, i):
            dim = dims[grp]
            d, h = ((0, 0), (0, 1), (3, 0), (0, 1), (0, 0), (1, 1))[i]
            ref = half(buf, grp, around[dim][d], h)
            return remote(ref, ref, ssem.at[grp, i], rsem.at[grp, i], peer(dim, 1 if i < 3 else 3))

        def first(groups=(0, 1, 2)):
            for grp in groups:
                for i in (0, 3, 1, 4):
                    desc(grp, i).start()

        def second(groups=(0, 1, 2)):
            for grp in groups:
                desc(grp, 0).wait_recv()
                desc(grp, 2).start()
                desc(grp, 3).wait_recv()
                desc(grp, 5).start()

        def last(groups=(0, 1, 2)):
            for grp in groups:
                for i in (1, 4, 2, 5):
                    desc(grp, i).wait_recv()

        def drain():
            for grp in range(3):
                for i in range(6):
                    desc(grp, i).wait_send()

        return first, second, last, drain

    def rs_direct(buf, ssem, rsem):
        def desc(grp, i):
            delta = (2, 1, 3)[i]
            j = around[DIMS3[grp]][delta]
            return remote(seg3(buf, grp, j), r3.at[grp, i], ssem.at[grp, i], rsem.at[grp, i], peer(DIMS3[grp], delta))

        def first(groups=(0, 1, 2)):
            for i in range(3):
                for grp in groups:
                    desc(grp, i).start()

        def last(groups=(0, 1, 2)):
            for grp in groups:
                for i in range(3):
                    desc(grp, i).wait_recv()

        def drain():
            for grp in range(3):
                for i in range(3):
                    desc(grp, i).wait_send()

        return first, last, drain

    def ag_direct(buf, ssem, rsem):
        def desc(grp, i):
            delta = (2, 1, 3)[i]
            ref = block(buf, grp)
            return remote(ref, ref, ssem.at[grp, i], rsem.at[grp, i], peer(DIMS3[grp], delta))

        def first(groups=(0, 1, 2)):
            for i in range(3):
                for grp in groups:
                    desc(grp, i).start()

        def last(groups=(0, 1, 2)):
            for grp in groups:
                for i in range(3):
                    desc(grp, i).wait_recv()

        def drain():
            for grp in range(3):
                for i in range(3):
                    desc(grp, i).wait_send()

        return first, last, drain

    rs1 = rs_ring(half1, acc, DIMS1, (r1a, r1b, r1c), rs1_s, rs1_r)
    rs2 = rs_ring(half2, acc, DIMS2, (r2.at[0], r2.at[1], r2.at[2]), rs2_s, rs2_r)
    rs3 = rs_direct(acc, rs3_s, rs3_r)
    u3 = ag_direct(xg, u3_s, u3_r)
    u2 = ag_ring(half2, xg, DIMS2, u2_s, u2_r)
    u1 = ag_ring(half1, xg, DIMS1, u1_s, u1_r)
    wg3 = ag_direct(wg, w3_s, w3_r)
    wg2 = ag_ring(half2, wg, DIMS2, w2_s, w2_r)
    wg1 = ag_ring(half1, wg, DIMS1, w1_s, w1_r)

    for k in range(4):
        start_own(k)

    def row_copies():
        pairs = ((m_sq, w_sq, q_sq), (m_kv, w_kv, q_kv), (m_up, w_up, q_up), (m_dn, w_dn, q_dn))
        return [pltpu.make_async_copy(src[a], src[2].at[a], row_s.at[a, i]) for i, src in enumerate(pairs) for a in range(2)]

    for cp in row_copies():
        cp.start()

    def pack_pieces():
        for cp in row_copies():
            cp.wait()
        for a in range(2):
            for c in range(2):
                for xd in range(4):
                    pieces[a, c, xd, 0:7, :] = q_sq[a, :, c, 128 * xd:128 * xd + 128]
                    if xd < 3:
                        pieces[a, c, xd, 8:15, :] = q_sq[a, :, c, 512 + 128 * xd:640 + 128 * xd]
            pieces[a, 0, 3, 8:15, 0:64] = q_kv[a, :, 0, :]
            pieces[a, 0, 3, 8:15, 64:128] = q_kv[a, :, 1, :]
            pieces[a, 1, 3, 8:15, :] = q_up[a, :, 0, 0:128]
            pieces[a, 1, 0, 16:23, :] = q_up[a, :, 0, 128:256]
            pieces[a, 1, 1, 16:23, :] = q_up[a, :, 1, 0:128]
            pieces[a, 1, 2, 16:23, :] = q_up[a, :, 1, 128:256]
            for xd in range(2):
                for j in range(7):
                    pieces[a, 0, xd, 24 + 2 * j:26 + 2 * j, :] = q_dn[a, 0, :, 128 * j:128 * j + 128]

    acc[11] = jnp.zeros((4, 4, 56, 128), F32)

    @pl.when(core == 0)
    def _():
        acc[10] = jnp.zeros((4, 4, 56, 128), F32)

    pack_pieces()
    pl.semaphore_wait(barrier, 13)

    for k in range(4):
        start_par(k)

    def pre(a, i):
        dx, dc = row_peers[i]
        return remote(pieces.at[a, (core, other)[dc], around["x"][dx]], recvp.at[a, slot], pre_s.at[a, i], pre_r.at[a, i], row_peer(dx, dc))

    def pre_start(a):
        for i in range(7):
            pre(a, i).start()
        recvp[a, slot] = pieces[a, core, x]

    def pre_done(a):
        for i in range(7):
            pre(a, i).wait_recv()
        for g in range(3):
            for s in range(8):
                mb[a, g, 7 * s:7 * s + 7, :] = recvp[a, s, 8 * g:8 * g + 7, :]

        @pl.when(jnp.logical_and(core == 0, x < 2))
        def _():
            for i in range(4):
                for j in range(7):
                    mb[a, 2, 8 * j + 2 * i:8 * j + 2 * i + 2, :] = recvp[a, 4 * x + i, 24 + 2 * j:26 + 2 * j, :]

    pre_start(0)
    add_r(0)
    rs1[0]((0,))
    add_q(0)
    rs1[0]((2,))
    add_p(0)
    add_kv()
    rs1[0]((1,))
    for add, g in ((add_r, 0), (add_p, 1), (add_q, 2)):
        add(1)
        add(2)
        rs1[1]((g,))
    for add in (add_r, add_p, add_q):
        add(3)
    pre_done(0)

    ORDER = (2, 1, 0)
    for g in ORDER:
        rs1[2]((g,))
    for g in ORDER:
        rs1[3]((g,))
        rs2[0]((g,))
        rs2[1]((g,))
    for g in ORDER:
        rs2[2]((g,))
    for g in ORDER:
        rs2[3]((g,))
        rs3[0]((g,))
    pre_start(1)
    for g in ORDER:
        rs3[1]((g,))
        grad = (acc[4 * g + x, z, y] + r3[g, 0] + r3[g, 1] + r3[g, 2]) * (1.0 / GROUP)
        mom_new = MU * mb[0, g] + grad
        nb[g] = mom_new
        xg[4 * g + x, z, y] = (grad + MU * mom_new).astype(BF16)
        u3[0]((g,))

    def pack_rows(src, dst):
        for s in range(8):
            for g in range(3):
                dst[s, 8 * g:8 * g + 7, :] = src[g, 7 * s:7 * s + 7, :]
            for j in range(7):
                r = 8 * j + 2 * (s % 4)
                dst[s, 24 + 2 * j:26 + 2 * j, :] = src[2, r:r + 2, :]

    def post(src, dst, ssem, rsem, i):
        dx, dc = row_peers[i]
        dest = row_slot[dx, dc]
        return remote(src.at[dest], dst.at[slot], ssem.at[i], rsem.at[i], row_peer(dx, dc))

    pack_rows(nb, outp)
    pre_done(1)
    for g in range(3):
        wg[4 * g + x, z, y] = mb[1, g]
    for g in ORDER:
        u3[1]((g,))
        u2[0]((g,))
    for g in ORDER:
        u2[1]((g,))
    wg3[0]()
    for g in ORDER:
        u2[2]((g,))
        u1[0]((g,))
    for g in ORDER:
        u1[1]((g,))
    for i in range(7):
        post(outp, mrecv, mo_s, mo_r, i).start()
    mrecv[slot] = outp[slot]
    wg3[1]()
    wg2[0]()
    for g in ORDER:
        u1[2]((g,))

    def total(units):
        part = jnp.zeros((56, 128), F32)
        for u in units:
            v = xg[u].astype(F32)
            part = part + jnp.sum(v * v, axis=(0, 1))
        return 1.0 / (jnp.sqrt(jnp.sum(part, keepdims=True)) + EPS)

    def column(u, inv):
        return xg[u].astype(F32).reshape(D, 128) * inv

    inv = total(range(7))
    for u in range(7):
        xx[0, :, 128 * u:128 * u + 128] = column(u, inv).astype(BF16)

    @pl.when(core == 0)
    def _():
        inv_d = total((8, 9))
        both = [(xg[u].astype(F32) * inv_d).reshape(16, 7, 8, 128) for u in (8, 9)]
        both = jnp.concatenate(both, axis=2)
        for j in range(7):
            ss[0, 0, :, 128 * j:128 * j + 128] = both[:, j].reshape(256, 128).astype(BF16)
        v = xg[7].astype(F32)
        v = v.reshape(D, 128).T
        for i in range(2):
            h = v[64 * i:64 * i + 64]
            norm = jnp.sqrt(jnp.sum(h * h, keepdims=True))
            ss[0, 1, 64 * i:64 * i + 64, :] = (h * (1.0 / (norm + EPS))).astype(BF16)
        ss[0, 1, 128:256, :] = jnp.zeros((128, D), BF16)

    @pl.when(core == 1)
    def _():
        for i in range(2):
            inv_u = total((7 + 2 * i, 8 + 2 * i))
            for h in range(2):
                ss[0, i, 128 * h:128 * h + 128, :] = column(7 + 2 * i + h, inv_u).T.astype(BF16)

    wg2[1]()

    NT = (((1,), (1,)), ((), ()))
    ROWS = ((0, 256), (256, 256), (512, 256), (768, 128))
    row_id = lax.broadcasted_iota(jnp.int32, (256, 256), 0) // 64
    col_id = lax.broadcasted_iota(jnp.int32, (256, 256), 1) // 64
    keep = jnp.logical_or(row_id == col_id, core == 1)

    def symmetric(product, out):
        for r in (0, 256, 512):
            value = product(r, 256, r, 768 - r)
            out[r:r + 256, r:768] = value
            if r < 512:
                out[r + 256:768, r:r + 256] = value[:, 256:].T
        value = product(768, 128, 0, D)
        out[768:896, :] = value
        out[0:768, 768:896] = value[:, 0:768].T

    def step(it, carry):
        cur = lax.rem(it, 2)
        nxt = 1 - cur
        def gram(r, n, c, m):
            return lax.dot_general(xx[cur, r:r + n, :], xx[cur, c:c + m, :], NT, preferred_element_type=F32).astype(BF16)

        symmetric(gram, aa)
        for i in range(2):
            g = lax.dot_general(ss[cur, i], ss[cur, i], NT, preferred_element_type=F32)
            if i == 1:
                g = jnp.where(keep, g, 0.0)
            sa[i] = g.astype(BF16)

        @pl.when(it == 0)
        def _():
            wg2[2]()
            wg1[0]()

        @pl.when(it == 2)
        def _():
            wg1[1]()

        def poly(r, n, c, m):
            sq = jnp.dot(aa[r:r + n, :], aa[:, c:c + m], preferred_element_type=F32)
            return (COEF_B * aa[r:r + n, c:c + m].astype(F32) + COEF_C * sq).astype(BF16)

        symmetric(poly, bb)
        for i in range(2):
            sq = jnp.dot(sa[i], sa[i], preferred_element_type=F32)
            sb[i] = (COEF_B * sa[i].astype(F32) + COEF_C * sq).astype(BF16)
        for r, n in ROWS:
            prod = jnp.dot(bb[r:r + n, :], xx[cur], preferred_element_type=F32)
            xx[nxt, r:r + n, :] = (COEF_A * xx[cur, r:r + n, :].astype(F32) + prod).astype(BF16)
        for i in range(2):
            prod = jnp.dot(sb[i], ss[cur, i], preferred_element_type=F32)
            ss[nxt, i] = (COEF_A * ss[cur, i].astype(F32) + prod).astype(BF16)
        return carry

    lax.fori_loop(0, NS_STEPS, step, 0)
    fin = NS_STEPS % 2

    wg1[2]()
    wg1[3]()
    wg2[3]()
    wg3[2]()

    def update(w, v):
        return w - LR * (SCALE * v + WD * w)

    def out_copy(i, ref):
        return remote(ref, ref, or_s.at[i], or_r.at[i], partner)

    def sq_ref(p, c):
        return vb_sq.at[c, pl.ds(112 * p, 112)]

    def small_refs(c):
        return (vb_kv, vb_dn) if c == 0 else (vb_up.at[0], vb_up.at[1])

    def column_new(u, v):
        new = update(wg[u].reshape(D, 128), v)
        wg[u] = new.reshape(4, 4, 56, 128)
        return new

    @pl.when(core == 0)
    def _():
        v = ss[fin, 1, 0:128, :].astype(F32).T
        vb_kv[...] = column_new(7, v).T.astype(BF16)
        for j in range(7):
            v = ss[fin, 0, :, 128 * j:128 * j + 128].astype(F32).reshape(4, 4, 16, 128)
            lo = update(wg[8, :, :, 8 * j:8 * j + 8, :], v[:, :, 0:8])
            hi = update(wg[9, :, :, 8 * j:8 * j + 8, :], v[:, :, 8:16])
            wg[8, :, :, 8 * j:8 * j + 8, :] = lo
            wg[9, :, :, 8 * j:8 * j + 8, :] = hi
            vb_dn[:, 128 * j:128 * j + 128] = jnp.concatenate([lo, hi], axis=2).reshape(256, 128).astype(BF16)
        for i in range(2):
            out_copy(8 + i, small_refs(0)[i]).start()

    @pl.when(core == 1)
    def _():
        for i in range(2):
            for h in range(2):
                v = ss[fin, i, 128 * h:128 * h + 128, :].astype(F32).T
                vb_up[i, :, 128 * h:128 * h + 128] = column_new(7 + 2 * i + h, v).astype(BF16)
        for i in range(2):
            out_copy(8 + i, small_refs(1)[i]).start()

    for p in range(8):
        zz, yy = p // 2, 2 * (p % 2)
        v = xx[fin, 112 * p:112 * p + 112, :].astype(F32)
        for u in range(7):
            new = update(wg[u, zz, yy:yy + 2].reshape(112, 128), v[:, 128 * u:128 * u + 128])
            wg[u, zz, yy:yy + 2] = new.reshape(2, 56, 128)
            vb_sq[core, 112 * p:112 * p + 112, 128 * u:128 * u + 128] = new.astype(BF16)
        out_copy(p, sq_ref(p, core)).start()

    for g in range(3):
        nb[g] = wg[4 * g + x, z, y]
    pack_rows(nb, outw)
    for i in range(7):
        post(outw, wrecv, wo_s, wo_r, i).start()
    wrecv[slot] = outw[slot]

    for i in range(7):
        post(outp, mrecv, mo_s, mo_r, i).wait_recv()
        post(outw, wrecv, wo_s, wo_r, i).wait_recv()

    for p in range(8):
        out_copy(p, sq_ref(p, core)).wait()
    for c in range(2):
        @pl.when(core == c)
        def _():
            for i in range(2):
                out_copy(8 + i, small_refs(c)[i]).wait_send()
                out_copy(8 + i, small_refs(1 - c)[i]).wait_recv()
    for i in range(7):
        pre(0, i).wait_send()
        pre(1, i).wait_send()
        post(outp, mrecv, mo_s, mo_r, i).wait_send()
        post(outw, wrecv, wo_s, wo_r, i).wait_send()
    for k in range(4):
        for i, item in enumerate(common_items(other, k, 1)):
            par_copy(k, i, item).wait_send()
        for tc in range(2):
            @pl.when(core == 1 - tc)
            def _():
                for i, item in enumerate(special_items(tc, k, 1)):
                    par_copy(k, 2 + i, item).wait_send()
    rs1[4]()
    rs2[4]()
    rs3[2]()
    u3[2]()
    u2[3]()
    u1[3]()


def unpack_rows(slot, src, o_sq, o_kv, o_up, o_dn):
    for c in range(2):
        for xs in range(4):
            t = 2 * xs + c
            o_sq[:, c, 128 * xs:128 * xs + 128] = src[t, 0:7, :]
            if xs < 3:
                o_sq[:, c, 512 + 128 * xs:640 + 128 * xs] = src[t, 8:15, :]
    o_kv[:, 0, :] = src[6, 8:15, 0:64]
    o_kv[:, 1, :] = src[6, 8:15, 64:128]
    o_up[:, 0, 0:128] = src[7, 8:15, :]
    o_up[:, 0, 128:256] = src[1, 16:23, :]
    o_up[:, 1, 0:128] = src[3, 16:23, :]
    o_up[:, 1, 128:256] = src[5, 16:23, :]
    t = 2 * lax.div(slot, 4)
    for j in range(7):
        o_dn[0, :, 128 * j:128 * j + 128] = src[t, 24 + 2 * j:26 + 2 * j, :]


def write_out(
    mrecv, wrecv, vb_sq, vb_kv, vb_up, vb_dn,
    mo_sq, mo_kv, mo_up, mo_dn, wo_sq, wo_kv, wo_up, wo_dn, b_sq, b_kv, b_up, b_dn, sem,
):
    copies = [pltpu.make_async_copy(src, dst, sem.at[i]) for i, (src, dst) in enumerate(
        ((vb_sq, b_sq), (vb_kv, b_kv), (vb_up, b_up), (vb_dn, b_dn)))]
    for cp in copies:
        cp.start()
    me = lax.axis_index("data")
    slot = lax.rem(me, 8)
    unpack_rows(slot, mrecv, mo_sq, mo_kv, mo_up, mo_dn)
    unpack_rows(slot, wrecv, wo_sq, wo_kv, wo_up, wo_dn)
    for cp in copies:
        cp.wait()


def solution(mesh):
    grad_spec = P(("model", "data"))
    slab_spec = P("model", "data")
    full_spec = P("model")

    def local_step(g_sq, m_sq, w_sq, g_kv, m_kv, w_kv, g_up, m_up, w_up, g_dn, m_dn, w_dn):
        g_sq = g_sq.reshape(2, 4, 4, 56, 896)
        g_kv = g_kv[0].transpose(0, 2, 1)
        g_up = g_up.reshape(2, 4, 4, 56, 256)
        g_dn = g_dn.reshape(4, 4, 16, 896)
        vm = pl.BlockSpec(memory_space=pltpu.VMEM)
        hb = pl.BlockSpec(memory_space=pltpu.HBM)
        V = pltpu.VMEM
        scratch = [
            V((2, 4, 4, 4, 56, 128), F32), V((2, 4, 4, 56, 384), F32), V((2, 2, 64, 896), F32),
            V((2, 2, 4, 4, 56, 256), F32), V((2, 4, 4, 16, 896), F32), V((12, 4, 4, 56, 128), F32),
            V((6, 2, 4, 56, 128), F32), V((6, 2, 4, 56, 128), F32), V((6, 3, 2, 56, 128), F32),
            V((3, 6, 2, 56, 128), F32), V((3, 3, 56, 128), F32),
            V((2, 7, 2, 896), F32), V((2, 7, 2, 64), F32), V((2, 7, 2, 256), F32), V((2, 1, 2, 896), F32),
            V((2, 2, 4, 40, 128), F32), V((2, 8, 40, 128), F32), V((2, 3, 56, 128), F32), V((3, 56, 128), F32),
            V((8, 40, 128), F32), V((8, 40, 128), F32),
            V((12, 4, 4, 56, 128), BF16), V((12, 4, 4, 56, 128), F32),
            V((2, D, D), BF16), V((D, D), BF16), V((D, D), BF16),
            V((2, 2, 256, D), BF16), V((2, 256, 256), BF16), V((2, 256, 256), BF16),
            DMA((4, 5)), DMA((2, 4)), DMA((4, 5)), DMA((4, 5)), DMA((2, 7)), DMA((2, 7)), DMA((7,)), DMA((7,)), DMA((7,)), DMA((7,)),
            DMA((3, 6)), DMA((3, 6)), DMA((3, 6)), DMA((3, 6)), DMA((3, 3)), DMA((3, 3)),
            DMA((3, 3)), DMA((3, 3)), DMA((3, 6)), DMA((3, 6)), DMA((3, 6)), DMA((3, 6)),
            DMA((3, 3)), DMA((3, 3)), DMA((3, 6)), DMA((3, 6)), DMA((3, 6)), DMA((3, 6)),
            DMA((10,)), DMA((10,)),
        ]

        def rows(a):
            return a.transpose(1, 0, 2)

        mid = [V(s, F32) for s in ((8, 40, 128), (8, 40, 128))]
        mid += [V(s, BF16) for s in ((2, D, D), (128, D), (2, D, 256), (256, D))]
        parts = pl.pallas_call(
            kernel,
            out_shape=mid,
            in_specs=[hb] * 12,
            out_specs=[vm] * 6,
            scratch_shapes=scratch,
            compiler_params=pltpu.CompilerParams(collective_id=0, has_side_effects=True, vmem_limit_bytes=61700000),
            name="muon",
        )(g_sq, g_kv, g_up, g_dn, rows(m_sq), rows(m_kv), rows(m_up), m_dn, rows(w_sq), rows(w_kv), rows(w_up), w_dn)
        small = [jax.ShapeDtypeStruct(s, F32) for s in ((7, 2, 896), (7, 2, 64), (7, 2, 256), (1, 2, 896))]
        full = [jax.ShapeDtypeStruct(s, BF16) for s in ((2, D, D), (128, D), (2, D, 256), (256, D))]
        out = pl.pallas_call(
            write_out,
            out_shape=small + small + full,
            in_specs=[vm] * 6,
            out_specs=[vm] * 8 + [hb] * 4,
            scratch_shapes=[DMA((4,))],
            compiler_params=pltpu.CompilerParams(vmem_limit_bytes=4_000_000),
            name="write_out",
        )(*parts)
        m, w, b = out[0:4], out[4:8], out[8:12]
        return (
            rows(m[0]), rows(w[0]), b[0],
            rows(m[1]), rows(w[1]), b[1].reshape(2, 64, D).transpose(0, 2, 1),
            rows(m[2]), rows(w[2]), b[2],
            m[3], w[3], b[3].reshape(1, 256, D),
        )

    in_specs = (grad_spec, slab_spec, slab_spec) * 4
    out_specs = (slab_spec, slab_spec, full_spec) * 4
    return jax.shard_map(local_step, mesh=mesh, in_specs=in_specs, out_specs=out_specs, check_vma=False)
```

```python
import math
import jax
import jax.numpy as jnp
from jax import lax
from jax.experimental import pallas as pl
from jax.experimental.pallas import tpu as pltpu
from jax.sharding import PartitionSpec as P

NS_STEPS = 5
MU = 0.95
LR = 0.1
WD = 0.5
EPS = 1e-7
COEF_A = 3.4445
COEF_B = -4.7750
COEF_C = 2.0315
GROUP = 128
D = 896
SCALE = 0.2 * math.sqrt(896.0)
MESH = pl.DeviceIdType.MESH
F32 = jnp.float32
BF16 = jnp.bfloat16
DMA = pltpu.SemaphoreType.DMA


def kernel(
    g_sq, g_kv, g_up, g_dn,
    m_sq, m_kv, m_up, m_dn,
    w_sq, w_kv, w_up, w_dn,
    mrecv, wrecv, vb_sq, vb_kv, vb_up, vb_dn,
    br, bp, kvb, upb, dnb, acc,
    r1a, r1b, r1c, r2, r3, s3, mg, mt,
    q_sq, q_kv, q_up, q_dn,
    pieces, recvp, mb, nb, outp, outw,
    xg, wg, xx, aa, bb, ss, sa, sb,
    own_s, row_s, d2d_s, d2d_r, pre_s, pre_r, mo_s, mo_r, wo_s, wo_r,
    rs1_s, rs1_r, rs2_s, rs2_r, rs3_s, rs3_r,
    m3_s, m3_r, u2_s, u2_r, u1_s, u1_r,
    w3_s, w3_r, w2_s, w2_r, w1_s, w1_r,
    or_s, or_r,
):
    me = lax.axis_index("data")
    core = lax.rem(me, 2)
    x = lax.rem(lax.div(me, 2), 4)
    y = lax.rem(lax.div(me, 8), 4)
    z = lax.div(me, 32)
    slot = 2 * x + core
    other = 1 - core
    around = {
        "x": [x] + [lax.rem(x + d, 4) for d in (1, 2, 3)],
        "y": [y] + [lax.rem(y + d, 4) for d in (1, 2, 3)],
        "z": [z] + [lax.rem(z + d, 4) for d in (1, 2, 3)],
    }
    partner = me + other - core
    stride = {"x": 2, "y": 8, "z": 32}
    peers = {dim: [me + (a - around[dim][0]) * stride[dim] for a in around[dim]] for dim in "xyz"}
    row_x = [2 * a - 2 * x for a in around["x"]]

    def peer(dim, delta):
        return peers[dim][delta]

    def remote(src, dst, ssem, rsem, device):
        return pltpu.make_async_remote_copy(
            src_ref=src, dst_ref=dst, send_sem=ssem, recv_sem=rsem,
            device_id={"data": device}, device_id_type=MESH)

    row_peers = [(dx, dc) for dx in range(4) for dc in range(2) if (dx, dc) != (0, 0)]

    row_dev = {(dx, dc): (me, partner)[dc] + row_x[dx] for dx in range(4) for dc in range(2)}
    row_slot = {(dx, dc): 2 * around["x"][dx] + (core, other)[dc] for dx in range(4) for dc in range(2)}

    def row_peer(dx, dc):
        return row_dev[dx, dc]

    barrier = pltpu.get_barrier_semaphore()
    for dx, dc in row_peers:
        pl.semaphore_signal(barrier, inc=1, device_id={"data": row_peer(dx, dc)}, device_id_type=MESH)
    for dim in ("y", "z"):
        for delta in (1, 2, 3):
            pl.semaphore_signal(barrier, inc=1, device_id={"data": peer(dim, delta)}, device_id_type=MESH)

    OFFS = (2, 1, 3, 0)

    def lanes(j):
        return pl.ds(pl.multiple_of(j * 128, 128), 128)

    def common_items(tc, k, w):
        jx, jz = around["x"][OFFS[k]], around["z"][OFFS[k]]
        return [
            (g_sq.at[tc, :, :, :, lanes(jx)], br.at[w, jx]),
            (g_sq.at[tc, jz, :, :, pl.ds(512, 384)], bp.at[w, jz]),
        ]

    def special_items(tc, k, w):
        jz, jy = around["z"][OFFS[k]], around["y"][OFFS[k]]
        if tc == 0:
            items = [(g_dn.at[:, jy], dnb.at[w, :, jy])]
            return items + [(g_kv, kvb.at[w])] if k == 0 else items
        return [
            (g_up.at[0, jz, :, :, pl.ds(0, 128)], upb.at[w, 0, jz, :, :, pl.ds(0, 128)]),
            (g_up.at[0, :, jy, :, pl.ds(128, 128)], upb.at[w, 0, :, jy, :, pl.ds(128, 128)]),
            (g_up.at[1, :, jy], upb.at[w, 1, :, jy]),
        ]

    def own_copy(k, i, item):
        return pltpu.make_async_copy(item[0], item[1], own_s.at[k, i])

    def par_copy(k, i, item):
        return remote(item[0], item[1], d2d_s.at[k, i], d2d_r.at[k, i], partner)

    def start_own(k):
        for i, item in enumerate(common_items(core, k, 0)):
            own_copy(k, i, item).start()
        for tc in range(2):
            @pl.when(core == tc)
            def _():
                for i, item in enumerate(special_items(tc, k, 0)):
                    own_copy(k, 2 + i, item).start()

    def start_par(k):
        for i, item in enumerate(common_items(other, k, 1)):
            par_copy(k, i, item).start()
        for tc in range(2):
            @pl.when(core == 1 - tc)
            def _():
                for i, item in enumerate(special_items(tc, k, 1)):
                    par_copy(k, 2 + i, item).start()

    def arrive(k, i, own, par):
        own_copy(k, i, own).wait()
        par_copy(k, i, par).wait_recv()

    def add_r(k):
        jx = around["x"][OFFS[k]]
        arrive(k, 0, common_items(core, k, 0)[0], common_items(core, k, 1)[0])
        acc[jx] = br[0, jx] + br[1, jx]

    def add_p(k):
        jz = around["z"][OFFS[k]]
        arrive(k, 1, common_items(core, k, 0)[1], common_items(core, k, 1)[1])
        for u in range(3):
            acc[4 + u, jz] = bp[0, jz, :, :, 128 * u:128 * u + 128] + bp[1, jz, :, :, 128 * u:128 * u + 128]

        @pl.when(core == 1)
        def _():
            arrive(k, 2, special_items(1, k, 0)[0], special_items(1, k, 1)[0])
            acc[7, jz] = upb[0, 0, jz, :, :, 0:128] + upb[1, 0, jz, :, :, 0:128]

    def add_q(k):
        jy = around["y"][OFFS[k]]

        @pl.when(core == 0)
        def _():
            arrive(k, 2, special_items(0, k, 0)[0], special_items(0, k, 1)[0])
            rows = dnb[0, :, jy] + dnb[1, :, jy]
            for i in range(7):
                acc[8, :, jy, 8 * i:8 * i + 8, :] = rows[:, 0:8, 128 * i:128 * i + 128]
                acc[9, :, jy, 8 * i:8 * i + 8, :] = rows[:, 8:16, 128 * i:128 * i + 128]

        @pl.when(core == 1)
        def _():
            for i in (1, 2):
                arrive(k, 2 + i, special_items(1, k, 0)[i], special_items(1, k, 1)[i])
            acc[8, :, jy] = upb[0, 0, :, jy, :, 128:256] + upb[1, 0, :, jy, :, 128:256]
            acc[9, :, jy] = upb[0, 1, :, jy, :, 0:128] + upb[1, 1, :, jy, :, 0:128]
            acc[10, :, jy] = upb[0, 1, :, jy, :, 128:256] + upb[1, 1, :, jy, :, 128:256]

    def add_kv():
        @pl.when(core == 0)
        def _():
            own_copy(0, 3, special_items(0, 0, 0)[1]).wait()
            par_copy(0, 3, special_items(0, 0, 1)[1]).wait_recv()
            acc[7] = (kvb[0] + kvb[1]).reshape(128, D).T.reshape(4, 4, 56, 128)

    DIMS1, DIMS2, DIMS3 = ("x", "z", "y"), ("y", "x", "z"), ("z", "y", "x")

    def half1(buf, grp, j, h):
        if grp == 0:
            return buf.at[j, pl.ds(2 * h, 2)]
        if grp == 1:
            return buf.at[pl.ds(4 + 2 * h, 2), j]
        return buf.at[pl.ds(8, 3), pl.ds(2 * h, 2), j]

    def half2(buf, grp, j, h):
        if grp == 0:
            return buf.at[x, pl.ds(2 * h, 2), j]
        if grp == 1:
            return buf.at[4 + j, z, pl.ds(2 * h, 2)]
        return buf.at[pl.ds(8 + 2 * h, 2), j, y]

    def half3(buf, grp, h):
        if grp == 0:
            return buf.at[x, pl.ds(2 * h, 2), y]
        if grp == 1:
            return buf.at[4 + x, z, pl.ds(2 * h, 2)]
        return buf.at[pl.ds(8 + 2 * h, 2), z, y]

    def block(buf, grp):
        return buf.at[4 * grp + x, z, y]

    def rs_ring(half, buf, dims, rbufs, ssem, rsem):
        def desc(grp, i):
            dim = dims[grp]
            d, h = ((2, 0), (1, 1), (1, 0), (2, 1), (3, 0), (3, 1))[i]
            src = (around[dim][d], h)
            return remote(half(buf, grp, src[0], src[1]), rbufs[grp].at[i], ssem.at[grp, i], rsem.at[grp, i], peer(dim, 1 if i < 3 else 3))

        def add(grp, j, h, i):
            desc(grp, i).wait_recv()
            ref = half(buf, grp, j, h)
            ref[...] += rbufs[grp][i]

        def first(groups=(0, 1, 2)):
            for grp in groups:
                desc(grp, 0).start()
                desc(grp, 3).start()

        def second(groups=(0, 1, 2)):
            for grp in groups:
                desc(grp, 1).start()
                desc(grp, 4).start()

        def third(groups=(0, 1, 2)):
            for grp in groups:
                p = around[dims[grp]]
                add(grp, p[1], 0, 0)
                desc(grp, 2).start()
                add(grp, p[3], 1, 3)
                desc(grp, 5).start()

        def last(groups=(0, 1, 2)):
            for grp in groups:
                p = around[dims[grp]][0]
                add(grp, p, 1, 1)
                add(grp, p, 0, 4)
                add(grp, p, 0, 2)
                add(grp, p, 1, 5)

        def drain():
            for grp in range(3):
                for i in range(6):
                    desc(grp, i).wait_send()

        return first, second, third, last, drain

    def ag_ring(half, buf, dims, ssem, rsem):
        def desc(grp, i):
            dim = dims[grp]
            d, h = ((0, 0), (0, 1), (3, 0), (0, 1), (0, 0), (1, 1))[i]
            ref = half(buf, grp, around[dim][d], h)
            return remote(ref, ref, ssem.at[grp, i], rsem.at[grp, i], peer(dim, 1 if i < 3 else 3))

        def first(groups=(0, 1, 2)):
            for grp in groups:
                for i in (0, 3, 1, 4):
                    desc(grp, i).start()

        def second(groups=(0, 1, 2)):
            for grp in groups:
                desc(grp, 0).wait_recv()
                desc(grp, 2).start()
                desc(grp, 3).wait_recv()
                desc(grp, 5).start()

        def last(groups=(0, 1, 2)):
            for grp in groups:
                for i in (1, 4, 2, 5):
                    desc(grp, i).wait_recv()

        def drain():
            for grp in range(3):
                for i in range(6):
                    desc(grp, i).wait_send()

        return first, second, last, drain

    swap = {}
    for d in "xyz":
        p = around[d][0]
        swap[d] = (me + (1 - 2 * lax.rem(p, 2)) * stride[d], me + (3 - 2 * p) * stride[d])

    def sum_pairs():
        def desc(grp, st, h):
            src = half3(acc, grp, h) if st == 0 else s3.at[grp, h]
            return remote(src, r3.at[grp, st, h], rs3_s.at[grp, 2 * st + h], rs3_r.at[grp, 2 * st + h], swap[DIMS3[grp]][(st + h) % 2])

        def first(groups=(0, 1, 2)):
            for grp in groups:
                for h in range(2):
                    desc(grp, 0, h).start()

        def second(groups=(0, 1, 2)):
            for grp in groups:
                for h in range(2):
                    desc(grp, 0, h).wait_recv()
                    s3[grp, h] = half3(acc, grp, h)[...] + r3[grp, 0, h]
                    desc(grp, 1, h).start()

        def last(grp, h):
            desc(grp, 1, h).wait_recv()
            return s3[grp, h] + r3[grp, 1, h]

        def drain():
            for grp in range(3):
                for i in range(4):
                    desc(grp, i // 2, i % 2).wait_send()

        return first, second, last, drain

    def ag_direct(buf, ssem, rsem):
        def desc(grp, i):
            delta = (2, 1, 3)[i]
            ref = block(buf, grp)
            return remote(ref, ref, ssem.at[grp, i], rsem.at[grp, i], peer(DIMS3[grp], delta))

        def first(groups=(0, 1, 2)):
            for i in range(3):
                for grp in groups:
                    desc(grp, i).start()

        def last(groups=(0, 1, 2)):
            for grp in groups:
                for i in range(3):
                    desc(grp, i).wait_recv()

        def drain():
            for grp in range(3):
                for i in range(3):
                    desc(grp, i).wait_send()

        return first, last, drain

    rs1 = rs_ring(half1, acc, DIMS1, (r1a, r1b, r1c), rs1_s, rs1_r)
    rs2 = rs_ring(half2, acc, DIMS2, (r2.at[0], r2.at[1], r2.at[2]), rs2_s, rs2_r)
    rs3 = sum_pairs()
    m3 = ag_direct(mg, m3_s, m3_r)
    u2 = ag_ring(half2, xg, DIMS2, u2_s, u2_r)
    u1 = ag_ring(half1, xg, DIMS1, u1_s, u1_r)
    wg3 = ag_direct(wg, w3_s, w3_r)
    wg2 = ag_ring(half2, wg, DIMS2, w2_s, w2_r)
    wg1 = ag_ring(half1, wg, DIMS1, w1_s, w1_r)

    for k in range(4):
        start_own(k)

    def row_copies():
        pairs = ((m_sq, w_sq, q_sq), (m_kv, w_kv, q_kv), (m_up, w_up, q_up), (m_dn, w_dn, q_dn))
        return [pltpu.make_async_copy(src[a], src[2].at[a], row_s.at[a, i]) for i, src in enumerate(pairs) for a in range(2)]

    for cp in row_copies():
        cp.start()

    def pack_pieces():
        for cp in row_copies():
            cp.wait()
        for a in range(2):
            for c in range(2):
                for xd in range(4):
                    pieces[a, c, xd, 0:7, :] = q_sq[a, :, c, 128 * xd:128 * xd + 128]
                    if xd < 3:
                        pieces[a, c, xd, 8:15, :] = q_sq[a, :, c, 512 + 128 * xd:640 + 128 * xd]
            pieces[a, 0, 3, 8:15, 0:64] = q_kv[a, :, 0, :]
            pieces[a, 0, 3, 8:15, 64:128] = q_kv[a, :, 1, :]
            pieces[a, 1, 3, 8:15, :] = q_up[a, :, 0, 0:128]
            pieces[a, 1, 0, 16:23, :] = q_up[a, :, 0, 128:256]
            pieces[a, 1, 1, 16:23, :] = q_up[a, :, 1, 0:128]
            pieces[a, 1, 2, 16:23, :] = q_up[a, :, 1, 128:256]
            for xd in range(2):
                for j in range(7):
                    pieces[a, 0, xd, 24 + 2 * j:26 + 2 * j, :] = q_dn[a, 0, :, 128 * j:128 * j + 128]

    acc[11] = jnp.zeros((4, 4, 56, 128), F32)

    @pl.when(core == 0)
    def _():
        acc[10] = jnp.zeros((4, 4, 56, 128), F32)

    pack_pieces()
    pl.semaphore_wait(barrier, 13)

    for k in range(4):
        start_par(k)

    def pre(a, i):
        dx, dc = row_peers[i]
        return remote(pieces.at[a, (core, other)[dc], around["x"][dx]], recvp.at[a, slot], pre_s.at[a, i], pre_r.at[a, i], row_peer(dx, dc))

    def pre_start(a):
        for i in range(7):
            pre(a, i).start()
        recvp[a, slot] = pieces[a, core, x]

    def pre_done(a):
        for i in range(7):
            pre(a, i).wait_recv()
        for g in range(3):
            for s in range(8):
                mb[a, g, 7 * s:7 * s + 7, :] = recvp[a, s, 8 * g:8 * g + 7, :]

        @pl.when(jnp.logical_and(core == 0, x < 2))
        def _():
            for i in range(4):
                for j in range(7):
                    mb[a, 2, 8 * j + 2 * i:8 * j + 2 * i + 2, :] = recvp[a, 4 * x + i, 24 + 2 * j:26 + 2 * j, :]

    pre_start(0)
    add_r(0)
    rs1[0]((0,))
    add_q(0)
    rs1[0]((2,))
    add_p(0)
    add_kv()
    rs1[0]((1,))
    for add, g in ((add_r, 0), (add_p, 1), (add_q, 2)):
        add(1)
        add(2)
        rs1[1]((g,))
    for add in (add_r, add_p, add_q):
        add(3)
    pre_done(0)

    ORDER = (2, 1, 0)
    for g in ORDER:
        rs1[2]((g,))
    for g in ORDER:
        rs1[3]((g,))
        rs2[0]((g,))
        rs2[1]((g,))
    for g in ORDER:
        rs2[2]((g,))
    for g in range(3):
        mg[4 * g + x, z, y] = mb[0, g]
    m3[0]()
    for g in ORDER:
        rs2[3]((g,))
        rs3[0]((g,))
    pre_start(1)
    for g in ORDER:
        rs3[1]((g,))
    m3[1]()
    for g in ORDER:
        for h in range(2):
            grad = rs3[2](g, h) * (1.0 / GROUP)
            mom_new = MU * half3(mg, g, h)[...] + grad
            mt[g, 2 * h:2 * h + 2] = mom_new
            half3(xg, g, h)[...] = (grad + MU * mom_new).astype(BF16)
        u2[0]((g,))
    for g in range(3):
        nb[g] = mt[g, around[DIMS3[g]][0]]

    def pack_rows(src, dst):
        for s in range(8):
            for g in range(3):
                dst[s, 8 * g:8 * g + 7, :] = src[g, 7 * s:7 * s + 7, :]
            for j in range(7):
                r = 8 * j + 2 * (s % 4)
                dst[s, 24 + 2 * j:26 + 2 * j, :] = src[2, r:r + 2, :]

    def post(src, dst, ssem, rsem, i):
        dx, dc = row_peers[i]
        dest = row_slot[dx, dc]
        return remote(src.at[dest], dst.at[slot], ssem.at[i], rsem.at[i], row_peer(dx, dc))

    for g in ORDER:
        u2[1]((g,))
    pre_done(1)
    for g in range(3):
        wg[4 * g + x, z, y] = mb[1, g]
    wg3[0]()
    for g in ORDER:
        u2[2]((g,))
        u1[0]((g,))
    pack_rows(nb, outp)
    for g in ORDER:
        u1[1]((g,))
    for i in range(7):
        post(outp, mrecv, mo_s, mo_r, i).start()
    mrecv[slot] = outp[slot]
    wg3[1]()
    wg2[0]()
    for g in ORDER:
        u1[2]((g,))

    def total(units):
        part = jnp.zeros((56, 128), F32)
        for u in units:
            v = xg[u].astype(F32)
            part = part + jnp.sum(v * v, axis=(0, 1))
        return 1.0 / (jnp.sqrt(jnp.sum(part, keepdims=True)) + EPS)

    def column(u, inv):
        return xg[u].astype(F32).reshape(D, 128) * inv

    inv = total(range(7))
    for u in range(7):
        xx[0, :, 128 * u:128 * u + 128] = column(u, inv).astype(BF16)

    @pl.when(core == 0)
    def _():
        inv_d = total((8, 9))
        both = [(xg[u].astype(F32) * inv_d).reshape(16, 7, 8, 128) for u in (8, 9)]
        both = jnp.concatenate(both, axis=2)
        for j in range(7):
            ss[0, 0, :, 128 * j:128 * j + 128] = both[:, j].reshape(256, 128).astype(BF16)
        v = xg[7].astype(F32)
        v = v.reshape(D, 128).T
        for i in range(2):
            h = v[64 * i:64 * i + 64]
            norm = jnp.sqrt(jnp.sum(h * h, keepdims=True))
            ss[0, 1, 64 * i:64 * i + 64, :] = (h * (1.0 / (norm + EPS))).astype(BF16)
        ss[0, 1, 128:256, :] = jnp.zeros((128, D), BF16)

    @pl.when(core == 1)
    def _():
        for i in range(2):
            inv_u = total((7 + 2 * i, 8 + 2 * i))
            for h in range(2):
                ss[0, i, 128 * h:128 * h + 128, :] = column(7 + 2 * i + h, inv_u).T.astype(BF16)

    wg2[1]()

    NT = (((1,), (1,)), ((), ()))
    ROWS = ((0, 256), (256, 256), (512, 256), (768, 128))
    row_id = lax.broadcasted_iota(jnp.int32, (256, 256), 0) // 64
    col_id = lax.broadcasted_iota(jnp.int32, (256, 256), 1) // 64
    keep = jnp.logical_or(row_id == col_id, core == 1)

    def symmetric(product, out):
        for r in (0, 256, 512):
            value = product(r, 256, r, 768 - r)
            out[r:r + 256, r:768] = value
            if r < 512:
                out[r + 256:768, r:r + 256] = value[:, 256:].T
        value = product(768, 128, 0, D)
        out[768:896, :] = value
        out[0:768, 768:896] = value[:, 0:768].T

    def poly_step(cur, it):
        def gram(r, n, c, m):
            return lax.dot_general(xx[cur, r:r + n, :], xx[cur, c:c + m, :], NT, preferred_element_type=F32).astype(BF16)

        symmetric(gram, aa)
        for i in range(2):
            g = lax.dot_general(ss[cur, i], ss[cur, i], NT, preferred_element_type=F32)
            if i == 1:
                g = jnp.where(keep, g, 0.0)
            sa[i] = g.astype(BF16)

        if it == 0:
            wg2[2]()
            wg1[0]()
        if it == 2:
            wg1[1]()

        def poly(r, n, c, m):
            sq = jnp.dot(aa[r:r + n, :], aa[:, c:c + m], preferred_element_type=F32)
            return (COEF_B * aa[r:r + n, c:c + m].astype(F32) + COEF_C * sq).astype(BF16)

        symmetric(poly, bb)
        for i in range(2):
            sq = jnp.dot(sa[i], sa[i], preferred_element_type=F32)
            sb[i] = (COEF_B * sa[i].astype(F32) + COEF_C * sq).astype(BF16)

    def apply_small(cur, nxt):
        for i in range(2):
            prod = jnp.dot(sb[i], ss[cur, i], preferred_element_type=F32)
            ss[nxt, i] = (COEF_A * ss[cur, i].astype(F32) + prod).astype(BF16)

    def apply_rows(cur, r, n):
        prod = jnp.dot(bb[pl.ds(r, n), :], xx[cur], preferred_element_type=F32)
        return (COEF_A * xx[cur, pl.ds(r, n), :].astype(F32) + prod).astype(BF16)

    def step(it, carry):
        cur = it % 2
        nxt = 1 - cur
        poly_step(cur, it)
        for r, n in ROWS:
            xx[nxt, r:r + n, :] = apply_rows(cur, r, n)
        apply_small(cur, nxt)
        return carry

    for it in range(NS_STEPS - 1):
        step(it, 0)
    cur = (NS_STEPS - 1) % 2
    fin = 1 - cur
    poly_step(cur, None)
    apply_small(cur, fin)

    wg1[2]()
    wg1[3]()
    wg2[3]()
    wg3[2]()

    def update(w, v):
        return w - LR * (SCALE * v + WD * w)

    def out_copy(i, ref):
        return remote(ref, ref, or_s.at[i], or_r.at[i], partner)

    def sq_ref(p, c):
        return vb_sq.at[c, pl.ds(pl.multiple_of(224 * p, 32), 224)]

    def small_refs(c):
        return (vb_kv, vb_dn) if c == 0 else (vb_up.at[0], vb_up.at[1])

    def column_new(u, v):
        new = update(wg[u].reshape(D, 128), v)
        wg[u] = new.reshape(4, 4, 56, 128)
        return new

    @pl.when(core == 0)
    def _():
        v = ss[fin, 1, 0:128, :].astype(F32).T
        vb_kv[...] = column_new(7, v).T.astype(BF16)
        for j in range(7):
            v = ss[fin, 0, :, 128 * j:128 * j + 128].astype(F32).reshape(4, 4, 16, 128)
            lo = update(wg[8, :, :, 8 * j:8 * j + 8, :], v[:, :, 0:8])
            hi = update(wg[9, :, :, 8 * j:8 * j + 8, :], v[:, :, 8:16])
            wg[8, :, :, 8 * j:8 * j + 8, :] = lo
            wg[9, :, :, 8 * j:8 * j + 8, :] = hi
            vb_dn[:, 128 * j:128 * j + 128] = jnp.concatenate([lo, hi], axis=2).reshape(256, 128).astype(BF16)
        for i in range(2):
            out_copy(8 + i, small_refs(0)[i]).start()

    @pl.when(core == 1)
    def _():
        for i in range(2):
            for h in range(2):
                v = ss[fin, i, 128 * h:128 * h + 128, :].astype(F32).T
                vb_up[i, :, 128 * h:128 * h + 128] = column_new(7 + 2 * i + h, v).astype(BF16)
        for i in range(2):
            out_copy(8 + i, small_refs(1)[i]).start()

    for i in range(4):
        q = around["z"][i]
        v = apply_rows(cur, pl.multiple_of(224 * q, 32), 224).astype(F32)
        for u in range(7):
            new = update(wg[u, q].reshape(224, 128), v[:, 128 * u:128 * u + 128])
            wg[u, q] = new.reshape(4, 56, 128)
            vb_sq[core, pl.ds(pl.multiple_of(224 * q, 32), 224), 128 * u:128 * u + 128] = new.astype(BF16)
        out_copy(i, sq_ref(q, core)).start()
        if i == 0:
            for g in range(3):
                nb[g] = wg[4 * g + x, z, y]
            pack_rows(nb, outw)
            for k in range(7):
                post(outw, wrecv, wo_s, wo_r, k).start()
            wrecv[slot] = outw[slot]

    for i in range(7):
        post(outp, mrecv, mo_s, mo_r, i).wait_recv()
        post(outw, wrecv, wo_s, wo_r, i).wait_recv()

    for p in range(4):
        out_copy(p, sq_ref(around["z"][p], core)).wait()
    for c in range(2):
        @pl.when(core == c)
        def _():
            for i in range(2):
                out_copy(8 + i, small_refs(c)[i]).wait_send()
                out_copy(8 + i, small_refs(1 - c)[i]).wait_recv()
    for i in range(7):
        pre(0, i).wait_send()
        pre(1, i).wait_send()
        post(outp, mrecv, mo_s, mo_r, i).wait_send()
        post(outw, wrecv, wo_s, wo_r, i).wait_send()
    for k in range(4):
        for i, item in enumerate(common_items(other, k, 1)):
            par_copy(k, i, item).wait_send()
        for tc in range(2):
            @pl.when(core == 1 - tc)
            def _():
                for i, item in enumerate(special_items(tc, k, 1)):
                    par_copy(k, 2 + i, item).wait_send()
    rs1[4]()
    rs2[4]()
    rs3[3]()
    m3[2]()
    u2[3]()
    u1[3]()


def unpack_rows(slot, src, o_sq, o_kv, o_up, o_dn):
    for c in range(2):
        for xs in range(4):
            t = 2 * xs + c
            o_sq[:, c, 128 * xs:128 * xs + 128] = src[t, 0:7, :]
            if xs < 3:
                o_sq[:, c, 512 + 128 * xs:640 + 128 * xs] = src[t, 8:15, :]
    o_kv[:, 0, :] = src[6, 8:15, 0:64]
    o_kv[:, 1, :] = src[6, 8:15, 64:128]
    o_up[:, 0, 0:128] = src[7, 8:15, :]
    o_up[:, 0, 128:256] = src[1, 16:23, :]
    o_up[:, 1, 0:128] = src[3, 16:23, :]
    o_up[:, 1, 128:256] = src[5, 16:23, :]
    t = 2 * lax.div(slot, 4)
    for j in range(7):
        o_dn[0, :, 128 * j:128 * j + 128] = src[t, 24 + 2 * j:26 + 2 * j, :]


def write_out(
    mrecv, wrecv, vb_sq, vb_kv, vb_up, vb_dn,
    mo_sq, mo_kv, mo_up, mo_dn, wo_sq, wo_kv, wo_up, wo_dn, b_sq, b_kv, b_up, b_dn, sem,
):
    copies = [pltpu.make_async_copy(src, dst, sem.at[i]) for i, (src, dst) in enumerate(
        ((vb_sq, b_sq), (vb_kv, b_kv), (vb_up, b_up), (vb_dn, b_dn)))]
    for cp in copies:
        cp.start()
    me = lax.axis_index("data")
    slot = lax.rem(me, 8)
    unpack_rows(slot, mrecv, mo_sq, mo_kv, mo_up, mo_dn)
    unpack_rows(slot, wrecv, wo_sq, wo_kv, wo_up, wo_dn)
    for cp in copies:
        cp.wait()


def solution(mesh):
    grad_spec = P(("model", "data"))
    slab_spec = P("model", "data")
    full_spec = P("model")

    def local_step(g_sq, m_sq, w_sq, g_kv, m_kv, w_kv, g_up, m_up, w_up, g_dn, m_dn, w_dn):
        g_sq = g_sq.reshape(2, 4, 4, 56, 896)
        g_kv = g_kv[0].transpose(0, 2, 1)
        g_up = g_up.reshape(2, 4, 4, 56, 256)
        g_dn = g_dn.reshape(4, 4, 16, 896)
        vm = pl.BlockSpec(memory_space=pltpu.VMEM)
        hb = pl.BlockSpec(memory_space=pltpu.HBM)
        V = pltpu.VMEM
        scratch = [
            V((2, 4, 4, 4, 56, 128), F32), V((2, 4, 4, 56, 384), F32), V((2, 2, 64, 896), F32),
            V((2, 2, 4, 4, 56, 256), F32), V((2, 4, 4, 16, 896), F32), V((12, 4, 4, 56, 128), F32),
            V((6, 2, 4, 56, 128), F32), V((6, 2, 4, 56, 128), F32), V((6, 3, 2, 56, 128), F32),
            V((3, 6, 2, 56, 128), F32), V((3, 2, 2, 2, 56, 128), F32), V((3, 2, 2, 56, 128), F32),
            V((12, 4, 4, 56, 128), F32), V((3, 4, 56, 128), F32),
            V((2, 7, 2, 896), F32), V((2, 7, 2, 64), F32), V((2, 7, 2, 256), F32), V((2, 1, 2, 896), F32),
            V((2, 2, 4, 40, 128), F32), V((2, 8, 40, 128), F32), V((2, 3, 56, 128), F32), V((3, 56, 128), F32),
            V((8, 40, 128), F32), V((8, 40, 128), F32),
            V((12, 4, 4, 56, 128), BF16), V((12, 4, 4, 56, 128), F32),
            V((2, D, D), BF16), V((D, D), BF16), V((D, D), BF16),
            V((2, 2, 256, D), BF16), V((2, 256, 256), BF16), V((2, 256, 256), BF16),
            DMA((4, 5)), DMA((2, 4)), DMA((4, 5)), DMA((4, 5)), DMA((2, 7)), DMA((2, 7)), DMA((7,)), DMA((7,)), DMA((7,)), DMA((7,)),
            DMA((3, 6)), DMA((3, 6)), DMA((3, 6)), DMA((3, 6)), DMA((3, 4)), DMA((3, 4)),
            DMA((3, 3)), DMA((3, 3)), DMA((3, 6)), DMA((3, 6)), DMA((3, 6)), DMA((3, 6)),
            DMA((3, 3)), DMA((3, 3)), DMA((3, 6)), DMA((3, 6)), DMA((3, 6)), DMA((3, 6)),
            DMA((10,)), DMA((10,)),
        ]

        def rows(a):
            return a.transpose(1, 0, 2)

        mid = [V(s, F32) for s in ((8, 40, 128), (8, 40, 128))]
        mid += [V(s, BF16) for s in ((2, D, D), (128, D), (2, D, 256), (256, D))]
        parts = pl.pallas_call(
            kernel,
            out_shape=mid,
            in_specs=[hb] * 12,
            out_specs=[vm] * 6,
            scratch_shapes=scratch,
            compiler_params=pltpu.CompilerParams(collective_id=0, has_side_effects=True, vmem_limit_bytes=61700000),
            name="muon",
        )(g_sq, g_kv, g_up, g_dn, rows(m_sq), rows(m_kv), rows(m_up), m_dn, rows(w_sq), rows(w_kv), rows(w_up), w_dn)
        small = [jax.ShapeDtypeStruct(s, F32) for s in ((7, 2, 896), (7, 2, 64), (7, 2, 256), (1, 2, 896))]
        full = [jax.ShapeDtypeStruct(s, BF16) for s in ((2, D, D), (128, D), (2, D, 256), (256, D))]
        out = pl.pallas_call(
            write_out,
            out_shape=small + small + full,
            in_specs=[vm] * 6,
            out_specs=[vm] * 8 + [hb] * 4,
            scratch_shapes=[DMA((4,))],
            compiler_params=pltpu.CompilerParams(vmem_limit_bytes=4_000_000),
            name="write_out",
        )(*parts)
        m, w, b = out[0:4], out[4:8], out[8:12]
        return (
            rows(m[0]), rows(w[0]), b[0],
            rows(m[1]), rows(w[1]), b[1].reshape(2, 64, D).transpose(0, 2, 1),
            rows(m[2]), rows(w[2]), b[2],
            m[3], w[3], b[3].reshape(1, 256, D),
        )

    in_specs = (grad_spec, slab_spec, slab_spec) * 4
    out_specs = (slab_spec, slab_spec, full_spec) * 4
    return jax.shard_map(local_step, mesh=mesh, in_specs=in_specs, out_specs=out_specs, check_vma=False)
```

```python
import math
import jax
import jax.numpy as jnp
from jax import lax
from jax.experimental import pallas as pl
from jax.experimental.pallas import tpu as pltpu
from jax.sharding import PartitionSpec as P

NS_STEPS = 5
MU = 0.95
LR = 0.1
WD = 0.5
EPS = 1e-7
COEF_A = 3.4445
COEF_B = -4.7750
COEF_C = 2.0315
GROUP = 128
D = 896
SCALE = 0.2 * math.sqrt(896.0)
GROUPS = 3
PAIR = 2
ALL = tuple(range(GROUPS))
RING = 4
HOPS = 6
SLAB = 7
SUB = 8
UNITS = 12
PEERS = 13
P_END = 15
TILE16 = 16
Q_END = 23
DOWN_AT = 24
DOWN_NEXT = 26
ALIGN = 32
PACK = 40
BROWS = 56
KVD = 64
LANES = 128
QROWS = 224
FF = 256
TRIO = 384
HALF_D = 512
P_AT = 640
TAIL_D = 768
PACKED = (SUB, PACK, LANES)
MESH = pl.DeviceIdType.MESH
F32 = jnp.float32
BF16 = jnp.bfloat16
DMA = pltpu.SemaphoreType.DMA


def kernel(
    g_sq, g_kv, g_up, g_dn,
    m_sq, m_kv, m_up, m_dn,
    w_sq, w_kv, w_up, w_dn,
    mrecv, wrecv, vb_sq, vb_kv, vb_up, vb_dn,
    br, bp, kvb, upb, dnb, acc,
    r1a, r1b, r1c, r2, r3, s3, mg, mt,
    q_sq, q_kv, q_up, q_dn,
    pieces, recvp, mb, nb, outp, outw,
    xg, wg, xx, aa, bb, ss, sa, sb,
    own_s, row_s, d2d_s, d2d_r, pre_s, pre_r, mo_s, mo_r, wo_s, wo_r,
    rs1_s, rs1_r, rs2_s, rs2_r, rs3_s, rs3_r,
    m3_s, m3_r, u2_s, u2_r, u1_s, u1_r,
    w3_s, w3_r, w2_s, w2_r, w1_s, w1_r,
    or_s, or_r,
):
    me = lax.axis_index("data")
    core = lax.rem(me, 2)
    x = lax.rem(lax.div(me, 2), RING)
    y = lax.rem(lax.div(me, SUB), RING)
    z = lax.div(me, ALIGN)
    slot = 2 * x + core
    other = 1 - core
    around = {
        "x": [x] + [lax.rem(x + d, RING) for d in (1, 2, 3)],
        "y": [y] + [lax.rem(y + d, RING) for d in (1, 2, 3)],
        "z": [z] + [lax.rem(z + d, RING) for d in (1, 2, 3)],
    }
    partner = me + other - core
    stride = {"x": 2, "y": SUB, "z": ALIGN}
    peers = {dim: [me + (a - around[dim][0]) * stride[dim] for a in around[dim]] for dim in "xyz"}
    row_x = [2 * a - 2 * x for a in around["x"]]

    def peer(dim, delta):
        return peers[dim][delta]

    def remote(src, dst, ssem, rsem, device):
        return pltpu.make_async_remote_copy(
            src_ref=src, dst_ref=dst, send_sem=ssem, recv_sem=rsem,
            device_id={"data": device}, device_id_type=MESH)

    row_peers = [(dx, dc) for dx in range(RING) for dc in range(PAIR) if (dx, dc) != (0, 0)]

    row_dev = {(dx, dc): (me, partner)[dc] + row_x[dx] for dx in range(RING) for dc in range(PAIR)}
    row_slot = {(dx, dc): 2 * around["x"][dx] + (core, other)[dc] for dx in range(RING) for dc in range(PAIR)}

    def row_peer(dx, dc):
        return row_dev[dx, dc]

    barrier = pltpu.get_barrier_semaphore()
    for dx, dc in row_peers:
        pl.semaphore_signal(barrier, inc=1, device_id={"data": row_peer(dx, dc)}, device_id_type=MESH)
    for dim in ("y", "z"):
        for delta in (1, 2, 3):
            pl.semaphore_signal(barrier, inc=1, device_id={"data": peer(dim, delta)}, device_id_type=MESH)

    OFFS = (2, 1, 3, 0)

    def lanes(j):
        return pl.ds(pl.multiple_of(j * LANES, LANES), LANES)

    def common_items(tc, k, w):
        jx, jz = around["x"][OFFS[k]], around["z"][OFFS[k]]
        return [
            (g_sq.at[tc, :, :, :, lanes(jx)], br.at[w, jx]),
            (g_sq.at[tc, jz, :, :, pl.ds(HALF_D, TRIO)], bp.at[w, jz]),
        ]

    def special_items(tc, k, w):
        jz, jy = around["z"][OFFS[k]], around["y"][OFFS[k]]
        if tc == 0:
            items = [(g_dn.at[:, jy], dnb.at[w, :, jy])]
            return items + [(g_kv, kvb.at[w])] if k == 0 else items
        return [
            (g_up.at[0, jz, :, :, pl.ds(0, LANES)], upb.at[w, 0, jz, :, :, pl.ds(0, LANES)]),
            (g_up.at[0, :, jy, :, pl.ds(LANES, LANES)], upb.at[w, 0, :, jy, :, pl.ds(LANES, LANES)]),
            (g_up.at[1, :, jy], upb.at[w, 1, :, jy]),
        ]

    def own_copy(k, i, item):
        return pltpu.make_async_copy(item[0], item[1], own_s.at[k, i])

    def par_copy(k, i, item):
        return remote(item[0], item[1], d2d_s.at[k, i], d2d_r.at[k, i], partner)

    def start_own(k):
        for i, item in enumerate(common_items(core, k, 0)):
            own_copy(k, i, item).start()
        for tc in range(PAIR):
            @pl.when(core == tc)
            def _():
                for i, item in enumerate(special_items(tc, k, 0)):
                    own_copy(k, 2 + i, item).start()

    def start_par(k):
        for i, item in enumerate(common_items(other, k, 1)):
            par_copy(k, i, item).start()
        for tc in range(PAIR):
            @pl.when(core == 1 - tc)
            def _():
                for i, item in enumerate(special_items(tc, k, 1)):
                    par_copy(k, 2 + i, item).start()

    def common(k, w):
        return common_items(core, k, w)

    def down_kv(k, w):
        return special_items(0, k, w)

    def ups(k, w):
        return special_items(1, k, w)

    def arrive(k, i, items, at):
        own_copy(k, i, items(k, 0)[at]).wait()
        par_copy(k, i, items(k, 1)[at]).wait_recv()

    def add_r(k):
        jx = around["x"][OFFS[k]]
        arrive(k, 0, common, 0)
        acc[jx] = br[0, jx] + br[1, jx]

    def add_p(k):
        jz = around["z"][OFFS[k]]
        arrive(k, 1, common, 1)
        for u in range(GROUPS):
            acc[RING + u, jz] = bp[0, jz, :, :, LANES * u:LANES * u + LANES] + bp[1, jz, :, :, LANES * u:LANES * u + LANES]

        @pl.when(core == 1)
        def _():
            arrive(k, PAIR, ups, 0)
            acc[SLAB, jz] = upb[0, 0, jz, :, :, :LANES] + upb[1, 0, jz, :, :, :LANES]

    def add_q(k):
        jy = around["y"][OFFS[k]]

        @pl.when(core == 0)
        def _():
            arrive(k, PAIR, down_kv, 0)
            rows = dnb[0, :, jy] + dnb[1, :, jy]
            for i in range(SLAB):
                acc[SUB, :, jy, SUB * i:SUB * i + SUB, :] = rows[:, :SUB, LANES * i:LANES * i + LANES]
                acc[9, :, jy, SUB * i:SUB * i + SUB, :] = rows[:, SUB:TILE16, LANES * i:LANES * i + LANES]

        @pl.when(core == 1)
        def _():
            for i in (1, 2):
                arrive(k, PAIR + i, ups, i)
            acc[SUB, :, jy] = upb[0, 0, :, jy, :, LANES:FF] + upb[1, 0, :, jy, :, LANES:FF]
            acc[9, :, jy] = upb[0, 1, :, jy, :, :LANES] + upb[1, 1, :, jy, :, :LANES]
            acc[10, :, jy] = upb[0, 1, :, jy, :, LANES:FF] + upb[1, 1, :, jy, :, LANES:FF]

    def add_kv():
        @pl.when(core == 0)
        def _():
            arrive(0, GROUPS, down_kv, 1)
            acc[SLAB] = (kvb[0] + kvb[1]).reshape(LANES, D).T.reshape(RING, RING, BROWS, LANES)

    DIMS1, DIMS2, DIMS3 = ("x", "z", "y"), ("y", "x", "z"), ("z", "y", "x")

    def half1(buf, grp, j, h):
        if grp == 0:
            return buf.at[j, pl.ds(PAIR * h, PAIR)]
        if grp == 1:
            return buf.at[pl.ds(RING + PAIR * h, PAIR), j]
        return buf.at[pl.ds(SUB, 3), pl.ds(PAIR * h, PAIR), j]

    def half2(buf, grp, j, h):
        if grp == 0:
            return buf.at[x, pl.ds(PAIR * h, PAIR), j]
        if grp == 1:
            return buf.at[RING + j, z, pl.ds(PAIR * h, PAIR)]
        return buf.at[pl.ds(SUB + PAIR * h, PAIR), j, y]

    def half3(buf, grp, h):
        if grp == 0:
            return buf.at[x, pl.ds(PAIR * h, PAIR), y]
        if grp == 1:
            return buf.at[RING + x, z, pl.ds(PAIR * h, PAIR)]
        return buf.at[pl.ds(SUB + PAIR * h, PAIR), z, y]

    def block(buf, grp):
        return buf.at[RING * grp + x, z, y]

    def rs_ring(half, buf, dims, rbufs, ssem, rsem):
        def desc(grp, i):
            dim = dims[grp]
            d, h = ((2, 0), (1, 1), (1, 0), (2, 1), (3, 0), (3, 1))[i]
            src = (around[dim][d], h)
            return remote(half(buf, grp, src[0], src[1]), rbufs[grp].at[i], ssem.at[grp, i], rsem.at[grp, i], peer(dim, 1 if i < GROUPS else GROUPS))

        def add(grp, j, h, i):
            desc(grp, i).wait_recv()
            ref = half(buf, grp, j, h)
            ref[...] += rbufs[grp][i]

        def first(groups=ALL):
            for grp in groups:
                desc(grp, 0).start()
                desc(grp, 3).start()

        def second(groups=ALL):
            for grp in groups:
                desc(grp, 1).start()
                desc(grp, RING).start()

        def third(groups=ALL):
            for grp in groups:
                p = around[dims[grp]]
                add(grp, p[1], 0, 0)
                desc(grp, 2).start()
                add(grp, p[3], 1, 3)
                desc(grp, 5).start()

        def last(groups=ALL):
            for grp in groups:
                p = around[dims[grp]][0]
                add(grp, p, 1, 1)
                add(grp, p, 0, RING)
                add(grp, p, 0, 2)
                add(grp, p, 1, 5)

        def drain():
            for grp in range(GROUPS):
                for i in range(HOPS):
                    desc(grp, i).wait_send()

        return first, second, third, last, drain

    def ag_ring(half, buf, dims, ssem, rsem):
        def desc(grp, i):
            dim = dims[grp]
            d, h = ((0, 0), (0, 1), (3, 0), (0, 1), (0, 0), (1, 1))[i]
            ref = half(buf, grp, around[dim][d], h)
            return remote(ref, ref, ssem.at[grp, i], rsem.at[grp, i], peer(dim, 1 if i < GROUPS else GROUPS))

        def first(groups=ALL):
            for grp in groups:
                for i in (0, 3, 1, RING):
                    desc(grp, i).start()

        def second(groups=ALL):
            for grp in groups:
                desc(grp, 0).wait_recv()
                desc(grp, 2).start()
                desc(grp, 3).wait_recv()
                desc(grp, 5).start()

        def last(groups=ALL):
            for grp in groups:
                for i in (1, RING, 2, 5):
                    desc(grp, i).wait_recv()

        def drain():
            for grp in range(GROUPS):
                for i in range(HOPS):
                    desc(grp, i).wait_send()

        return first, second, last, drain

    swap = {}
    for d in "xyz":
        p = around[d][0]
        swap[d] = (me + (1 - 2 * lax.rem(p, 2)) * stride[d], me + (3 - 2 * p) * stride[d])

    def sum_pairs():
        def desc(grp, st, h):
            src = half3(acc, grp, h) if st == 0 else s3.at[grp, h]
            return remote(src, r3.at[grp, st, h], rs3_s.at[grp, 2 * st + h], rs3_r.at[grp, 2 * st + h], swap[DIMS3[grp]][(st + h) % 2])

        def first(groups=ALL):
            for grp in groups:
                for h in range(PAIR):
                    desc(grp, 0, h).start()

        def second(groups=ALL):
            for grp in groups:
                for h in range(PAIR):
                    desc(grp, 0, h).wait_recv()
                    s3[grp, h] = half3(acc, grp, h)[...] + r3[grp, 0, h]
                    desc(grp, 1, h).start()

        def last(grp, h):
            desc(grp, 1, h).wait_recv()
            return s3[grp, h] + r3[grp, 1, h]

        def drain():
            for grp in range(GROUPS):
                for i in range(RING):
                    desc(grp, i // 2, i % 2).wait_send()

        return first, second, last, drain

    def ag_direct(buf, ssem, rsem):
        def desc(grp, i):
            delta = (2, 1, 3)[i]
            ref = block(buf, grp)
            return remote(ref, ref, ssem.at[grp, i], rsem.at[grp, i], peer(DIMS3[grp], delta))

        def first(groups=ALL):
            for i in range(GROUPS):
                for grp in groups:
                    desc(grp, i).start()

        def last(groups=ALL):
            for grp in groups:
                for i in range(GROUPS):
                    desc(grp, i).wait_recv()

        def drain():
            for grp in range(GROUPS):
                for i in range(GROUPS):
                    desc(grp, i).wait_send()

        return first, last, drain

    rs1 = rs_ring(half1, acc, DIMS1, (r1a, r1b, r1c), rs1_s, rs1_r)
    rs2 = rs_ring(half2, acc, DIMS2, (r2.at[0], r2.at[1], r2.at[2]), rs2_s, rs2_r)
    rs3 = sum_pairs()
    m3 = ag_direct(mg, m3_s, m3_r)
    u2 = ag_ring(half2, xg, DIMS2, u2_s, u2_r)
    u1 = ag_ring(half1, xg, DIMS1, u1_s, u1_r)
    wg3 = ag_direct(wg, w3_s, w3_r)
    wg2 = ag_ring(half2, wg, DIMS2, w2_s, w2_r)
    wg1 = ag_ring(half1, wg, DIMS1, w1_s, w1_r)

    for k in range(RING):
        start_own(k)

    def row_copies():
        pairs = ((m_sq, w_sq, q_sq), (m_kv, w_kv, q_kv), (m_up, w_up, q_up), (m_dn, w_dn, q_dn))
        return [pltpu.make_async_copy(src[a], src[2].at[a], row_s.at[a, i]) for i, src in enumerate(pairs) for a in range(PAIR)]

    for cp in row_copies():
        cp.start()

    def pack_pieces():
        for cp in row_copies():
            cp.wait()
        for a in range(PAIR):
            for c in range(PAIR):
                for xd in range(RING):
                    pieces[a, c, xd, :SLAB, :] = q_sq[a, :, c, LANES * xd:LANES * xd + LANES]
                    if xd < 3:
                        pieces[a, c, xd, SUB:P_END, :] = q_sq[a, :, c, HALF_D + LANES * xd:P_AT + LANES * xd]
            pieces[a, 0, 3, SUB:P_END, :KVD] = q_kv[a, :, 0, :]
            pieces[a, 0, 3, SUB:P_END, KVD:LANES] = q_kv[a, :, 1, :]
            pieces[a, 1, 3, SUB:P_END, :] = q_up[a, :, 0, :LANES]
            pieces[a, 1, 0, TILE16:Q_END, :] = q_up[a, :, 0, LANES:FF]
            pieces[a, 1, 1, TILE16:Q_END, :] = q_up[a, :, 1, :LANES]
            pieces[a, 1, 2, TILE16:Q_END, :] = q_up[a, :, 1, LANES:FF]
            for xd in range(PAIR):
                for j in range(SLAB):
                    pieces[a, 0, xd, DOWN_AT + PAIR * j:DOWN_NEXT + PAIR * j, :] = q_dn[a, 0, :, LANES * j:LANES * j + LANES]

    acc[11] = jnp.zeros((RING, RING, BROWS, LANES), F32)

    @pl.when(core == 0)
    def _():
        acc[10] = jnp.zeros((RING, RING, BROWS, LANES), F32)

    pack_pieces()
    pl.semaphore_wait(barrier, PEERS)

    for k in range(RING):
        start_par(k)

    def pre(a, i):
        dx, dc = row_peers[i]
        return remote(pieces.at[a, (core, other)[dc], around["x"][dx]], recvp.at[a, slot], pre_s.at[a, i], pre_r.at[a, i], row_peer(dx, dc))

    def pre_start(a):
        for i in range(SLAB):
            pre(a, i).start()
        recvp[a, slot] = pieces[a, core, x]

    def pre_done(a):
        for i in range(SLAB):
            pre(a, i).wait_recv()
        for g in range(GROUPS):
            for s in range(SUB):
                mb[a, g, SLAB * s:SLAB * s + SLAB, :] = recvp[a, s, SUB * g:SUB * g + SLAB, :]

        @pl.when(jnp.logical_and(core == 0, x < 2))
        def _():
            for i in range(RING):
                for j in range(SLAB):
                    mb[a, 2, SUB * j + 2 * i:SUB * j + 2 * i + 2, :] = recvp[a, RING * x + i, DOWN_AT + PAIR * j:DOWN_NEXT + PAIR * j, :]

    pre_start(0)
    add_r(0)
    rs1[0]((0,))
    add_q(0)
    rs1[0]((2,))
    add_p(0)
    add_kv()
    rs1[0]((1,))
    for add, g in ((add_r, 0), (add_p, 1), (add_q, 2)):
        add(1)
        add(2)
        rs1[1]((g,))
    for add in (add_r, add_p, add_q):
        add(3)
    pre_done(0)

    ORDER = (2, 1, 0)
    for g in ORDER:
        rs1[2]((g,))
    for g in ORDER:
        rs1[3]((g,))
        rs2[0]((g,))
        rs2[1]((g,))
    for g in ORDER:
        rs2[2]((g,))
    for g in range(GROUPS):
        mg[RING * g + x, z, y] = mb[0, g]
    m3[0]()
    for g in ORDER:
        rs2[3]((g,))
        rs3[0]((g,))
    pre_start(1)
    for g in ORDER:
        rs3[1]((g,))
    m3[1]()
    for g in ORDER:
        for h in range(PAIR):
            grad = rs3[2](g, h) * (1.0 / GROUP)
            mom_new = MU * half3(mg, g, h)[...] + grad
            mt[g, 2 * h:2 * h + 2] = mom_new
            half3(xg, g, h)[...] = (grad + MU * mom_new).astype(BF16)
        u2[0]((g,))
    for g in range(GROUPS):
        nb[g] = mt[g, around[DIMS3[g]][0]]

    def pack_rows(src, dst):
        for s in range(SUB):
            for g in range(GROUPS):
                dst[s, SUB * g:SUB * g + SLAB, :] = src[g, SLAB * s:SLAB * s + SLAB, :]
            for j in range(SLAB):
                r = SUB * j + 2 * (s % RING)
                dst[s, DOWN_AT + PAIR * j:DOWN_NEXT + PAIR * j, :] = src[2, r:r + 2, :]

    def post(src, dst, ssem, rsem, i):
        dx, dc = row_peers[i]
        dest = row_slot[dx, dc]
        return remote(src.at[dest], dst.at[slot], ssem.at[i], rsem.at[i], row_peer(dx, dc))

    for g in ORDER:
        u2[1]((g,))
    pre_done(1)
    for g in range(GROUPS):
        wg[RING * g + x, z, y] = mb[1, g]
    wg3[0]()
    for g in ORDER:
        u2[2]((g,))
        u1[0]((g,))
    pack_rows(nb, outp)
    for g in ORDER:
        u1[1]((g,))
    for i in range(SLAB):
        post(outp, mrecv, mo_s, mo_r, i).start()
    mrecv[slot] = outp[slot]
    wg3[1]()
    wg2[0]()
    for g in ORDER:
        u1[2]((g,))

    def total(units):
        part = jnp.zeros((BROWS, LANES), F32)
        for u in units:
            v = xg[u].astype(F32)
            part = part + jnp.sum(v * v, axis=(0, 1))
        return 1.0 / (jnp.sqrt(jnp.sum(part, keepdims=True)) + EPS)

    def column(u, inv):
        return xg[u].astype(F32).reshape(D, LANES) * inv

    inv = total(range(SLAB))
    for u in range(SLAB):
        xx[0, :, LANES * u:LANES * u + LANES] = column(u, inv).astype(BF16)

    @pl.when(core == 0)
    def _():
        inv_d = total((SUB, 9))
        both = [(xg[u].astype(F32) * inv_d).reshape(TILE16, SLAB, SUB, LANES) for u in (SUB, 9)]
        both = jnp.concatenate(both, axis=2)
        for j in range(SLAB):
            ss[0, 0, :, LANES * j:LANES * j + LANES] = both[:, j].reshape(FF, LANES).astype(BF16)
        v = xg[SLAB].astype(F32)
        v = v.reshape(D, LANES).T
        for i in range(PAIR):
            h = v[KVD * i:KVD * i + KVD]
            norm = jnp.sqrt(jnp.sum(h * h, keepdims=True))
            ss[0, 1, KVD * i:KVD * i + KVD, :] = (h * (1.0 / (norm + EPS))).astype(BF16)
        ss[0, 1, LANES:FF, :] = jnp.zeros((LANES, D), BF16)

    @pl.when(core == 1)
    def _():
        for i in range(PAIR):
            inv_u = total((SLAB + 2 * i, SUB + 2 * i))
            for h in range(PAIR):
                ss[0, i, LANES * h:LANES * h + LANES, :] = column(SLAB + 2 * i + h, inv_u).T.astype(BF16)

    wg2[1]()

    NT = (((1,), (1,)), ((), ()))
    ROWS = ((0, FF), (FF, FF), (HALF_D, FF), (TAIL_D, LANES))
    row_id = lax.broadcasted_iota(jnp.int32, (FF, FF), 0) // KVD
    col_id = lax.broadcasted_iota(jnp.int32, (FF, FF), 1) // KVD
    keep = jnp.logical_or(row_id == col_id, core == 1)

    def symmetric(product, out):
        for r in (0, FF, HALF_D):
            value = product(r, FF, r, TAIL_D - r)
            out[r:r + FF, r:TAIL_D] = value
            if r < HALF_D:
                out[r + FF:TAIL_D, r:r + FF] = value[:, FF:].T
        value = product(TAIL_D, LANES, 0, D)
        out[TAIL_D:D, :] = value
        out[:TAIL_D, TAIL_D:D] = value[:, :TAIL_D].T

    def poly_step(cur, it):
        def gram(r, n, c, m):
            return lax.dot_general(xx[cur, r:r + n, :], xx[cur, c:c + m, :], NT, preferred_element_type=F32).astype(BF16)

        symmetric(gram, aa)
        for i in range(PAIR):
            g = lax.dot_general(ss[cur, i], ss[cur, i], NT, preferred_element_type=F32)
            if i == 1:
                g = jnp.where(keep, g, 0.0)
            sa[i] = g.astype(BF16)

        if it == 0:
            wg2[2]()
            wg1[0]()
        if it == 2:
            wg1[1]()

        def poly(r, n, c, m):
            sq = jnp.dot(aa[r:r + n, :], aa[:, c:c + m], preferred_element_type=F32)
            return (COEF_B * aa[r:r + n, c:c + m].astype(F32) + COEF_C * sq).astype(BF16)

        symmetric(poly, bb)
        for i in range(PAIR):
            sq = jnp.dot(sa[i], sa[i], preferred_element_type=F32)
            sb[i] = (COEF_B * sa[i].astype(F32) + COEF_C * sq).astype(BF16)

    def apply_small(cur, nxt):
        for i in range(PAIR):
            prod = jnp.dot(sb[i], ss[cur, i], preferred_element_type=F32)
            ss[nxt, i] = (COEF_A * ss[cur, i].astype(F32) + prod).astype(BF16)

    def apply_rows(cur, r, n):
        prod = jnp.dot(bb[pl.ds(r, n), :], xx[cur], preferred_element_type=F32)
        return (COEF_A * xx[cur, pl.ds(r, n), :].astype(F32) + prod).astype(BF16)

    def step(it, carry):
        cur = it % 2
        nxt = 1 - cur
        poly_step(cur, it)
        for r, n in ROWS:
            xx[nxt, r:r + n, :] = apply_rows(cur, r, n)
        apply_small(cur, nxt)
        return carry

    for it in range(NS_STEPS - 1):
        step(it, 0)
    cur = (NS_STEPS - 1) % 2
    fin = 1 - cur
    poly_step(cur, None)
    apply_small(cur, fin)

    wg1[2]()
    wg1[3]()
    wg2[3]()
    wg3[2]()

    def update(w, v):
        return w - LR * (SCALE * v + WD * w)

    def out_copy(i, ref):
        return remote(ref, ref, or_s.at[i], or_r.at[i], partner)

    def sq_ref(p, c):
        return vb_sq.at[c, pl.ds(pl.multiple_of(QROWS * p, ALIGN), QROWS)]

    def small_refs(c):
        return (vb_kv, vb_dn) if c == 0 else (vb_up.at[0], vb_up.at[1])

    def column_new(u, v):
        new = update(wg[u].reshape(D, LANES), v)
        wg[u] = new.reshape(RING, RING, BROWS, LANES)
        return new

    @pl.when(core == 0)
    def _():
        v = ss[fin, 1, :LANES, :].astype(F32).T
        vb_kv[...] = column_new(SLAB, v).T.astype(BF16)
        for j in range(SLAB):
            v = ss[fin, 0, :, LANES * j:LANES * j + LANES].astype(F32).reshape(RING, RING, TILE16, LANES)
            lo = update(wg[SUB, :, :, SUB * j:SUB * j + SUB, :], v[:, :, :SUB])
            hi = update(wg[9, :, :, SUB * j:SUB * j + SUB, :], v[:, :, SUB:TILE16])
            wg[SUB, :, :, SUB * j:SUB * j + SUB, :] = lo
            wg[9, :, :, SUB * j:SUB * j + SUB, :] = hi
            vb_dn[:, LANES * j:LANES * j + LANES] = jnp.concatenate([lo, hi], axis=2).reshape(FF, LANES).astype(BF16)
        for i in range(PAIR):
            out_copy(SUB + i, small_refs(0)[i]).start()

    @pl.when(core == 1)
    def _():
        for i in range(PAIR):
            for h in range(PAIR):
                v = ss[fin, i, LANES * h:LANES * h + LANES, :].astype(F32).T
                vb_up[i, :, LANES * h:LANES * h + LANES] = column_new(SLAB + 2 * i + h, v).astype(BF16)
        for i in range(PAIR):
            out_copy(SUB + i, small_refs(1)[i]).start()

    for i in range(RING):
        q = around["z"][i]
        v = apply_rows(cur, pl.multiple_of(QROWS * q, ALIGN), QROWS).astype(F32)
        for u in range(SLAB):
            new = update(wg[u, q].reshape(QROWS, LANES), v[:, LANES * u:LANES * u + LANES])
            wg[u, q] = new.reshape(RING, BROWS, LANES)
            vb_sq[core, pl.ds(pl.multiple_of(QROWS * q, ALIGN), QROWS), LANES * u:LANES * u + LANES] = new.astype(BF16)
        out_copy(i, sq_ref(q, core)).start()
        if i == 0:
            for g in range(GROUPS):
                nb[g] = wg[RING * g + x, z, y]
            pack_rows(nb, outw)
            for k in range(SLAB):
                post(outw, wrecv, wo_s, wo_r, k).start()
            wrecv[slot] = outw[slot]

    for i in range(SLAB):
        post(outp, mrecv, mo_s, mo_r, i).wait_recv()
        post(outw, wrecv, wo_s, wo_r, i).wait_recv()

    for p in range(RING):
        out_copy(p, sq_ref(around["z"][p], core)).wait()
    for c in range(PAIR):
        @pl.when(core == c)
        def _():
            for i in range(PAIR):
                out_copy(SUB + i, small_refs(c)[i]).wait_send()
                out_copy(SUB + i, small_refs(1 - c)[i]).wait_recv()
    for i in range(SLAB):
        pre(0, i).wait_send()
        pre(1, i).wait_send()
        post(outp, mrecv, mo_s, mo_r, i).wait_send()
        post(outw, wrecv, wo_s, wo_r, i).wait_send()
    for k in range(RING):
        for i, item in enumerate(common_items(other, k, 1)):
            par_copy(k, i, item).wait_send()
        for tc in range(PAIR):
            @pl.when(core == 1 - tc)
            def _():
                for i, item in enumerate(special_items(tc, k, 1)):
                    par_copy(k, 2 + i, item).wait_send()
    rs1[RING]()
    rs2[RING]()
    rs3[3]()
    m3[2]()
    u2[3]()
    u1[3]()


def unpack_rows(slot, src, o_sq, o_kv, o_up, o_dn):
    for c in range(PAIR):
        for xs in range(RING):
            t = 2 * xs + c
            o_sq[:, c, LANES * xs:LANES * xs + LANES] = src[t, :SLAB, :]
            if xs < 3:
                o_sq[:, c, HALF_D + LANES * xs:P_AT + LANES * xs] = src[t, SUB:P_END, :]
    o_kv[:, 0, :] = src[HOPS, SUB:P_END, :KVD]
    o_kv[:, 1, :] = src[HOPS, SUB:P_END, KVD:LANES]
    o_up[:, 0, :LANES] = src[SLAB, SUB:P_END, :]
    o_up[:, 0, LANES:FF] = src[1, TILE16:Q_END, :]
    o_up[:, 1, :LANES] = src[3, TILE16:Q_END, :]
    o_up[:, 1, LANES:FF] = src[5, TILE16:Q_END, :]
    t = 2 * lax.div(slot, RING)
    for j in range(SLAB):
        o_dn[0, :, LANES * j:LANES * j + LANES] = src[t, DOWN_AT + PAIR * j:DOWN_NEXT + PAIR * j, :]


def write_out(
    mrecv, wrecv, vb_sq, vb_kv, vb_up, vb_dn,
    mo_sq, mo_kv, mo_up, mo_dn, wo_sq, wo_kv, wo_up, wo_dn, b_sq, b_kv, b_up, b_dn, sem,
):
    copies = [pltpu.make_async_copy(src, dst, sem.at[i]) for i, (src, dst) in enumerate(
        ((vb_sq, b_sq), (vb_kv, b_kv), (vb_up, b_up), (vb_dn, b_dn)))]
    for cp in copies:
        cp.start()
    me = lax.axis_index("data")
    slot = lax.rem(me, SUB)
    unpack_rows(slot, mrecv, mo_sq, mo_kv, mo_up, mo_dn)
    unpack_rows(slot, wrecv, wo_sq, wo_kv, wo_up, wo_dn)
    for cp in copies:
        cp.wait()


def solution(mesh):
    grad_spec = P(("model", "data"))
    slab_spec = P("model", "data")
    full_spec = P("model")

    def local_step(g_sq, m_sq, w_sq, g_kv, m_kv, w_kv, g_up, m_up, w_up, g_dn, m_dn, w_dn):
        g_sq = g_sq.reshape(2, RING, RING, BROWS, D)
        g_kv = g_kv[0].transpose(0, 2, 1)
        g_up = g_up.reshape(2, RING, RING, BROWS, FF)
        g_dn = g_dn.reshape(RING, RING, TILE16, D)
        vm = pl.BlockSpec(memory_space=pltpu.VMEM)
        hb = pl.BlockSpec(memory_space=pltpu.HBM)
        V = pltpu.VMEM
        block = (BROWS, LANES)
        unit = (RING, RING) + block
        half = (PAIR, RING) + block
        two = (PAIR,) + block
        mats = (PAIR, PAIR)
        rows_of = (PAIR, SLAB, PAIR)
        floats = [
            (PAIR, RING) + unit, (PAIR, RING, RING, BROWS, TRIO), mats + (KVD, D), mats + (RING, RING, BROWS, FF), (PAIR, RING, RING, TILE16, D), (UNITS,) + unit,
            (HOPS,) + half, (HOPS,) + half, (HOPS, GROUPS) + two, (GROUPS, HOPS) + two, (GROUPS,) + mats + two, (GROUPS, PAIR) + two,
            (UNITS,) + unit, (GROUPS, RING) + block,
            rows_of + (D,), rows_of + (KVD,), rows_of + (FF,), (2, 1, 2, D),
            mats + (RING, PACK, LANES), (PAIR, SUB, PACK, LANES), (PAIR, GROUPS) + block, (GROUPS,) + block, PACKED, PACKED,
        ]
        scratch = [V(a, F32) for a in floats] + [V((UNITS,) + unit, BF16), V((UNITS,) + unit, F32)]
        scratch += [V(a, BF16) for a in ((PAIR, D, D), (D, D), (D, D), mats + (FF, D), (PAIR, FF, FF), (PAIR, FF, FF))]
        ring, pairs, direct, row = (GROUPS, HOPS), (GROUPS, RING), (GROUPS, GROUPS), (SLAB,)
        sems = [(RING, 5), (2, RING)]
        for a in ((RING, 5), (PAIR,) + row, row, row, ring, ring, pairs, direct, ring, ring, direct, ring, ring, (10,)):
            sems += [a, a]
        scratch += [DMA(a) for a in sems]

        def rows(a):
            return a.transpose(1, 0, 2)

        mid = [V(s, F32) for s in (PACKED, PACKED)]
        mid += [V(s, BF16) for s in ((2, D, D), (LANES, D), (2, D, FF), (FF, D))]
        parts = pl.pallas_call(
            kernel,
            out_shape=mid,
            in_specs=[hb] * UNITS,
            out_specs=[vm] * HOPS,
            scratch_shapes=scratch,
            compiler_params=pltpu.CompilerParams(collective_id=0, has_side_effects=True, vmem_limit_bytes=61700000),
            name="muon",
        )(g_sq, g_kv, g_up, g_dn, rows(m_sq), rows(m_kv), rows(m_up), m_dn, rows(w_sq), rows(w_kv), rows(w_up), w_dn)
        small = [jax.ShapeDtypeStruct(s, F32) for s in ((SLAB, PAIR, D), (SLAB, PAIR, KVD), (SLAB, PAIR, FF), (1, PAIR, D))]
        full = [jax.ShapeDtypeStruct(s, BF16) for s in ((2, D, D), (LANES, D), (2, D, FF), (FF, D))]
        out = pl.pallas_call(
            write_out,
            out_shape=small + small + full,
            in_specs=[vm] * HOPS,
            out_specs=[vm] * SUB + [hb] * RING,
            scratch_shapes=[DMA((RING,))],
            compiler_params=pltpu.CompilerParams(vmem_limit_bytes=4_000_000),
            name="write_out",
        )(*parts)
        m, w, b = out[0:RING], out[RING:SUB], out[SUB:UNITS]
        return (
            rows(m[0]), rows(w[0]), b[0],
            rows(m[1]), rows(w[1]), b[1].reshape(2, KVD, D).transpose(0, 2, 1),
            rows(m[2]), rows(w[2]), b[2],
            m[3], w[3], b[3].reshape(1, FF, D),
        )

    in_specs = (grad_spec, slab_spec, slab_spec) * RING
    out_specs = (slab_spec, slab_spec, full_spec) * RING
    return jax.shard_map(local_step, mesh=mesh, in_specs=in_specs, out_specs=out_specs, check_vma=False)
```

```python
import math
import jax
import jax.numpy as jnp
from jax import lax
from jax.experimental import pallas as pl
from jax.experimental.pallas import tpu as pltpu
from jax.sharding import PartitionSpec as P

NS_STEPS = 5
MU = 0.95
LR = 0.1
WD = 0.5
EPS = 1e-7
COEF_A = 3.4445
COEF_B = -4.7750
COEF_C = 2.0315
GROUP = 128
D = 896
SCALE = 0.2 * math.sqrt(896.0)
GROUPS = 3
PAIR = 2
ALL = tuple(range(GROUPS))
RING = 4
HOPS = 6
SLAB = 7
SUB = 8
UNITS = 12
PEERS = 13
P_END = 15
TILE16 = 16
Q_END = 23
DOWN_AT = 24
DOWN_NEXT = 26
ALIGN = 32
PACK = 40
BROWS = 56
KVD = 64
LANES = 128
QROWS = 224
FF = 256
TRIO = 384
HALF_D = 512
P_AT = 640
TAIL_D = 768
PACKED = (SUB, PACK, LANES)
MESH = pl.DeviceIdType.MESH
F32 = jnp.float32
BF16 = jnp.bfloat16
DMA = pltpu.SemaphoreType.DMA


def kernel(
    g_sq, g_kv, g_up, g_dn,
    m_sq, m_kv, m_up, m_dn,
    w_sq, w_kv, w_up, w_dn,
    mrecv, wrecv, vb_sq, vb_kv, vb_up, vb_dn,
    br, bp, kvb, upb, dnb, acc,
    r1, r2, r3, s3, mg, mt,
    q_sq, q_kv, q_up, q_dn,
    pieces, recvp, mb, nb, outp, outw,
    xg, wg, xx, aa, bb, ss, sa, sb,
    own_s, row_s, d2d_s, d2d_r, pre_s, pre_r, mo_s, mo_r, wo_s, wo_r,
    rs1_s, rs1_r, rs2_s, rs2_r, rs3_s, rs3_r,
    m3_s, m3_r, u2_s, u2_r, u1_s, u1_r,
    w3_s, w3_r, w2_s, w2_r, w1_s, w1_r,
    or_s, or_r,
):
    me = lax.axis_index("data")
    core = lax.rem(me, 2)
    x = lax.rem(lax.div(me, 2), RING)
    y = lax.rem(lax.div(me, SUB), RING)
    z = lax.div(me, ALIGN)
    slot = 2 * x + core
    other = 1 - core
    around = {
        "x": [x] + [lax.rem(x + d, RING) for d in (1, 2, 3)],
        "y": [y] + [lax.rem(y + d, RING) for d in (1, 2, 3)],
        "z": [z] + [lax.rem(z + d, RING) for d in (1, 2, 3)],
    }
    partner = me + other - core
    stride = {"x": 2, "y": SUB, "z": ALIGN}
    peers = {dim: [me + (a - around[dim][0]) * stride[dim] for a in around[dim]] for dim in "xyz"}
    row_x = [2 * a - 2 * x for a in around["x"]]

    def peer(dim, delta):
        return peers[dim][delta]

    def remote(src, dst, ssem, rsem, device):
        return pltpu.make_async_remote_copy(
            src_ref=src, dst_ref=dst, send_sem=ssem, recv_sem=rsem,
            device_id={"data": device}, device_id_type=MESH)

    row_peers = [(dx, dc) for dx in range(RING) for dc in range(PAIR) if (dx, dc) != (0, 0)]

    row_dev = {(dx, dc): (me, partner)[dc] + row_x[dx] for dx in range(RING) for dc in range(PAIR)}
    row_slot = {(dx, dc): 2 * around["x"][dx] + (core, other)[dc] for dx in range(RING) for dc in range(PAIR)}

    def row_peer(dx, dc):
        return row_dev[dx, dc]

    barrier = pltpu.get_barrier_semaphore()
    for dx, dc in row_peers:
        pl.semaphore_signal(barrier, inc=1, device_id={"data": row_peer(dx, dc)}, device_id_type=MESH)
    for dim in ("y", "z"):
        for delta in (1, 2, 3):
            pl.semaphore_signal(barrier, inc=1, device_id={"data": peer(dim, delta)}, device_id_type=MESH)

    OFFS = (2, 1, 3, 0)

    def lanes(j):
        return pl.ds(pl.multiple_of(j * LANES, LANES), LANES)

    def common_items(tc, k, w):
        jx, jz = around["x"][OFFS[k]], around["z"][OFFS[k]]
        return [
            (g_sq.at[tc, :, :, :, lanes(jx)], br.at[w, jx]),
            (g_sq.at[tc, jz, :, :, pl.ds(HALF_D, TRIO)], bp.at[w, jz]),
        ]

    def special_items(tc, k, w):
        jz, jy = around["z"][OFFS[k]], around["y"][OFFS[k]]
        if tc == 0:
            items = [(g_dn.at[:, jy], dnb.at[w, :, jy])]
            return items + [(g_kv, kvb.at[w])] if k == 0 else items
        return [
            (g_up.at[0, jz, :, :, pl.ds(0, LANES)], upb.at[w, 0, jz, :, :, pl.ds(0, LANES)]),
            (g_up.at[0, :, jy, :, pl.ds(LANES, LANES)], upb.at[w, 0, :, jy, :, pl.ds(LANES, LANES)]),
            (g_up.at[1, :, jy], upb.at[w, 1, :, jy]),
        ]

    def own_copy(k, i, item):
        return pltpu.make_async_copy(item[0], item[1], own_s.at[k, i])

    def par_copy(k, i, item):
        return remote(item[0], item[1], d2d_s.at[k, i], d2d_r.at[k, i], partner)

    def start_own(k):
        for i, item in enumerate(common_items(core, k, 0)):
            own_copy(k, i, item).start()
        for tc in range(PAIR):
            @pl.when(core == tc)
            def _():
                for i, item in enumerate(special_items(tc, k, 0)):
                    own_copy(k, 2 + i, item).start()

    def start_par(k):
        for i, item in enumerate(common_items(other, k, 1)):
            par_copy(k, i, item).start()
        for tc in range(PAIR):
            @pl.when(core == 1 - tc)
            def _():
                for i, item in enumerate(special_items(tc, k, 1)):
                    par_copy(k, 2 + i, item).start()

    def common(k, w):
        return common_items(core, k, w)

    def down_kv(k, w):
        return special_items(0, k, w)

    def ups(k, w):
        return special_items(1, k, w)

    def arrive(k, i, items, at):
        own_copy(k, i, items(k, 0)[at]).wait()
        par_copy(k, i, items(k, 1)[at]).wait_recv()

    def add_r(k):
        jx = around["x"][OFFS[k]]
        arrive(k, 0, common, 0)
        acc[jx] = br[0, jx] + br[1, jx]

    def add_p(k):
        jz = around["z"][OFFS[k]]
        arrive(k, 1, common, 1)
        for u in range(GROUPS):
            acc[RING + u, jz] = bp[0, jz, :, :, LANES * u:LANES * u + LANES] + bp[1, jz, :, :, LANES * u:LANES * u + LANES]

        @pl.when(core == 1)
        def _():
            arrive(k, PAIR, ups, 0)
            acc[SLAB, jz] = upb[0, 0, jz, :, :, :LANES] + upb[1, 0, jz, :, :, :LANES]

    def add_q(k):
        jy = around["y"][OFFS[k]]

        @pl.when(core == 0)
        def _():
            arrive(k, PAIR, down_kv, 0)
            rows = dnb[0, :, jy] + dnb[1, :, jy]
            for i in range(SLAB):
                acc[SUB, :, jy, SUB * i:SUB * i + SUB, :] = rows[:, :SUB, LANES * i:LANES * i + LANES]
                acc[9, :, jy, SUB * i:SUB * i + SUB, :] = rows[:, SUB:TILE16, LANES * i:LANES * i + LANES]

        @pl.when(core == 1)
        def _():
            for i in (1, 2):
                arrive(k, PAIR + i, ups, i)
            acc[SUB, :, jy] = upb[0, 0, :, jy, :, LANES:FF] + upb[1, 0, :, jy, :, LANES:FF]
            acc[9, :, jy] = upb[0, 1, :, jy, :, :LANES] + upb[1, 1, :, jy, :, :LANES]
            acc[10, :, jy] = upb[0, 1, :, jy, :, LANES:FF] + upb[1, 1, :, jy, :, LANES:FF]

    def add_kv():
        @pl.when(core == 0)
        def _():
            arrive(0, GROUPS, down_kv, 1)
            acc[SLAB] = (kvb[0] + kvb[1]).reshape(LANES, D).T.reshape(RING, RING, BROWS, LANES)

    DIMS1, DIMS2, DIMS3 = ("x", "z", "y"), ("y", "x", "z"), ("z", "y", "x")

    def half1(buf, grp, j, h):
        if grp == 0:
            return buf.at[j, pl.ds(PAIR * h, PAIR)]
        if grp == 1:
            return buf.at[pl.ds(RING + PAIR * h, PAIR), j]
        return buf.at[pl.ds(SUB, 3), pl.ds(PAIR * h, PAIR), j]

    def half2(buf, grp, j, h):
        if grp == 0:
            return buf.at[x, pl.ds(PAIR * h, PAIR), j]
        if grp == 1:
            return buf.at[RING + j, z, pl.ds(PAIR * h, PAIR)]
        return buf.at[pl.ds(SUB + PAIR * h, PAIR), j, y]

    def piece(d2):
        def half(buf, grp, j1, h):
            j2 = around[DIMS2[grp]][d2]
            if grp == 0:
                return buf.at[j1, pl.ds(PAIR * h, PAIR), j2]
            if grp == 1:
                return buf.at[RING + j2, j1, pl.ds(PAIR * h, PAIR)]
            return buf.at[pl.ds(SUB + PAIR * h, PAIR), j2, j1]

        return half

    def half3(buf, grp, h):
        if grp == 0:
            return buf.at[x, pl.ds(PAIR * h, PAIR), y]
        if grp == 1:
            return buf.at[RING + x, z, pl.ds(PAIR * h, PAIR)]
        return buf.at[pl.ds(SUB + PAIR * h, PAIR), z, y]

    def block(buf, grp):
        return buf.at[RING * grp + x, z, y]

    def rs_ring(half, buf, dims, rbufs, ssem, rsem):
        def desc(grp, i):
            dim = dims[grp]
            d, h = ((2, 0), (1, 1), (1, 0), (2, 1), (3, 0), (3, 1))[i]
            src = (around[dim][d], h)
            return remote(half(buf, grp, src[0], src[1]), rbufs[grp].at[i], ssem.at[grp, i], rsem.at[grp, i], peer(dim, 1 if i < GROUPS else GROUPS))

        def add(grp, j, h, i):
            desc(grp, i).wait_recv()
            ref = half(buf, grp, j, h)
            ref[...] += rbufs[grp][i]

        def first(groups=ALL):
            for grp in groups:
                desc(grp, 0).start()
                desc(grp, 3).start()

        def second(groups=ALL):
            for grp in groups:
                desc(grp, 1).start()
                desc(grp, RING).start()

        def third(groups=ALL):
            for grp in groups:
                p = around[dims[grp]]
                add(grp, p[1], 0, 0)
                desc(grp, 2).start()
                add(grp, p[3], 1, 3)
                desc(grp, 5).start()

        def last(groups=ALL):
            for grp in groups:
                p = around[dims[grp]][0]
                add(grp, p, 1, 1)
                add(grp, p, 0, RING)
                add(grp, p, 0, 2)
                add(grp, p, 1, 5)

        def drain():
            for grp in range(GROUPS):
                for i in range(HOPS):
                    desc(grp, i).wait_send()

        return first, second, third, last, drain

    def ag_ring(half, buf, dims, ssem, rsem):
        def desc(grp, i):
            dim = dims[grp]
            d, h = ((0, 0), (0, 1), (3, 0), (0, 1), (0, 0), (1, 1))[i]
            ref = half(buf, grp, around[dim][d], h)
            return remote(ref, ref, ssem.at[grp, i], rsem.at[grp, i], peer(dim, 1 if i < GROUPS else GROUPS))

        def first(groups=ALL):
            for grp in groups:
                for i in (0, 3, 1, RING):
                    desc(grp, i).start()

        def second(groups=ALL):
            for grp in groups:
                desc(grp, 0).wait_recv()
                desc(grp, 2).start()
                desc(grp, 3).wait_recv()
                desc(grp, 5).start()

        def arrived(grp, which):
            for i in which:
                desc(grp, i).wait_recv()

        def last(groups=ALL):
            for grp in groups:
                arrived(grp, (1, RING, PAIR, 5))

        def drain():
            for grp in range(GROUPS):
                for i in range(HOPS):
                    desc(grp, i).wait_send()

        return first, second, last, drain, arrived

    swap = {}
    for d in "xyz":
        p = around[d][0]
        swap[d] = (me + (1 - 2 * lax.rem(p, 2)) * stride[d], me + (3 - 2 * p) * stride[d])

    def sum_pairs():
        def desc(grp, st, h):
            src = half3(acc, grp, h) if st == 0 else s3.at[grp, h]
            return remote(src, r3.at[grp, st, h], rs3_s.at[grp, 2 * st + h], rs3_r.at[grp, 2 * st + h], swap[DIMS3[grp]][(st + h) % 2])

        def first(groups=ALL):
            for grp in groups:
                for h in range(PAIR):
                    desc(grp, 0, h).start()

        def second(groups=ALL):
            for grp in groups:
                for h in range(PAIR):
                    desc(grp, 0, h).wait_recv()
                    s3[grp, h] = half3(acc, grp, h)[...] + r3[grp, 0, h]
                    desc(grp, 1, h).start()

        def last(grp, h):
            desc(grp, 1, h).wait_recv()
            return s3[grp, h] + r3[grp, 1, h]

        def drain():
            for grp in range(GROUPS):
                for i in range(RING):
                    desc(grp, i // 2, i % 2).wait_send()

        return first, second, last, drain

    def ag_direct(buf, ssem, rsem):
        def desc(grp, i):
            delta = (2, 1, 3)[i]
            ref = block(buf, grp)
            return remote(ref, ref, ssem.at[grp, i], rsem.at[grp, i], peer(DIMS3[grp], delta))

        def first(groups=ALL):
            for i in range(GROUPS):
                for grp in groups:
                    desc(grp, i).start()

        def last(groups=ALL):
            for grp in groups:
                for i in range(GROUPS):
                    desc(grp, i).wait_recv()

        def drain():
            for grp in range(GROUPS):
                for i in range(GROUPS):
                    desc(grp, i).wait_send()

        return first, last, drain

    rs1 = [rs_ring(piece(OFFS[k]), acc, DIMS1, [r1.at[k, g] for g in ALL], rs1_s.at[k], rs1_r.at[k]) for k in range(RING)]
    rs2 = rs_ring(half2, acc, DIMS2, (r2.at[0], r2.at[1], r2.at[2]), rs2_s, rs2_r)
    rs3 = sum_pairs()
    m3 = ag_direct(mg, m3_s, m3_r)
    u2 = ag_ring(half2, xg, DIMS2, u2_s, u2_r)
    u1 = [ag_ring(piece(d), xg, DIMS1, u1_s.at[d], u1_r.at[d]) for d in range(RING)]
    wg3 = ag_direct(wg, w3_s, w3_r)
    wg2 = ag_ring(half2, wg, DIMS2, w2_s, w2_r)
    wg1 = ag_ring(half1, wg, DIMS1, w1_s, w1_r)

    for k in range(RING):
        start_own(k)

    def row_copies():
        pairs = ((m_sq, w_sq, q_sq), (m_kv, w_kv, q_kv), (m_up, w_up, q_up), (m_dn, w_dn, q_dn))
        return [pltpu.make_async_copy(src[a], src[2].at[a], row_s.at[a, i]) for i, src in enumerate(pairs) for a in range(PAIR)]

    for cp in row_copies():
        cp.start()

    def pack_pieces():
        for cp in row_copies():
            cp.wait()
        for a in range(PAIR):
            for c in range(PAIR):
                for xd in range(RING):
                    pieces[a, c, xd, :SLAB, :] = q_sq[a, :, c, LANES * xd:LANES * xd + LANES]
                    if xd < 3:
                        pieces[a, c, xd, SUB:P_END, :] = q_sq[a, :, c, HALF_D + LANES * xd:P_AT + LANES * xd]
            pieces[a, 0, 3, SUB:P_END, :KVD] = q_kv[a, :, 0, :]
            pieces[a, 0, 3, SUB:P_END, KVD:LANES] = q_kv[a, :, 1, :]
            pieces[a, 1, 3, SUB:P_END, :] = q_up[a, :, 0, :LANES]
            pieces[a, 1, 0, TILE16:Q_END, :] = q_up[a, :, 0, LANES:FF]
            pieces[a, 1, 1, TILE16:Q_END, :] = q_up[a, :, 1, :LANES]
            pieces[a, 1, 2, TILE16:Q_END, :] = q_up[a, :, 1, LANES:FF]
            for xd in range(PAIR):
                for j in range(SLAB):
                    pieces[a, 0, xd, DOWN_AT + PAIR * j:DOWN_NEXT + PAIR * j, :] = q_dn[a, 0, :, LANES * j:LANES * j + LANES]

    acc[11] = jnp.zeros((RING, RING, BROWS, LANES), F32)

    @pl.when(core == 0)
    def _():
        acc[10] = jnp.zeros((RING, RING, BROWS, LANES), F32)

    pack_pieces()
    pl.semaphore_wait(barrier, PEERS)

    for k in range(RING):
        start_par(k)

    def pre(a, i):
        dx, dc = row_peers[i]
        return remote(pieces.at[a, (core, other)[dc], around["x"][dx]], recvp.at[a, slot], pre_s.at[a, i], pre_r.at[a, i], row_peer(dx, dc))

    def pre_start(a):
        for i in range(SLAB):
            pre(a, i).start()
        recvp[a, slot] = pieces[a, core, x]

    def pre_done(a):
        for i in range(SLAB):
            pre(a, i).wait_recv()
        for g in range(GROUPS):
            for s in range(SUB):
                mb[a, g, SLAB * s:SLAB * s + SLAB, :] = recvp[a, s, SUB * g:SUB * g + SLAB, :]

        @pl.when(jnp.logical_and(core == 0, x < 2))
        def _():
            for i in range(RING):
                for j in range(SLAB):
                    mb[a, 2, SUB * j + 2 * i:SUB * j + 2 * i + 2, :] = recvp[a, RING * x + i, DOWN_AT + PAIR * j:DOWN_NEXT + PAIR * j, :]

    ORDER = (2, 1, 0)
    pre_start(0)
    for add, g in ((add_r, 0), (add_q, PAIR), (add_p, 1)):
        add(0)
        if g == 1:
            add_kv()
        for k in range(RING):
            rs1[k][0]((g,))
    for add, g in ((add_r, 0), (add_p, 1), (add_q, PAIR)):
        add(1)
        add(PAIR)
        rs1[0][1]((g,))
    for add in (add_r, add_p, add_q):
        add(GROUPS)
    def forward(k):
        for g in ORDER:
            if k:
                rs1[k][1]((g,))
            rs1[k][2]((g,))

    def finish(k):
        for g in ORDER:
            rs1[k][GROUPS]((g,))
            if k == 0:
                rs2[0]((g,))
            if k == 2:
                rs2[1]((g,))

    forward(0)
    forward(1)
    finish(0)
    forward(2)
    finish(1)
    forward(GROUPS)
    pre_done(0)
    finish(2)
    for g in ORDER:
        rs2[2]((g,))
    finish(GROUPS)
    for g in range(GROUPS):
        mg[RING * g + x, z, y] = mb[0, g]
    m3[0]()
    for g in ORDER:
        rs2[3]((g,))
        rs3[0]((g,))
    pre_start(1)
    for g in ORDER:
        rs3[1]((g,))
    m3[1]()
    for g in ORDER:
        for h in range(PAIR):
            grad = rs3[2](g, h) * (1.0 / GROUP)
            mom_new = MU * half3(mg, g, h)[...] + grad
            mt[g, 2 * h:2 * h + 2] = mom_new
            half3(xg, g, h)[...] = (grad + MU * mom_new).astype(BF16)
        u2[0]((g,))
    for g in ORDER:
        u1[0][0]((g,))
    for g in range(GROUPS):
        nb[g] = mt[g, around[DIMS3[g]][0]]

    def pack_rows(src, dst):
        for s in range(SUB):
            for g in range(GROUPS):
                dst[s, SUB * g:SUB * g + SLAB, :] = src[g, SLAB * s:SLAB * s + SLAB, :]
            for j in range(SLAB):
                r = SUB * j + 2 * (s % RING)
                dst[s, DOWN_AT + PAIR * j:DOWN_NEXT + PAIR * j, :] = src[2, r:r + 2, :]

    def post(src, dst, ssem, rsem, i):
        dx, dc = row_peers[i]
        dest = row_slot[dx, dc]
        return remote(src.at[dest], dst.at[slot], ssem.at[i], rsem.at[i], row_peer(dx, dc))

    for g in ORDER:
        u2[1]((g,))
    for g in ORDER:
        u2[RING](g, (1, RING))
        u1[GROUPS][0]((g,))
        u1[1][0]((g,))
    for g in ORDER:
        u1[0][1]((g,))
    pre_done(1)
    for g in range(GROUPS):
        wg[RING * g + x, z, y] = mb[1, g]
    for g in ORDER:
        u2[RING](g, (PAIR, 5))
        u1[PAIR][0]((g,))
    wg3[0]()
    for g in ORDER:
        u1[GROUPS][1]((g,))
        u1[1][1]((g,))
    pack_rows(nb, outp)
    for g in ORDER:
        u1[PAIR][1]((g,))
    for i in range(SLAB):
        post(outp, mrecv, mo_s, mo_r, i).start()
    mrecv[slot] = outp[slot]
    wg3[1]()
    wg2[0]()
    for d in (0, GROUPS, 1, PAIR):
        u1[d][2]()

    def total(units):
        part = jnp.zeros((BROWS, LANES), F32)
        for u in units:
            v = xg[u].astype(F32)
            part = part + jnp.sum(v * v, axis=(0, 1))
        return 1.0 / (jnp.sqrt(jnp.sum(part, keepdims=True)) + EPS)

    def column(u, inv):
        return xg[u].astype(F32).reshape(D, LANES) * inv

    inv = total(range(SLAB))
    for u in range(SLAB):
        xx[0, :, LANES * u:LANES * u + LANES] = column(u, inv).astype(BF16)

    @pl.when(core == 0)
    def _():
        inv_d = total((SUB, 9))
        both = [(xg[u].astype(F32) * inv_d).reshape(TILE16, SLAB, SUB, LANES) for u in (SUB, 9)]
        both = jnp.concatenate(both, axis=2)
        for j in range(SLAB):
            ss[0, 0, :, LANES * j:LANES * j + LANES] = both[:, j].reshape(FF, LANES).astype(BF16)
        v = xg[SLAB].astype(F32)
        v = v.reshape(D, LANES).T
        for i in range(PAIR):
            h = v[KVD * i:KVD * i + KVD]
            norm = jnp.sqrt(jnp.sum(h * h, keepdims=True))
            ss[0, 1, KVD * i:KVD * i + KVD, :] = (h * (1.0 / (norm + EPS))).astype(BF16)
        ss[0, 1, LANES:FF, :] = jnp.zeros((LANES, D), BF16)

    @pl.when(core == 1)
    def _():
        for i in range(PAIR):
            inv_u = total((SLAB + 2 * i, SUB + 2 * i))
            for h in range(PAIR):
                ss[0, i, LANES * h:LANES * h + LANES, :] = column(SLAB + 2 * i + h, inv_u).T.astype(BF16)


    NT = (((1,), (1,)), ((), ()))
    ROWS = ((0, FF), (FF, FF), (HALF_D, FF), (TAIL_D, LANES))
    row_id = lax.broadcasted_iota(jnp.int32, (FF, FF), 0) // KVD
    col_id = lax.broadcasted_iota(jnp.int32, (FF, FF), 1) // KVD
    keep = jnp.logical_or(row_id == col_id, core == 1)

    def symmetric(product, out):
        for r in (0, FF, HALF_D):
            value = product(r, FF, r, TAIL_D - r)
            out[r:r + FF, r:TAIL_D] = value
            if r < HALF_D:
                out[r + FF:TAIL_D, r:r + FF] = value[:, FF:].T
        value = product(TAIL_D, LANES, 0, D)
        out[TAIL_D:D, :] = value
        out[:TAIL_D, TAIL_D:D] = value[:, :TAIL_D].T

    def poly_step(cur, it):
        def gram(r, n, c, m):
            return lax.dot_general(xx[cur, r:r + n, :], xx[cur, c:c + m, :], NT, preferred_element_type=F32).astype(BF16)

        symmetric(gram, aa)
        for i in range(PAIR):
            g = lax.dot_general(ss[cur, i], ss[cur, i], NT, preferred_element_type=F32)
            if i == 1:
                g = jnp.where(keep, g, 0.0)
            sa[i] = g.astype(BF16)

        if it == 0:
            wg2[1]()
        if it == 1:
            wg2[2]()
            wg1[0]()

        def poly(r, n, c, m):
            sq = jnp.dot(aa[r:r + n, :], aa[:, c:c + m], preferred_element_type=F32)
            return (COEF_B * aa[r:r + n, c:c + m].astype(F32) + COEF_C * sq).astype(BF16)

        symmetric(poly, bb)
        for i in range(PAIR):
            sq = jnp.dot(sa[i], sa[i], preferred_element_type=F32)
            sb[i] = (COEF_B * sa[i].astype(F32) + COEF_C * sq).astype(BF16)
        if it == 2:
            wg1[1]()

    def apply_small(cur, nxt):
        for i in range(PAIR):
            prod = jnp.dot(sb[i], ss[cur, i], preferred_element_type=F32)
            ss[nxt, i] = (COEF_A * ss[cur, i].astype(F32) + prod).astype(BF16)

    def apply_rows(cur, r, n):
        prod = jnp.dot(bb[pl.ds(r, n), :], xx[cur], preferred_element_type=F32)
        return (COEF_A * xx[cur, pl.ds(r, n), :].astype(F32) + prod).astype(BF16)

    def step(it, carry):
        cur = it % 2
        nxt = 1 - cur
        poly_step(cur, it)
        for r, n in ROWS:
            xx[nxt, r:r + n, :] = apply_rows(cur, r, n)
        apply_small(cur, nxt)
        return carry

    for it in range(NS_STEPS - 1):
        step(it, 0)
    cur = (NS_STEPS - 1) % 2
    fin = 1 - cur
    poly_step(cur, None)
    apply_small(cur, fin)

    wg1[2]()
    wg1[3]()
    wg2[3]()
    wg3[2]()

    def update(w, v):
        return w - LR * (SCALE * v + WD * w)

    def out_copy(i, ref):
        return remote(ref, ref, or_s.at[i], or_r.at[i], partner)

    def sq_ref(p, c):
        return vb_sq.at[c, pl.ds(pl.multiple_of(QROWS * p, ALIGN), QROWS)]

    def small_refs(c):
        return (vb_kv, vb_dn) if c == 0 else (vb_up.at[0], vb_up.at[1])

    def column_new(u, v):
        new = update(wg[u].reshape(D, LANES), v)
        wg[u] = new.reshape(RING, RING, BROWS, LANES)
        return new

    @pl.when(core == 0)
    def _():
        v = ss[fin, 1, :LANES, :].astype(F32).T
        vb_kv[...] = column_new(SLAB, v).T.astype(BF16)
        for j in range(SLAB):
            v = ss[fin, 0, :, LANES * j:LANES * j + LANES].astype(F32).reshape(RING, RING, TILE16, LANES)
            lo = update(wg[SUB, :, :, SUB * j:SUB * j + SUB, :], v[:, :, :SUB])
            hi = update(wg[9, :, :, SUB * j:SUB * j + SUB, :], v[:, :, SUB:TILE16])
            wg[SUB, :, :, SUB * j:SUB * j + SUB, :] = lo
            wg[9, :, :, SUB * j:SUB * j + SUB, :] = hi
            vb_dn[:, LANES * j:LANES * j + LANES] = jnp.concatenate([lo, hi], axis=2).reshape(FF, LANES).astype(BF16)
        for i in range(PAIR):
            out_copy(SUB + i, small_refs(0)[i]).start()

    @pl.when(core == 1)
    def _():
        for i in range(PAIR):
            for h in range(PAIR):
                v = ss[fin, i, LANES * h:LANES * h + LANES, :].astype(F32).T
                vb_up[i, :, LANES * h:LANES * h + LANES] = column_new(SLAB + 2 * i + h, v).astype(BF16)
        for i in range(PAIR):
            out_copy(SUB + i, small_refs(1)[i]).start()

    for i in range(RING):
        q = around["z"][i]
        v = apply_rows(cur, pl.multiple_of(QROWS * q, ALIGN), QROWS).astype(F32)
        for u in range(SLAB):
            new = update(wg[u, q].reshape(QROWS, LANES), v[:, LANES * u:LANES * u + LANES])
            wg[u, q] = new.reshape(RING, BROWS, LANES)
            vb_sq[core, pl.ds(pl.multiple_of(QROWS * q, ALIGN), QROWS), LANES * u:LANES * u + LANES] = new.astype(BF16)
        out_copy(i, sq_ref(q, core)).start()
        if i == 0:
            for g in range(GROUPS):
                nb[g] = wg[RING * g + x, z, y]
            pack_rows(nb, outw)
            for k in range(SLAB):
                post(outw, wrecv, wo_s, wo_r, k).start()
            wrecv[slot] = outw[slot]

    for i in range(SLAB):
        post(outp, mrecv, mo_s, mo_r, i).wait_recv()
        post(outw, wrecv, wo_s, wo_r, i).wait_recv()

    for p in range(RING):
        out_copy(p, sq_ref(around["z"][p], core)).wait()
    for c in range(PAIR):
        @pl.when(core == c)
        def _():
            for i in range(PAIR):
                out_copy(SUB + i, small_refs(c)[i]).wait_send()
                out_copy(SUB + i, small_refs(1 - c)[i]).wait_recv()
    for i in range(SLAB):
        pre(0, i).wait_send()
        pre(1, i).wait_send()
        post(outp, mrecv, mo_s, mo_r, i).wait_send()
        post(outw, wrecv, wo_s, wo_r, i).wait_send()
    for k in range(RING):
        for i, item in enumerate(common_items(other, k, 1)):
            par_copy(k, i, item).wait_send()
        for tc in range(PAIR):
            @pl.when(core == 1 - tc)
            def _():
                for i, item in enumerate(special_items(tc, k, 1)):
                    par_copy(k, 2 + i, item).wait_send()
    for k in range(RING):
        rs1[k][RING]()
        u1[k][GROUPS]()
    rs2[RING]()
    rs3[3]()
    m3[2]()
    u2[3]()


def unpack_rows(slot, src, o_sq, o_kv, o_up, o_dn):
    for c in range(PAIR):
        for xs in range(RING):
            t = 2 * xs + c
            o_sq[:, c, LANES * xs:LANES * xs + LANES] = src[t, :SLAB, :]
            if xs < 3:
                o_sq[:, c, HALF_D + LANES * xs:P_AT + LANES * xs] = src[t, SUB:P_END, :]
    o_kv[:, 0, :] = src[HOPS, SUB:P_END, :KVD]
    o_kv[:, 1, :] = src[HOPS, SUB:P_END, KVD:LANES]
    o_up[:, 0, :LANES] = src[SLAB, SUB:P_END, :]
    o_up[:, 0, LANES:FF] = src[1, TILE16:Q_END, :]
    o_up[:, 1, :LANES] = src[3, TILE16:Q_END, :]
    o_up[:, 1, LANES:FF] = src[5, TILE16:Q_END, :]
    t = 2 * lax.div(slot, RING)
    for j in range(SLAB):
        o_dn[0, :, LANES * j:LANES * j + LANES] = src[t, DOWN_AT + PAIR * j:DOWN_NEXT + PAIR * j, :]


def write_out(
    mrecv, wrecv, vb_sq, vb_kv, vb_up, vb_dn,
    mo_sq, mo_kv, mo_up, mo_dn, wo_sq, wo_kv, wo_up, wo_dn, b_sq, b_kv, b_up, b_dn, sem,
):
    copies = [pltpu.make_async_copy(src, dst, sem.at[i]) for i, (src, dst) in enumerate(
        ((vb_sq, b_sq), (vb_kv, b_kv), (vb_up, b_up), (vb_dn, b_dn)))]
    for cp in copies:
        cp.start()
    me = lax.axis_index("data")
    slot = lax.rem(me, SUB)
    unpack_rows(slot, mrecv, mo_sq, mo_kv, mo_up, mo_dn)
    unpack_rows(slot, wrecv, wo_sq, wo_kv, wo_up, wo_dn)
    for cp in copies:
        cp.wait()


def solution(mesh):
    grad_spec = P(("model", "data"))
    slab_spec = P("model", "data")
    full_spec = P("model")

    def local_step(g_sq, m_sq, w_sq, g_kv, m_kv, w_kv, g_up, m_up, w_up, g_dn, m_dn, w_dn):
        g_sq = g_sq.reshape(2, RING, RING, BROWS, D)
        g_kv = g_kv[0].transpose(0, 2, 1)
        g_up = g_up.reshape(2, RING, RING, BROWS, FF)
        g_dn = g_dn.reshape(RING, RING, TILE16, D)
        vm = pl.BlockSpec(memory_space=pltpu.VMEM)
        hb = pl.BlockSpec(memory_space=pltpu.HBM)
        V = pltpu.VMEM
        block = (BROWS, LANES)
        unit = (RING, RING) + block
        half = (PAIR, RING) + block
        two = (PAIR,) + block
        mats = (PAIR, PAIR)
        rows_of = (PAIR, SLAB, PAIR)
        floats = [
            (PAIR, RING) + unit, (PAIR, RING, RING, BROWS, TRIO), mats + (KVD, D), mats + (RING, RING, BROWS, FF), (PAIR, RING, RING, TILE16, D), (UNITS,) + unit,
            (RING, GROUPS, HOPS) + two, (GROUPS, HOPS) + two, (GROUPS,) + mats + two, (GROUPS, PAIR) + two,
            (UNITS,) + unit, (GROUPS, RING) + block,
            rows_of + (D,), rows_of + (KVD,), rows_of + (FF,), (2, 1, 2, D),
            mats + (RING, PACK, LANES), (PAIR, SUB, PACK, LANES), (PAIR, GROUPS) + block, (GROUPS,) + block, PACKED, PACKED,
        ]
        scratch = [V(a, F32) for a in floats] + [V((UNITS,) + unit, BF16), V((UNITS,) + unit, F32)]
        scratch += [V(a, BF16) for a in ((PAIR, D, D), (D, D), (D, D), mats + (FF, D), (PAIR, FF, FF), (PAIR, FF, FF))]
        rings, ring, pairs, direct, row = (RING, GROUPS, HOPS), (GROUPS, HOPS), (GROUPS, RING), (GROUPS, GROUPS), (SLAB,)
        sems = [(RING, 5), (2, RING)]
        for a in ((RING, 5), (PAIR,) + row, row, row, rings, ring, pairs, direct, ring, rings, direct, ring, ring, (10,)):
            sems += [a, a]
        scratch += [DMA(a) for a in sems]

        def rows(a):
            return a.transpose(1, 0, 2)

        mid = [V(s, F32) for s in (PACKED, PACKED)]
        mid += [V(s, BF16) for s in ((2, D, D), (LANES, D), (2, D, FF), (FF, D))]
        parts = pl.pallas_call(
            kernel,
            out_shape=mid,
            in_specs=[hb] * UNITS,
            out_specs=[vm] * HOPS,
            scratch_shapes=scratch,
            compiler_params=pltpu.CompilerParams(collective_id=0, has_side_effects=True, vmem_limit_bytes=61700000),
            name="muon",
        )(g_sq, g_kv, g_up, g_dn, rows(m_sq), rows(m_kv), rows(m_up), m_dn, rows(w_sq), rows(w_kv), rows(w_up), w_dn)
        small = [jax.ShapeDtypeStruct(s, F32) for s in ((SLAB, PAIR, D), (SLAB, PAIR, KVD), (SLAB, PAIR, FF), (1, PAIR, D))]
        full = [jax.ShapeDtypeStruct(s, BF16) for s in ((2, D, D), (LANES, D), (2, D, FF), (FF, D))]
        out = pl.pallas_call(
            write_out,
            out_shape=small + small + full,
            in_specs=[vm] * HOPS,
            out_specs=[vm] * SUB + [hb] * RING,
            scratch_shapes=[DMA((RING,))],
            compiler_params=pltpu.CompilerParams(vmem_limit_bytes=4_000_000),
            name="write_out",
        )(*parts)
        m, w, b = out[0:RING], out[RING:SUB], out[SUB:UNITS]
        return (
            rows(m[0]), rows(w[0]), b[0],
            rows(m[1]), rows(w[1]), b[1].reshape(2, KVD, D).transpose(0, 2, 1),
            rows(m[2]), rows(w[2]), b[2],
            m[3], w[3], b[3].reshape(1, FF, D),
        )

    in_specs = (grad_spec, slab_spec, slab_spec) * RING
    out_specs = (slab_spec, slab_spec, full_spec) * RING
    return jax.shard_map(local_step, mesh=mesh, in_specs=in_specs, out_specs=out_specs, check_vma=False)
```

```python
import math
import jax
import jax.numpy as jnp
from jax import lax
from jax.experimental import pallas as pl
from jax.experimental.pallas import tpu as pltpu
from jax.sharding import PartitionSpec as P

NS_STEPS = 5
MU = 0.95
LR = 0.1
WD = 0.5
EPS = 1e-7
COEF_A = 3.4445
COEF_B = -4.7750
COEF_C = 2.0315
GROUP = 128
D = 896
SCALE = 0.2 * math.sqrt(896.0)
GROUPS = 3
PAIR = 2
ALL = tuple(range(GROUPS))
RING = 4
HOPS = 6
SLAB = 7
SUB = 8
UNITS = 12
PEERS = 13
P_END = 15
TILE16 = 16
Q_END = 23
DOWN_AT = 24
DOWN_NEXT = 26
ALIGN = 32
PACK = 40
BROWS = 56
KVD = 64
LANES = 128
QROWS = 224
FF = 256
TRIO = 384
HALF_D = 512
P_AT = 640
TAIL_D = 768
PACKED = (SUB, PACK, LANES)
MESH = pl.DeviceIdType.MESH
F32 = jnp.float32
BF16 = jnp.bfloat16
DMA = pltpu.SemaphoreType.DMA


def kernel(
    g_sq, g_kv, g_up, g_dn,
    m_sq, m_kv, m_up, m_dn,
    w_sq, w_kv, w_up, w_dn,
    mrecv, wrecv, vb_sq, vb_kv, vb_up, vb_dn,
    br, bp, kvb, upb, dnb, acc,
    r1, r2, r3, s3, mg, mt,
    q_sq, q_kv, q_up, q_dn,
    pieces, recvp, mb, nb, outp, outw,
    xg, wg, xx, aa, bb, ss, sa, sb,
    own_s, row_s, d2d_s, d2d_r, pre_s, pre_r, mo_s, mo_r, wo_s, wo_r,
    rs1_s, rs1_r, rs2_s, rs2_r, rs3_s, rs3_r,
    m3_s, m3_r, u2_s, u2_r, u1_s, u1_r,
    w3_s, w3_r, w2_s, w2_r, w1_s, w1_r,
    or_s, or_r,
):
    me = lax.axis_index("data")
    core = lax.rem(me, 2)
    x = lax.rem(lax.div(me, 2), RING)
    y = lax.rem(lax.div(me, SUB), RING)
    z = lax.div(me, ALIGN)
    slot = 2 * x + core
    other = 1 - core
    around = {
        "x": [x] + [lax.rem(x + d, RING) for d in (1, 2, 3)],
        "y": [y] + [lax.rem(y + d, RING) for d in (1, 2, 3)],
        "z": [z] + [lax.rem(z + d, RING) for d in (1, 2, 3)],
    }
    partner = me + other - core
    stride = {"x": 2, "y": SUB, "z": ALIGN}
    peers = {dim: [me + (a - around[dim][0]) * stride[dim] for a in around[dim]] for dim in "xyz"}
    row_x = [2 * a - 2 * x for a in around["x"]]

    def peer(dim, delta):
        return peers[dim][delta]

    def remote(src, dst, ssem, rsem, device):
        return pltpu.make_async_remote_copy(
            src_ref=src, dst_ref=dst, send_sem=ssem, recv_sem=rsem,
            device_id={"data": device}, device_id_type=MESH)

    row_peers = [(dx, dc) for dx in range(RING) for dc in range(PAIR) if (dx, dc) != (0, 0)]

    row_dev = {(dx, dc): (me, partner)[dc] + row_x[dx] for dx in range(RING) for dc in range(PAIR)}
    row_slot = {(dx, dc): 2 * around["x"][dx] + (core, other)[dc] for dx in range(RING) for dc in range(PAIR)}

    def row_peer(dx, dc):
        return row_dev[dx, dc]

    barrier = pltpu.get_barrier_semaphore()
    for dx, dc in row_peers:
        pl.semaphore_signal(barrier, inc=1, device_id={"data": row_peer(dx, dc)}, device_id_type=MESH)
    for dim in ("y", "z"):
        for delta in (1, 2, 3):
            pl.semaphore_signal(barrier, inc=1, device_id={"data": peer(dim, delta)}, device_id_type=MESH)

    OFFS = (2, 1, 3, 0)

    def lanes(j):
        return pl.ds(pl.multiple_of(j * LANES, LANES), LANES)

    def common_items(tc, k, w):
        jx, jz = around["x"][OFFS[k]], around["z"][OFFS[k]]
        return [
            (g_sq.at[tc, :, :, :, lanes(jx)], br.at[w, jx]),
            (g_sq.at[tc, jz, :, :, pl.ds(HALF_D, TRIO)], bp.at[w, jz]),
        ]

    def special_items(tc, k, w):
        jz, jy = around["z"][OFFS[k]], around["y"][OFFS[k]]
        if tc == 0:
            items = [(g_dn.at[:, jy], dnb.at[w, :, jy])]
            return items + [(g_kv, kvb.at[w])] if k == 0 else items
        return [
            (g_up.at[0, jz, :, :, pl.ds(0, LANES)], upb.at[w, 0, jz, :, :, pl.ds(0, LANES)]),
            (g_up.at[0, :, jy, :, pl.ds(LANES, LANES)], upb.at[w, 0, :, jy, :, pl.ds(LANES, LANES)]),
            (g_up.at[1, :, jy], upb.at[w, 1, :, jy]),
        ]

    def own_copy(k, i, item):
        return pltpu.make_async_copy(item[0], item[1], own_s.at[k, i])

    def par_copy(k, i, item):
        return remote(item[0], item[1], d2d_s.at[k, i], d2d_r.at[k, i], partner)

    def start_own(k):
        for i, item in enumerate(common_items(core, k, 0)):
            own_copy(k, i, item).start()
        for tc in range(PAIR):
            @pl.when(core == tc)
            def _():
                for i, item in enumerate(special_items(tc, k, 0)):
                    own_copy(k, 2 + i, item).start()

    def start_par(k):
        for i, item in enumerate(common_items(other, k, 1)):
            par_copy(k, i, item).start()
        for tc in range(PAIR):
            @pl.when(core == 1 - tc)
            def _():
                for i, item in enumerate(special_items(tc, k, 1)):
                    par_copy(k, 2 + i, item).start()

    def common(k, w):
        return common_items(core, k, w)

    def down_kv(k, w):
        return special_items(0, k, w)

    def ups(k, w):
        return special_items(1, k, w)

    def arrive(k, i, items, at):
        own_copy(k, i, items(k, 0)[at]).wait()
        par_copy(k, i, items(k, 1)[at]).wait_recv()

    def add_r(k):
        jx = around["x"][OFFS[k]]
        arrive(k, 0, common, 0)
        acc[jx] = br[0, jx] + br[1, jx]

    def add_p(k):
        jz = around["z"][OFFS[k]]
        arrive(k, 1, common, 1)
        for u in range(GROUPS):
            acc[RING + u, jz] = bp[0, jz, :, :, LANES * u:LANES * u + LANES] + bp[1, jz, :, :, LANES * u:LANES * u + LANES]

        @pl.when(core == 1)
        def _():
            arrive(k, PAIR, ups, 0)
            acc[SLAB, jz] = upb[0, 0, jz, :, :, :LANES] + upb[1, 0, jz, :, :, :LANES]

    def add_q(k):
        jy = around["y"][OFFS[k]]

        @pl.when(core == 0)
        def _():
            arrive(k, PAIR, down_kv, 0)
            rows = dnb[0, :, jy] + dnb[1, :, jy]
            for i in range(SLAB):
                acc[SUB, :, jy, SUB * i:SUB * i + SUB, :] = rows[:, :SUB, LANES * i:LANES * i + LANES]
                acc[9, :, jy, SUB * i:SUB * i + SUB, :] = rows[:, SUB:TILE16, LANES * i:LANES * i + LANES]

        @pl.when(core == 1)
        def _():
            for i in (1, 2):
                arrive(k, PAIR + i, ups, i)
            acc[SUB, :, jy] = upb[0, 0, :, jy, :, LANES:FF] + upb[1, 0, :, jy, :, LANES:FF]
            acc[9, :, jy] = upb[0, 1, :, jy, :, :LANES] + upb[1, 1, :, jy, :, :LANES]
            acc[10, :, jy] = upb[0, 1, :, jy, :, LANES:FF] + upb[1, 1, :, jy, :, LANES:FF]

    def add_kv():
        @pl.when(core == 0)
        def _():
            arrive(0, GROUPS, down_kv, 1)
            acc[SLAB] = (kvb[0] + kvb[1]).reshape(LANES, D).T.reshape(RING, RING, BROWS, LANES)

    DIMS1, DIMS2, DIMS3 = ("x", "z", "y"), ("y", "x", "z"), ("z", "y", "x")

    def half1(buf, grp, j, h):
        if grp == 0:
            return buf.at[j, pl.ds(PAIR * h, PAIR)]
        if grp == 1:
            return buf.at[pl.ds(RING + PAIR * h, PAIR), j]
        return buf.at[pl.ds(SUB, 3), pl.ds(PAIR * h, PAIR), j]

    def half2(buf, grp, j, h):
        if grp == 0:
            return buf.at[x, pl.ds(PAIR * h, PAIR), j]
        if grp == 1:
            return buf.at[RING + j, z, pl.ds(PAIR * h, PAIR)]
        return buf.at[pl.ds(SUB + PAIR * h, PAIR), j, y]

    def piece(d2):
        def half(buf, grp, j1, h):
            j2 = around[DIMS2[grp]][d2]
            if grp == 0:
                return buf.at[j1, pl.ds(PAIR * h, PAIR), j2]
            if grp == 1:
                return buf.at[RING + j2, j1, pl.ds(PAIR * h, PAIR)]
            return buf.at[pl.ds(SUB + PAIR * h, PAIR), j2, j1]

        return half

    def half3(buf, grp, h):
        if grp == 0:
            return buf.at[x, pl.ds(PAIR * h, PAIR), y]
        if grp == 1:
            return buf.at[RING + x, z, pl.ds(PAIR * h, PAIR)]
        return buf.at[pl.ds(SUB + PAIR * h, PAIR), z, y]

    def block(buf, grp):
        return buf.at[RING * grp + x, z, y]

    def rs_ring(half, buf, dims, rbufs, ssem, rsem):
        def desc(grp, i):
            dim = dims[grp]
            d, h = ((2, 0), (1, 1), (1, 0), (2, 1), (3, 0), (3, 1))[i]
            src = (around[dim][d], h)
            return remote(half(buf, grp, src[0], src[1]), rbufs[grp].at[i], ssem.at[grp, i], rsem.at[grp, i], peer(dim, 1 if i < GROUPS else GROUPS))

        def add(grp, j, h, i):
            desc(grp, i).wait_recv()
            ref = half(buf, grp, j, h)
            ref[...] += rbufs[grp][i]

        def first(groups=ALL):
            for grp in groups:
                desc(grp, 0).start()
                desc(grp, 3).start()

        def second(groups=ALL):
            for grp in groups:
                desc(grp, 1).start()
                desc(grp, RING).start()

        def third(groups=ALL):
            for grp in groups:
                p = around[dims[grp]]
                add(grp, p[1], 0, 0)
                desc(grp, 2).start()
                add(grp, p[3], 1, 3)
                desc(grp, 5).start()

        def last(groups=ALL):
            for grp in groups:
                p = around[dims[grp]][0]
                add(grp, p, 1, 1)
                add(grp, p, 0, RING)
                add(grp, p, 0, 2)
                add(grp, p, 1, 5)

        def drain():
            for grp in range(GROUPS):
                for i in range(HOPS):
                    desc(grp, i).wait_send()

        return first, second, third, last, drain

    def ag_ring(half, buf, dims, ssem, rsem):
        def desc(grp, i):
            dim = dims[grp]
            d, h = ((0, 0), (0, 1), (3, 0), (0, 1), (0, 0), (1, 1))[i]
            ref = half(buf, grp, around[dim][d], h)
            return remote(ref, ref, ssem.at[grp, i], rsem.at[grp, i], peer(dim, 1 if i < GROUPS else GROUPS))

        def first(groups=ALL):
            for grp in groups:
                for i in (0, 3, 1, RING):
                    desc(grp, i).start()

        def second(groups=ALL):
            for grp in groups:
                desc(grp, 0).wait_recv()
                desc(grp, 2).start()
                desc(grp, 3).wait_recv()
                desc(grp, 5).start()

        def arrived(grp, which):
            for i in which:
                desc(grp, i).wait_recv()

        def last(groups=ALL):
            for grp in groups:
                arrived(grp, (1, RING, PAIR, 5))

        def drain():
            for grp in range(GROUPS):
                for i in range(HOPS):
                    desc(grp, i).wait_send()

        return first, second, last, drain, arrived

    swap = {}
    for d in "xyz":
        p = around[d][0]
        swap[d] = (me + (1 - 2 * lax.rem(p, 2)) * stride[d], me + (3 - 2 * p) * stride[d])

    def sum_pairs():
        def desc(grp, st, h):
            src = half3(acc, grp, h) if st == 0 else s3.at[grp, h]
            return remote(src, r3.at[grp, st, h], rs3_s.at[grp, 2 * st + h], rs3_r.at[grp, 2 * st + h], swap[DIMS3[grp]][(st + h) % 2])

        def first(groups=ALL):
            for grp in groups:
                for h in range(PAIR):
                    desc(grp, 0, h).start()

        def second(groups=ALL):
            for grp in groups:
                for h in range(PAIR):
                    desc(grp, 0, h).wait_recv()
                    s3[grp, h] = half3(acc, grp, h)[...] + r3[grp, 0, h]
                    desc(grp, 1, h).start()

        def last(grp, h):
            desc(grp, 1, h).wait_recv()
            return s3[grp, h] + r3[grp, 1, h]

        def drain():
            for grp in range(GROUPS):
                for i in range(RING):
                    desc(grp, i // 2, i % 2).wait_send()

        return first, second, last, drain

    def ag_direct(buf, ssem, rsem):
        def desc(grp, i):
            delta = (2, 1, 3)[i]
            ref = block(buf, grp)
            return remote(ref, ref, ssem.at[grp, i], rsem.at[grp, i], peer(DIMS3[grp], delta))

        def first(groups=ALL):
            for i in range(GROUPS):
                for grp in groups:
                    desc(grp, i).start()

        def last(groups=ALL):
            for grp in groups:
                for i in range(GROUPS):
                    desc(grp, i).wait_recv()

        def drain():
            for grp in range(GROUPS):
                for i in range(GROUPS):
                    desc(grp, i).wait_send()

        return first, last, drain

    rs1 = [rs_ring(piece(OFFS[k]), acc, DIMS1, [r1.at[k, g] for g in ALL], rs1_s.at[k], rs1_r.at[k]) for k in range(RING)]
    rs2 = rs_ring(half2, acc, DIMS2, (r2.at[0], r2.at[1], r2.at[2]), rs2_s, rs2_r)
    rs3 = sum_pairs()
    m3 = ag_direct(mg, m3_s, m3_r)
    u2 = ag_ring(half2, xg, DIMS2, u2_s, u2_r)
    u1 = [ag_ring(piece(d), xg, DIMS1, u1_s.at[d], u1_r.at[d]) for d in range(RING)]
    wg3 = ag_direct(wg, w3_s, w3_r)
    wg2 = ag_ring(half2, wg, DIMS2, w2_s, w2_r)
    wg1 = ag_ring(half1, wg, DIMS1, w1_s, w1_r)

    for k in range(RING):
        start_own(k)

    def row_copies():
        pairs = ((m_sq, w_sq, q_sq), (m_kv, w_kv, q_kv), (m_up, w_up, q_up), (m_dn, w_dn, q_dn))
        return [pltpu.make_async_copy(src[a], src[2].at[a], row_s.at[a, i]) for i, src in enumerate(pairs) for a in range(PAIR)]

    for cp in row_copies():
        cp.start()

    def pack_pieces():
        for cp in row_copies():
            cp.wait()
        for a in range(PAIR):
            for c in range(PAIR):
                for xd in range(RING):
                    pieces[a, c, xd, :SLAB, :] = q_sq[a, :, c, LANES * xd:LANES * xd + LANES]
                    if xd < 3:
                        pieces[a, c, xd, SUB:P_END, :] = q_sq[a, :, c, HALF_D + LANES * xd:P_AT + LANES * xd]
            pieces[a, 0, 3, SUB:P_END, :KVD] = q_kv[a, :, 0, :]
            pieces[a, 0, 3, SUB:P_END, KVD:LANES] = q_kv[a, :, 1, :]
            pieces[a, 1, 3, SUB:P_END, :] = q_up[a, :, 0, :LANES]
            pieces[a, 1, 0, TILE16:Q_END, :] = q_up[a, :, 0, LANES:FF]
            pieces[a, 1, 1, TILE16:Q_END, :] = q_up[a, :, 1, :LANES]
            pieces[a, 1, 2, TILE16:Q_END, :] = q_up[a, :, 1, LANES:FF]
            for xd in range(PAIR):
                for j in range(SLAB):
                    pieces[a, 0, xd, DOWN_AT + PAIR * j:DOWN_NEXT + PAIR * j, :] = q_dn[a, 0, :, LANES * j:LANES * j + LANES]

    acc[11] = jnp.zeros((RING, RING, BROWS, LANES), F32)

    @pl.when(core == 0)
    def _():
        acc[10] = jnp.zeros((RING, RING, BROWS, LANES), F32)

    pack_pieces()
    pl.semaphore_wait(barrier, PEERS)

    for k in range(RING):
        start_par(k)

    def pre(a, i):
        dx, dc = row_peers[i]
        return remote(pieces.at[a, (core, other)[dc], around["x"][dx]], recvp.at[a, slot], pre_s.at[a, i], pre_r.at[a, i], row_peer(dx, dc))

    def pre_start(a):
        for i in range(SLAB):
            pre(a, i).start()
        recvp[a, slot] = pieces[a, core, x]

    def pre_done(a):
        for i in range(SLAB):
            pre(a, i).wait_recv()
        for g in range(GROUPS):
            for s in range(SUB):
                mb[a, g, SLAB * s:SLAB * s + SLAB, :] = recvp[a, s, SUB * g:SUB * g + SLAB, :]

        @pl.when(jnp.logical_and(core == 0, x < 2))
        def _():
            for i in range(RING):
                for j in range(SLAB):
                    mb[a, 2, SUB * j + 2 * i:SUB * j + 2 * i + 2, :] = recvp[a, RING * x + i, DOWN_AT + PAIR * j:DOWN_NEXT + PAIR * j, :]

    ORDER = (2, 1, 0)
    pre_start(0)
    for add, g in ((add_r, 0), (add_q, PAIR), (add_p, 1)):
        add(0)
        if g == 1:
            add_kv()
        for k in range(RING):
            rs1[k][0]((g,))
    for add, g in ((add_r, 0), (add_p, 1), (add_q, PAIR)):
        add(1)
        add(PAIR)
        rs1[0][1]((g,))
    for add in (add_r, add_p, add_q):
        add(GROUPS)
    def forward(k):
        for g in ORDER:
            if k:
                rs1[k][1]((g,))
            rs1[k][2]((g,))

    def finish(k):
        for g in ORDER:
            rs1[k][GROUPS]((g,))
            if k == 0:
                rs2[0]((g,))
            if k == 2:
                rs2[1]((g,))

    forward(0)
    forward(1)
    finish(0)
    forward(2)
    finish(1)
    forward(GROUPS)
    pre_done(0)
    finish(2)
    for g in ORDER:
        rs2[2]((g,))
    finish(GROUPS)
    for g in range(GROUPS):
        mg[RING * g + x, z, y] = mb[0, g]
    m3[0]()
    for g in ORDER:
        rs2[3]((g,))
        rs3[0]((g,))
    pre_start(1)
    for g in ORDER:
        rs3[1]((g,))
    m3[1]()
    for g in ORDER:
        for h in range(PAIR):
            grad = rs3[2](g, h) * (1.0 / GROUP)
            mom_new = MU * half3(mg, g, h)[...] + grad
            mt[g, 2 * h:2 * h + 2] = mom_new
            half3(xg, g, h)[...] = (grad + MU * mom_new).astype(BF16)
        u2[0]((g,))
    for g in ORDER:
        u1[0][0]((g,))
    for g in range(GROUPS):
        nb[g] = mt[g, around[DIMS3[g]][0]]

    def pack_rows(src, dst):
        for s in range(SUB):
            for g in range(GROUPS):
                dst[s, SUB * g:SUB * g + SLAB, :] = src[g, SLAB * s:SLAB * s + SLAB, :]
            for j in range(SLAB):
                r = SUB * j + 2 * (s % RING)
                dst[s, DOWN_AT + PAIR * j:DOWN_NEXT + PAIR * j, :] = src[2, r:r + 2, :]

    def post(src, dst, ssem, rsem, i):
        dx, dc = row_peers[i]
        dest = row_slot[dx, dc]
        return remote(src.at[dest], dst.at[slot], ssem.at[i], rsem.at[i], row_peer(dx, dc))

    for g in ORDER:
        u2[1]((g,))
    for g in ORDER:
        u2[RING](g, (1, RING))
        u1[GROUPS][0]((g,))
        u1[1][0]((g,))
    for g in ORDER:
        u1[0][1]((g,))
    pre_done(1)
    for g in range(GROUPS):
        wg[RING * g + x, z, y] = mb[1, g]
    for g in ORDER:
        u2[RING](g, (PAIR, 5))
        u1[PAIR][0]((g,))
    wg3[0]()
    for g in ORDER:
        u1[GROUPS][1]((g,))
        u1[1][1]((g,))
    pack_rows(nb, outp)
    for g in ORDER:
        u1[PAIR][1]((g,))
    for i in range(SLAB):
        post(outp, mrecv, mo_s, mo_r, i).start()
    mrecv[slot] = outp[slot]
    wg3[1]()
    wg2[0]()
    for d in (0, GROUPS, 1, PAIR):
        u1[d][2]()

    def total(units):
        part = jnp.zeros((BROWS, LANES), F32)
        for u in units:
            v = xg[u].astype(F32)
            part = part + jnp.sum(v * v, axis=(0, 1))
        return 1.0 / (jnp.sqrt(jnp.sum(part, keepdims=True)) + EPS)

    def column(u, inv):
        return xg[u].astype(F32).reshape(D, LANES) * inv

    inv = total(range(SLAB))
    for u in range(SLAB):
        xx[0, :, LANES * u:LANES * u + LANES] = column(u, inv).astype(BF16)

    @pl.when(core == 0)
    def _():
        inv_d = total((SUB, 9))
        both = [(xg[u].astype(F32) * inv_d).reshape(TILE16, SLAB, SUB, LANES) for u in (SUB, 9)]
        both = jnp.concatenate(both, axis=2)
        for j in range(SLAB):
            ss[0, 0, :, LANES * j:LANES * j + LANES] = both[:, j].reshape(FF, LANES).astype(BF16)
        v = xg[SLAB].astype(F32)
        v = v.reshape(D, LANES).T
        for i in range(PAIR):
            h = v[KVD * i:KVD * i + KVD]
            norm = jnp.sqrt(jnp.sum(h * h, keepdims=True))
            ss[0, 1, KVD * i:KVD * i + KVD, :] = (h * (1.0 / (norm + EPS))).astype(BF16)
        ss[0, 1, LANES:FF, :] = jnp.zeros((LANES, D), BF16)

    @pl.when(core == 1)
    def _():
        for i in range(PAIR):
            inv_u = total((SLAB + 2 * i, SUB + 2 * i))
            for h in range(PAIR):
                ss[0, i, LANES * h:LANES * h + LANES, :] = column(SLAB + 2 * i + h, inv_u).T.astype(BF16)


    NT = (((1,), (1,)), ((), ()))
    ROWS = ((0, FF), (FF, FF), (HALF_D, FF), (TAIL_D, LANES))
    row_id = lax.broadcasted_iota(jnp.int32, (FF, FF), 0) // KVD
    col_id = lax.broadcasted_iota(jnp.int32, (FF, FF), 1) // KVD
    keep = jnp.logical_or(row_id == col_id, core == 1)

    def symmetric(product, out):
        for r in (0, FF, HALF_D):
            value = product(r, FF, r, TAIL_D - r)
            out[r:r + FF, r:TAIL_D] = value
            if r < HALF_D:
                out[r + FF:TAIL_D, r:r + FF] = value[:, FF:].T
        value = product(TAIL_D, LANES, 0, D)
        out[TAIL_D:D, :] = value
        out[:TAIL_D, TAIL_D:D] = value[:, :TAIL_D].T

    def poly_step(cur, it):
        def gram(r, n, c, m):
            return lax.dot_general(xx[cur, r:r + n, :], xx[cur, c:c + m, :], NT, preferred_element_type=F32).astype(BF16)

        symmetric(gram, aa)
        for i in range(PAIR):
            g = lax.dot_general(ss[cur, i], ss[cur, i], NT, preferred_element_type=F32)
            if i == 1:
                g = jnp.where(keep, g, 0.0)
            sa[i] = g.astype(BF16)

        if it == 0:
            wg2[1]()
        if it == 1:
            wg2[2]()
            wg1[0]()

        def poly(r, n, c, m):
            sq = jnp.dot(aa[r:r + n, :], aa[:, c:c + m], preferred_element_type=F32)
            return (COEF_B * aa[r:r + n, c:c + m].astype(F32) + COEF_C * sq).astype(BF16)

        symmetric(poly, bb)
        for i in range(PAIR):
            sq = jnp.dot(sa[i], sa[i], preferred_element_type=F32)
            sb[i] = (COEF_B * sa[i].astype(F32) + COEF_C * sq).astype(BF16)
        if it == 2:
            wg1[1]()

    def apply_small(cur, nxt):
        for i in range(PAIR):
            prod = jnp.dot(sb[i], ss[cur, i], preferred_element_type=F32)
            ss[nxt, i] = (COEF_A * ss[cur, i].astype(F32) + prod).astype(BF16)

    def apply_rows(cur, r, n):
        prod = jnp.dot(bb[pl.ds(r, n), :], xx[cur], preferred_element_type=F32)
        return (COEF_A * xx[cur, pl.ds(r, n), :].astype(F32) + prod).astype(BF16)

    def step(it, carry):
        cur = it % 2
        nxt = 1 - cur
        poly_step(cur, it)
        for r, n in ROWS:
            xx[nxt, r:r + n, :] = apply_rows(cur, r, n)
        apply_small(cur, nxt)
        return carry

    for it in range(NS_STEPS - 1):
        step(it, 0)
    cur = (NS_STEPS - 1) % 2
    fin = 1 - cur
    poly_step(cur, None)
    apply_small(cur, fin)

    wg1[2]()
    wg1[3]()
    wg2[3]()
    wg3[2]()

    def update(w, v):
        return w - LR * (SCALE * v + WD * w)

    def out_copy(i, ref):
        return remote(ref, ref, or_s.at[i], or_r.at[i], partner)

    def sq_ref(p, c):
        return vb_sq.at[c, pl.ds(pl.multiple_of(QROWS * p, ALIGN), QROWS)]

    def small_refs(c):
        return (vb_kv, vb_dn) if c == 0 else (vb_up.at[0], vb_up.at[1])

    def column_new(u, v):
        new = update(wg[u].reshape(D, LANES), v)
        wg[u] = new.reshape(RING, RING, BROWS, LANES)
        return new

    @pl.when(core == 0)
    def _():
        v = ss[fin, 1, :LANES, :].astype(F32).T
        vb_kv[...] = column_new(SLAB, v).T.astype(BF16)
        for j in range(SLAB):
            v = ss[fin, 0, :, LANES * j:LANES * j + LANES].astype(F32).reshape(RING, RING, TILE16, LANES)
            lo = update(wg[SUB, :, :, SUB * j:SUB * j + SUB, :], v[:, :, :SUB])
            hi = update(wg[9, :, :, SUB * j:SUB * j + SUB, :], v[:, :, SUB:TILE16])
            wg[SUB, :, :, SUB * j:SUB * j + SUB, :] = lo
            wg[9, :, :, SUB * j:SUB * j + SUB, :] = hi
            vb_dn[:, LANES * j:LANES * j + LANES] = jnp.concatenate([lo, hi], axis=2).reshape(FF, LANES).astype(BF16)
        for i in range(PAIR):
            out_copy(SUB + i, small_refs(0)[i]).start()

    @pl.when(core == 1)
    def _():
        for i in range(PAIR):
            for h in range(PAIR):
                v = ss[fin, i, LANES * h:LANES * h + LANES, :].astype(F32).T
                vb_up[i, :, LANES * h:LANES * h + LANES] = column_new(SLAB + 2 * i + h, v).astype(BF16)
        for i in range(PAIR):
            out_copy(SUB + i, small_refs(1)[i]).start()

    for i in range(RING):
        q = around["z"][i]
        v = apply_rows(cur, pl.multiple_of(QROWS * q, ALIGN), QROWS).astype(F32)
        for u in range(SLAB):
            new = update(wg[u, q].reshape(QROWS, LANES), v[:, LANES * u:LANES * u + LANES])
            wg[u, q] = new.reshape(RING, BROWS, LANES)
            vb_sq[core, pl.ds(pl.multiple_of(QROWS * q, ALIGN), QROWS), LANES * u:LANES * u + LANES] = new.astype(BF16)
        out_copy(i, sq_ref(q, core)).start()
        if i == 0:
            for g in range(GROUPS):
                nb[g] = wg[RING * g + x, z, y]
            pack_rows(nb, outw)
            for k in range(SLAB):
                post(outw, wrecv, wo_s, wo_r, k).start()
            wrecv[slot] = outw[slot]

    for i in range(SLAB):
        post(outp, mrecv, mo_s, mo_r, i).wait_recv()
        post(outw, wrecv, wo_s, wo_r, i).wait_recv()

    for p in range(RING):
        out_copy(p, sq_ref(around["z"][p], core)).wait()
    for c in range(PAIR):
        @pl.when(core == c)
        def _():
            for i in range(PAIR):
                out_copy(SUB + i, small_refs(c)[i]).wait_send()
                out_copy(SUB + i, small_refs(1 - c)[i]).wait_recv()
    for i in range(SLAB):
        pre(0, i).wait_send()
        pre(1, i).wait_send()
        post(outp, mrecv, mo_s, mo_r, i).wait_send()
        post(outw, wrecv, wo_s, wo_r, i).wait_send()
    for k in range(RING):
        for i, item in enumerate(common_items(other, k, 1)):
            par_copy(k, i, item).wait_send()
        for tc in range(PAIR):
            @pl.when(core == 1 - tc)
            def _():
                for i, item in enumerate(special_items(tc, k, 1)):
                    par_copy(k, 2 + i, item).wait_send()
    for k in range(RING):
        rs1[k][RING]()
        u1[k][GROUPS]()
    rs2[RING]()
    rs3[3]()
    m3[2]()
    u2[3]()


def unpack_rows(slot, src, o_sq, o_kv, o_up, o_dn):
    for c in range(PAIR):
        for xs in range(RING):
            t = 2 * xs + c
            o_sq[:, c, LANES * xs:LANES * xs + LANES] = src[t, :SLAB, :]
            if xs < 3:
                o_sq[:, c, HALF_D + LANES * xs:P_AT + LANES * xs] = src[t, SUB:P_END, :]
    o_kv[:, 0, :] = src[HOPS, SUB:P_END, :KVD]
    o_kv[:, 1, :] = src[HOPS, SUB:P_END, KVD:LANES]
    o_up[:, 0, :LANES] = src[SLAB, SUB:P_END, :]
    o_up[:, 0, LANES:FF] = src[1, TILE16:Q_END, :]
    o_up[:, 1, :LANES] = src[3, TILE16:Q_END, :]
    o_up[:, 1, LANES:FF] = src[5, TILE16:Q_END, :]
    t = 2 * lax.div(slot, RING)
    for j in range(SLAB):
        o_dn[0, :, LANES * j:LANES * j + LANES] = src[t, DOWN_AT + PAIR * j:DOWN_NEXT + PAIR * j, :]


def write_out(
    mrecv, wrecv, vb_sq, vb_kv, vb_up, vb_dn,
    mo_sq, mo_kv, mo_up, mo_dn, wo_sq, wo_kv, wo_up, wo_dn, b_sq, b_kv, b_up, b_dn, *scratch,
):
    sem, stage = scratch[-1], scratch[:-1]
    copies = [pltpu.make_async_copy(src, dst, sem.at[i]) for i, (src, dst) in enumerate(
        ((vb_sq, b_sq), (vb_kv, b_kv), (vb_up, b_up), (vb_dn, b_dn)))]
    for cp in copies:
        cp.start()
    me = lax.axis_index("data")
    slot = lax.rem(me, SUB)
    for at, src, outs in ((0, mrecv, (mo_sq, mo_kv, mo_up, mo_dn)), (RING, wrecv, (wo_sq, wo_kv, wo_up, wo_dn))):
        bufs = stage[at:at + RING]
        unpack_rows(slot, src, *bufs)
        for i, out in enumerate(outs):
            copies.append(pltpu.make_async_copy(bufs[i], out, sem.at[RING + at + i]))
            copies[-1].start()
    for cp in copies:
        cp.wait()


def solution(mesh):
    grad_spec = P(("model", "data"))
    slab_spec = P("model", "data")
    full_spec = P("model")

    def local_step(g_sq, m_sq, w_sq, g_kv, m_kv, w_kv, g_up, m_up, w_up, g_dn, m_dn, w_dn):
        g_sq = g_sq.reshape(2, RING, RING, BROWS, D)
        g_kv = g_kv[0].transpose(0, 2, 1)
        g_up = g_up.reshape(2, RING, RING, BROWS, FF)
        g_dn = g_dn.reshape(RING, RING, TILE16, D)
        vm = pl.BlockSpec(memory_space=pltpu.VMEM)
        hb = pl.BlockSpec(memory_space=pltpu.HBM)
        V = pltpu.VMEM
        block = (BROWS, LANES)
        unit = (RING, RING) + block
        half = (PAIR, RING) + block
        two = (PAIR,) + block
        mats = (PAIR, PAIR)
        rows_of = (PAIR, SLAB, PAIR)
        floats = [
            (PAIR, RING) + unit, (PAIR, RING, RING, BROWS, TRIO), mats + (KVD, D), mats + (RING, RING, BROWS, FF), (PAIR, RING, RING, TILE16, D), (UNITS,) + unit,
            (RING, GROUPS, HOPS) + two, (GROUPS, HOPS) + two, (GROUPS,) + mats + two, (GROUPS, PAIR) + two,
            (UNITS,) + unit, (GROUPS, RING) + block,
            rows_of + (D,), rows_of + (KVD,), rows_of + (FF,), (2, 1, 2, D),
            mats + (RING, PACK, LANES), (PAIR, SUB, PACK, LANES), (PAIR, GROUPS) + block, (GROUPS,) + block, PACKED, PACKED,
        ]
        scratch = [V(a, F32) for a in floats] + [V((UNITS,) + unit, BF16), V((UNITS,) + unit, F32)]
        scratch += [V(a, BF16) for a in ((PAIR, D, D), (D, D), (D, D), mats + (FF, D), (PAIR, FF, FF), (PAIR, FF, FF))]
        rings, ring, pairs, direct, row = (RING, GROUPS, HOPS), (GROUPS, HOPS), (GROUPS, RING), (GROUPS, GROUPS), (SLAB,)
        sems = [(RING, 5), (2, RING)]
        for a in ((RING, 5), (PAIR,) + row, row, row, rings, ring, pairs, direct, ring, rings, direct, ring, ring, (10,)):
            sems += [a, a]
        scratch += [DMA(a) for a in sems]

        def rows(a):
            return a.transpose(1, 0, 2)

        mid = [V(s, F32) for s in (PACKED, PACKED)]
        mid += [V(s, BF16) for s in ((2, D, D), (LANES, D), (2, D, FF), (FF, D))]
        parts = pl.pallas_call(
            kernel,
            out_shape=mid,
            in_specs=[hb] * UNITS,
            out_specs=[vm] * HOPS,
            scratch_shapes=scratch,
            compiler_params=pltpu.CompilerParams(collective_id=0, has_side_effects=True, vmem_limit_bytes=61700000),
            name="muon",
        )(g_sq, g_kv, g_up, g_dn, rows(m_sq), rows(m_kv), rows(m_up), m_dn, rows(w_sq), rows(w_kv), rows(w_up), w_dn)
        small = [jax.ShapeDtypeStruct(s, F32) for s in ((SLAB, PAIR, D), (SLAB, PAIR, KVD), (SLAB, PAIR, FF), (1, PAIR, D))]
        full = [jax.ShapeDtypeStruct(s, BF16) for s in ((2, D, D), (LANES, D), (2, D, FF), (FF, D))]
        out = pl.pallas_call(
            write_out,
            out_shape=small + small + full,
            in_specs=[vm] * HOPS,
            out_specs=[hb] * UNITS,
            scratch_shapes=[V(a.shape, F32) for a in small + small] + [DMA((UNITS,))],
            compiler_params=pltpu.CompilerParams(vmem_limit_bytes=4_000_000),
            name="write_out",
        )(*parts)
        m, w, b = out[0:RING], out[RING:SUB], out[SUB:UNITS]
        return (
            rows(m[0]), rows(w[0]), b[0],
            rows(m[1]), rows(w[1]), b[1].reshape(2, KVD, D).transpose(0, 2, 1),
            rows(m[2]), rows(w[2]), b[2],
            m[3], w[3], b[3].reshape(1, FF, D),
        )

    in_specs = (grad_spec, slab_spec, slab_spec) * RING
    out_specs = (slab_spec, slab_spec, full_spec) * RING
    return jax.shard_map(local_step, mesh=mesh, in_specs=in_specs, out_specs=out_specs, check_vma=False)
```
